32 devices in a mesh: rep: 1 (over z), data: 4 (over y), expert: 8 (over x, core).
Axes of the slice: x: 4, y: 4, z: 1, core: 2. Of those that a mesh axis runs over, the one named last changes fastest.
The devices are a block of a 4x4x8 slice.
Arguments:
- x: bfloat16 [32768, 2304], P(('rep', 'expert', 'data'))
- expert_idx: int32 [32768, 2], P(('rep', 'expert', 'data'))
- gate: float32 [32768, 2], P(('rep', 'expert', 'data'))
- w_gate: bfloat16 [8, 2304, 5760], P('expert', 'data')
- w_up: bfloat16 [8, 2304, 5760], P('expert', 'data')
- w_down: bfloat16 [8, 5760, 2304], P('expert', None, 'data')
Outputs:
- output: bfloat16 [32768, 2304], P(('rep', 'expert', 'data'))
All inputs are finite; a program needn't handle non-finite values.
Results may differ from the reference program's by a relative error of at most 0.001.
Values are sent between devices in bfloat16 or wider.
A program may use at most 768 MiB of HBM per device.

```python
import jax
import jax.numpy as jnp
from jax import lax

TOK_DEV = 1024
D_MODEL = 2304
FFN = 5760
EXPERTS = 8
TOP_K = 2
EP_SIZE = 8
DP_SIZE = 4
CAPACITY = 320


def route_ids(key):
    n_blocks = EP_SIZE * DP_SIZE
    key_bias, key_hot, key_score = jax.random.split(key, 3)
    expert_bias = jax.random.randint(key_bias, (EXPERTS,), 0, 2 ** 20, dtype=jnp.int32)
    hot_expert = jax.random.randint(key_hot, (), 0, EXPERTS, dtype=jnp.int32)
    scores = jax.random.randint(key_score, (n_blocks, TOK_DEV, EXPERTS), 0, 2 ** 20, dtype=jnp.int32) + expert_bias
    forced = (jnp.arange(TOK_DEV) < CAPACITY)[None, :, None] & (jnp.arange(EXPERTS) == hot_expert)[None, None, :]
    scores = (scores + forced.astype(jnp.int32) * 2 ** 21) * EXPERTS + jnp.arange(EXPERTS, dtype=jnp.int32)
    chosen = lax.top_k(scores, TOP_K)[1]
    return chosen.reshape(n_blocks * TOK_DEV, TOP_K).astype(jnp.int32)


def setup_inputs(seed: int = 0, part: int = 0) -> dict:
    key_shared, key_local = jax.random.split(jax.random.key(seed))
    key_tok, key_route, key_gate = jax.random.split(jax.random.fold_in(key_local, part), 3)
    key_wg, key_wu, key_wd = jax.random.split(key_shared, 3)
    n_rows = EP_SIZE * DP_SIZE * TOK_DEV
    x = jax.random.normal(key_tok, (n_rows, D_MODEL), jnp.float32).astype(jnp.bfloat16)
    gate = jax.random.uniform(key_gate, (n_rows, TOP_K), jnp.float32, 0.2, 0.8)
    w_gate = (jax.random.normal(key_wg, (EXPERTS, D_MODEL, FFN), jnp.float32) * D_MODEL ** -0.5).astype(jnp.bfloat16)
    w_up = (jax.random.normal(key_wu, (EXPERTS, D_MODEL, FFN), jnp.float32) * D_MODEL ** -0.5).astype(jnp.bfloat16)
    w_down = (jax.random.normal(key_wd, (EXPERTS, FFN, D_MODEL), jnp.float32) * (1.5 * FFN ** -0.5)).astype(jnp.bfloat16)
    return {"x": x, "expert_idx": route_ids(key_route), "gate": gate, "w_gate": w_gate, "w_up": w_up, "w_down": w_down}


def slot_table(ids_flat):
    one_hot = (ids_flat[:, None] == jnp.arange(EXPERTS, dtype=jnp.int32)[None, :]).astype(jnp.int32)
    slot_ids = jnp.sum((jnp.cumsum(one_hot, axis=0) - one_hot) * one_hot, axis=1)
    return jnp.where(slot_ids < CAPACITY, ids_flat * CAPACITY + slot_ids, EXPERTS * CAPACITY)


def take_rows(block, index):
    return jnp.take(block, index, axis=0, mode="fill", fill_value=0)


def reference(x, expert_idx, gate, w_gate, w_up, w_down):
    n_blocks = EP_SIZE * DP_SIZE
    x_blocks = x.reshape(n_blocks, TOK_DEV, D_MODEL)
    dest_row = jax.vmap(slot_table)(expert_idx.reshape(n_blocks, TOK_DEV * TOP_K))
    block_ids = jnp.arange(n_blocks)[:, None]
    pair_token = jnp.broadcast_to(jnp.arange(TOK_DEV * TOP_K, dtype=jnp.int32) // TOP_K, dest_row.shape)
    src_tok = jnp.full((n_blocks, EXPERTS * CAPACITY), TOK_DEV, jnp.int32).at[block_ids, dest_row].set(pair_token, mode="drop")
    slot_gate = jnp.zeros((n_blocks, EXPERTS * CAPACITY), jnp.float32).at[block_ids, dest_row].set(gate.reshape(n_blocks, TOK_DEV * TOP_K), mode="drop")
    src_by_exp = src_tok.reshape(n_blocks, EXPERTS, CAPACITY).transpose(1, 0, 2)
    gate_by_exp = slot_gate.reshape(n_blocks, EXPERTS, CAPACITY).transpose(1, 0, 2)

    def expert_step(running, inputs):
        src_e, gate_e, wg_e, wu_e, wd_e = inputs
        expert_rows = jax.vmap(take_rows)(x_blocks, src_e).reshape(n_blocks * CAPACITY, D_MODEL)
        gate_act = jnp.dot(expert_rows, wg_e, preferred_element_type=jnp.float32)
        up_act = jnp.dot(expert_rows, wu_e, preferred_element_type=jnp.float32)
        hidden = (jax.nn.silu(gate_act) * up_act).astype(jnp.bfloat16)
        out_rows = jnp.dot(hidden, wd_e, preferred_element_type=jnp.float32).astype(jnp.bfloat16)
        contrib = out_rows.reshape(n_blocks, CAPACITY, D_MODEL).astype(jnp.float32) * gate_e[:, :, None]
        return running.at[block_ids, src_e].add(contrib, mode="drop"), None

    summed = lax.scan(expert_step, x_blocks.astype(jnp.float32), (src_by_exp, gate_by_exp, w_gate, w_up, w_down))[0]
    return summed.astype(jnp.bfloat16).reshape(n_blocks * TOK_DEV, D_MODEL)
```

```python
import functools

import jax
import jax.numpy as jnp
from jax import lax
from jax.experimental import pallas as pl
from jax.experimental.pallas import tpu as pltpu
from jax.sharding import PartitionSpec as P

MESH = pl.DeviceIdType.MESH
F32 = jnp.float32
BF16 = jnp.bfloat16
LEAD = 4
DOWN_STEP = 12


def capacity_rows(tok_rows, top_k, n_exp):
    return max(8, ((5 * top_k * tok_rows) // (4 * n_exp) + 7) // 8 * 8)


def pick(total, options):
    return next(c for c in options if total % c == 0)


def moe_kernel(dims, idx_ref, gate_ref, x_ref, wg_ref, wu_ref, wd_ref, y_ref, xpar_ref, xrows_ref, gu_ref, wdb_ref, back_ref,
               h, keyt, keyt_par, keyc, gate_e,
               s_x, r_x, s_own, r_own, s_par, r_par, l_loc, l_x,
               s_main, s_a, s_b, s_c, r_gu, l_w,
               t_main, t_a, t_b, t_c, r_wd, l_wd, s_ret, r_back, l_back):
    n_x, tok, d_model, d_q, ffn, cap, fc, n_k, n_w, n_j, tile = dims
    rows = 2 * n_x * cap
    wk = ffn // n_w
    xc = d_model // n_j
    p = lax.axis_index("expert")
    q = lax.axis_index("data")
    cx, cc = p // 2, p % 2
    half = q // 2
    inner = q + 1 - 2 * (q % 2)
    outer = 3 - q
    lead = cc == half

    def dev(x, y, c):
        return {"expert": 2 * x + c, "data": y}

    def quarter(i):
        base = q + (i // 2) * (inner - q)
        return base + (i % 2) * (3 - 2 * base)

    partner = dev(cx, q, 1 - cc)
    inner_dev = dev(cx, inner, cc)
    outer_dev = dev(cx, outer, 1 - cc)
    mirror = dev(cx, outer, cc)

    def remote(src, dst, send, recv, device):
        return pltpu.make_async_remote_copy(src_ref=src, dst_ref=dst, send_sem=send, recv_sem=recv, device_id=device, device_id_type=MESH)

    def wait_for(ref, sem):
        pltpu.make_async_copy(ref, ref, sem).wait()

    barrier = pltpu.get_barrier_semaphore()
    peers = [partner, inner_dev, outer_dev]
    peers += [dev((cx + d) % n_x, q, cc) for d in range(1, n_x)]
    peers += [dev((cx + d) % n_x, outer, cc) for d in range(n_x)]
    for peer in peers:
        pl.semaphore_signal(barrier, inc=1, device_id=peer, device_id_type=MESH)
    pl.semaphore_wait(barrier, len(peers))

    def gu_rows(k, i):
        return gu_ref.at[k, pl.ds(quarter(i) * d_q, d_q), :]

    def send_own_gu(k, device, send, recv):
        src = pl.ds(pl.multiple_of(k * fc, 128), fc)
        for w_ref, c0 in ((wg_ref, 0), (wu_ref, fc)):
            remote(w_ref.at[:, src], gu_ref.at[k, pl.ds(q * d_q, d_q), pl.ds(c0, fc)], send, recv, device).start()

    def pass_gu(k, i, device, send, i_there):
        remote(gu_rows(k, i), gu_rows(k, i), send, r_gu.at[i_there, k], device).start()

    for j in range(n_j):
        cols = pl.ds(j * xc, xc)
        remote(x_ref.at[:, cols], xpar_ref.at[:, cols], s_x.at[j], r_x.at[j], mirror).start()

    def start_gu(k, carry):
        @pl.when(lead)
        def _():
            send_own_gu(k, inner_dev, s_main.at[k], r_gu.at[2, k])

        @pl.when(jnp.logical_not(lead))
        def _():
            send_own_gu(k, outer_dev, s_main.at[k], r_gu.at[1, k])

        return carry

    lax.fori_loop(0, n_k, start_gu, 0)

    own_x = pltpu.make_async_copy(x_ref, h.at[pl.ds(0, tok), pl.ds(d_model, d_model)], l_x.at[0])
    own_x.start()
    lane = lax.broadcasted_iota(jnp.int32, (tok, 128), 1)
    first = lane == idx_ref[:, 0:1]
    second = lane == idx_ref[:, 1:2]
    chosen = jnp.logical_or(first, second)
    before = lax.broadcasted_iota(jnp.int32, (tok, tok), 0) > lax.broadcasted_iota(jnp.int32, (tok, tok), 1)
    slot = jnp.dot(before.astype(F32).astype(BF16), chosen.astype(F32).astype(BF16), preferred_element_type=F32)
    key = jnp.where(jnp.logical_and(chosen, slot < cap), slot, -1.0)
    keyc[...] = key
    keyt[...] = key.T[:8, :]
    gate_e[...] = jnp.where(first, gate_ref[:, 0:1], 0.0) + jnp.where(second, gate_ref[:, 1:2], 0.0)
    send_key = remote(keyt, keyt_par, s_x.at[n_j], r_x.at[n_j], mirror)
    send_key.start()

    slots = lax.broadcasted_iota(jnp.int32, (cap, tok), 0).astype(F32)

    def select(keys, d):
        e = 2 * lax.rem(cx + d, n_x) + half
        return (slots == keys[pl.ds(e, 1), :]).astype(F32).astype(BF16)

    own_x.wait()

    def own_rows(t, carry):
        d = lax.rem(t + 1, n_x)
        pick_rows = select(keyt, d)
        stage = h.at[pl.ds(pl.multiple_of(t * cap, 8), cap), pl.ds(0, d_model)]
        for j in range(n_j):
            got = jnp.dot(pick_rows, h[pl.ds(0, tok), pl.ds(d_model + j * xc, xc)], preferred_element_type=F32)
            h[pl.ds(pl.multiple_of(t * cap, 8), cap), pl.ds(j * xc, xc)] = got.astype(BF16)
        dst = xrows_ref.at[pl.ds(pl.multiple_of(cx * 2 * cap, 8), cap), :]

        @pl.when(t < n_x - 1)
        def _():
            remote(stage, dst, s_own.at[t], r_own, dev(lax.rem(cx + d, n_x), q, cc)).start()

        @pl.when(t == n_x - 1)
        def _():
            pltpu.make_async_copy(stage, dst, l_loc.at[n_j]).start()

        return carry

    lax.fori_loop(0, n_x, own_rows, 0)

    def start_own_pass(k, carry):
        @pl.when(lead)
        def _():
            send_own_gu(k, partner, s_a.at[k], r_gu.at[0, k])

        return carry

    lax.fori_loop(0, n_k, start_own_pass, 0)

    send_key.wait()

    def par_cols(j, carry):
        cols = pl.ds(pl.multiple_of(j * xc, 128), xc)
        wait_for(xpar_ref.at[:, cols], r_x.at[j])
        here = pl.ds(pl.multiple_of(d_model + j * xc, 128), xc)
        load = pltpu.make_async_copy(xpar_ref.at[:, cols], h.at[pl.ds(tok, tok), here], l_x.at[1])
        load.start()
        load.wait()

        def par_rows(t, carry2):
            d = lax.rem(t + 1, n_x)
            r0 = pl.multiple_of((n_x + t) * cap, 8)
            got = jnp.dot(select(keyt_par, d), h[pl.ds(tok, tok), here], preferred_element_type=F32)
            h[pl.ds(r0, cap), cols] = got.astype(BF16)
            stage = h.at[pl.ds(r0, cap), cols]
            dst = xrows_ref.at[pl.ds(pl.multiple_of((cx * 2 + 1) * cap, 8), cap), cols]

            @pl.when(t < n_x - 1)
            def _():
                remote(stage, dst, s_par.at[t, j], r_par, dev(lax.rem(cx + d, n_x), q, cc)).start()

            @pl.when(t == n_x - 1)
            def _():
                pltpu.make_async_copy(stage, dst, l_loc.at[j]).start()

            return carry2

        return lax.fori_loop(0, n_x, par_rows, carry)

    lax.fori_loop(0, n_j, par_cols, 0)

    def ahead(k):
        @pl.when(lead)
        def _():
            wait_for(gu_rows(k, 2), r_gu.at[2, k])
            pass_gu(k, 2, partner, s_b.at[k], 2)

        @pl.when(jnp.logical_not(lead))
        def _():
            wait_for(gu_rows(k, 1), r_gu.at[1, k])
            pass_gu(k, 1, inner_dev, s_a.at[k], 3)
            pass_gu(k, 1, partner, s_b.at[k], 1)

    def wd_rows(i, m):
        return wdb_ref.at[quarter(i), pl.ds(pl.multiple_of(m * wk, 8), wk), :]

    def send_own_wd(m, device, send, recv):
        src = wd_ref.at[pl.ds(pl.multiple_of(m * wk, 8), wk), :]
        remote(src, wd_rows(0, m), send, recv, device).start()

    def phase_up(xr, wbuf):
        def gather_chunk(k, slot):
            @pl.when(lead)
            def _():
                wait_for(gu_rows(k, 1), r_gu.at[1, k])
                wait_for(gu_rows(k, 3), r_gu.at[3, k])
                src = pl.ds(pl.multiple_of(k * fc, 128), fc)
                for w_ref, c0 in ((wg_ref, 0), (wu_ref, fc)):
                    pltpu.make_async_copy(w_ref.at[:, src], wbuf.at[slot, pl.ds(q * d_q, d_q), pl.ds(c0, fc)], l_w.at[slot]).start()
                for i in (1, 2, 3):
                    pltpu.make_async_copy(gu_rows(k, i), wbuf.at[slot, pl.ds(quarter(i) * d_q, d_q), :], l_w.at[slot]).start()

            @pl.when(jnp.logical_not(lead))
            def _():
                wait_for(gu_rows(k, 3), r_gu.at[3, k])
                pass_gu(k, 3, partner, s_c.at[k], 3)
                wait_for(gu_rows(k, 0), r_gu.at[0, k])
                wait_for(gu_rows(k, 2), r_gu.at[2, k])
                pltpu.make_async_copy(gu_ref.at[k], wbuf.at[slot], l_w.at[slot]).start()

        for k in range(LEAD):
            ahead(k)

        wait_for(xrows_ref.at[pl.ds(0, (n_x - 1) * cap), :], r_own)
        wait_for(xrows_ref.at[pl.ds(0, (n_x - 1) * cap), :], r_par)
        wait_for(xrows_ref.at[pl.ds(0, cap), :], l_loc.at[n_j])
        for j in range(n_j):
            wait_for(xrows_ref.at[pl.ds(0, cap), pl.ds(0, xc)], l_loc.at[j])
        load = pltpu.make_async_copy(xrows_ref, xr, l_x.at[0])
        load.start()

        def drain(t, carry):
            wait_for(xrows_ref.at[pl.ds(0, cap), :], s_own.at[t])

            def inner_drain(j, carry2):
                wait_for(xrows_ref.at[pl.ds(0, cap), pl.ds(0, xc)], s_par.at[t, j])
                return carry2

            return lax.fori_loop(0, n_j, inner_drain, carry)

        lax.fori_loop(0, n_x - 1, drain, 0)
        for j in range(n_j):
            wait_for(xpar_ref.at[:, pl.ds(0, xc)], s_x.at[j])

        def start_wd(m, carry):
            @pl.when(jnp.logical_not(lead))
            def _():
                send_own_wd(m, outer_dev, t_main.at[m], r_wd.at[1, m])

            @pl.when(lead)
            def _():
                send_own_wd(m, partner, t_a.at[m], r_wd.at[0, m])

            return carry

        lax.fori_loop(0, n_w, start_wd, 0)
        gather_chunk(0, 0)
        load.wait()

        def step(k, carry):
            slot = lax.rem(k, 2)

            @pl.when(k + LEAD < n_k)
            def _():
                ahead(k + LEAD)

            @pl.when(jnp.logical_and(k == min(DOWN_STEP, n_k - 1), lead))
            def _():
                def start_near(m, carry2):
                    send_own_wd(m, inner_dev, t_main.at[m], r_wd.at[2, m])
                    return carry2

                lax.fori_loop(0, n_w, start_near, 0)

            @pl.when(k + 1 < n_k)
            def _():
                gather_chunk(k + 1, lax.rem(k + 1, 2))

            wait_for(wbuf.at[slot], l_w.at[slot])

            def row_tile(r, carry2):
                r0 = pl.multiple_of(r * tile, 8)
                both = jnp.dot(xr[pl.ds(r0, tile), :], wbuf[slot], preferred_element_type=F32)
                act = jax.nn.silu(both[:, :fc]) * both[:, fc:]
                h[pl.ds(r0, tile), pl.ds(pl.multiple_of(k * fc, 128), fc)] = act.astype(BF16)
                return carry2

            lax.fori_loop(0, rows // tile, row_tile, 0)
            return carry

        lax.fori_loop(0, n_k, step, 0)

    def phase_down(wdv, stage, acc, cmat, backv):
        t_tile = min(256, tok)

        def ret_dst(i):
            return back_ref.at[quarter(i), half, pl.ds(pl.multiple_of(cx * cap, 8), cap), :]

        def load_wd(i):
            def load_part(m, carry):
                dst = wdv.at[pl.ds(pl.multiple_of(m * wk, 8), wk), :]

                @pl.when(jnp.logical_and(lead, i == 0))
                def _():
                    pltpu.make_async_copy(wd_ref.at[pl.ds(pl.multiple_of(m * wk, 8), wk), :], dst, l_wd.at[m]).start()

                @pl.when(jnp.logical_not(jnp.logical_and(lead, i == 0)))
                def _():
                    wait_for(wd_rows(i, m), r_wd.at[i, m])

                    @pl.when(jnp.logical_and(lead, i == 2))
                    def _():
                        remote(wd_rows(2, m), wd_rows(2, m), t_b.at[m], r_wd.at[2, m], partner).start()

                    @pl.when(jnp.logical_and(jnp.logical_not(lead), i == 1))
                    def _():
                        remote(wd_rows(1, m), wd_rows(1, m), t_b.at[m], r_wd.at[1, m], partner).start()

                    @pl.when(jnp.logical_and(jnp.logical_not(lead), i == 3))
                    def _():
                        remote(wd_rows(3, m), wd_rows(3, m), t_c.at[m], r_wd.at[3, m], partner).start()

                    pltpu.make_async_copy(wd_rows(i, m), dst, l_wd.at[m]).start()

                return carry

            lax.fori_loop(0, n_w, load_part, 0)
            for m in range(n_w):
                wait_for(wdv.at[pl.ds(m * wk, wk), :], l_wd.at[m])

        def combine(qt, g, add):
            load = pltpu.make_async_copy(back_ref.at[qt, g], backv, l_back)
            load.start()
            load.wait()

            def tok_tile(r, carry):
                r0 = pl.multiple_of(r * t_tile, 8)
                gates = gate_e[pl.ds(r0, t_tile), :]
                lanes = lax.broadcasted_iota(jnp.int32, (t_tile, 128), 1)
                total = None
                for x in range(n_x):
                    e = 2 * x + g
                    rows_x = jnp.dot(cmat[e, pl.ds(r0, t_tile), :], backv[pl.ds(x * cap, cap), :], preferred_element_type=F32)
                    gate_x = jnp.sum(jnp.where(lanes == e, gates, 0.0), axis=1, keepdims=True)
                    total = gate_x * rows_x if total is None else total + gate_x * rows_x
                if add:
                    total = total + acc[qt, pl.ds(r0, t_tile), :]
                acc[qt, pl.ds(r0, t_tile), :] = total
                return carry

            lax.fori_loop(0, tok // t_tile, tok_tile, 0)

        def units(i):
            def both(add):
                wait_for(back_ref.at[0, 0, pl.ds(0, (n_x - 1) * cap), :], r_back.at[quarter(i), half])
                combine(quarter(i), half, add)
                wait_for(back_ref.at[0, 0], r_back.at[3 - quarter(i), 1 - half])
                combine(3 - quarter(i), 1 - half, add)

            @pl.when(i % 2 == 0)
            def _():
                both(False)

            @pl.when(i % 2 == 1)
            def _():
                both(True)

        def piece(i, carry):
            load_wd(i)

            def block(t, carry2):
                s = 1 - t // n_x
                x_src = lax.rem(cx + 1 + t % n_x, n_x)
                r0 = pl.multiple_of((x_src * 2 + s) * cap, 8)
                out = jnp.dot(h[pl.ds(r0, cap), :], wdv[...], preferred_element_type=F32)

                @pl.when(i > 0)
                def _():
                    wait_for(stage.at[t], s_ret.at[t])

                stage[t] = out.astype(BF16)

                @pl.when(t < 2 * n_x - 1)
                def _():
                    remote(stage.at[t], ret_dst(i), s_ret.at[t], r_back.at[quarter(i), half], dev(x_src, q + s * (outer - q), cc)).start()

                @pl.when(t == 2 * n_x - 1)
                def _():
                    pltpu.make_async_copy(stage.at[t], ret_dst(i), s_ret.at[t]).start()

                return carry2

            lax.fori_loop(0, 2 * n_x, block, 0)

            @pl.when(jnp.logical_and(i == 1, jnp.logical_not(lead)))
            def _():
                def near(m, carry2):
                    remote(wd_rows(1, m), wd_rows(1, m), t_a.at[m], r_wd.at[3, m], inner_dev).start()
                    return carry2

                lax.fori_loop(0, n_w, near, 0)

            @pl.when(i == 0)
            def _():
                slot_lane = lax.broadcasted_iota(jnp.int32, (tok, cap), 1).astype(F32)
                for e in range(2 * n_x):
                    cmat[e] = (slot_lane == keyc[:, e:e + 1]).astype(F32).astype(BF16)

            @pl.when(i > 0)
            def _():
                units(i - 1)

            return carry

        lax.fori_loop(0, 4, piece, 0)

        x_here = h.at[pl.ds(0, tok), pl.ds(0, d_model)]
        load = pltpu.make_async_copy(x_ref, x_here, l_x.at[0])
        load.start()
        for t in range(2 * n_x):
            wait_for(stage.at[t], s_ret.at[t])
        units(jnp.int32(3))
        load.wait()

        def finish(r, carry):
            r0 = pl.multiple_of(r * t_tile, 8)
            for qt in range(4):
                cols = pl.ds(qt * d_q, d_q)
                total = h[pl.ds(r0, t_tile), cols].astype(F32) + acc[qt, pl.ds(r0, t_tile), :]
                h[pl.ds(r0, t_tile), cols] = total.astype(BF16)
            return carry

        lax.fori_loop(0, tok // t_tile, finish, 0)
        store = pltpu.make_async_copy(x_here, y_ref, l_x.at[0])
        store.start()
        store.wait()

    pl.run_scoped(phase_up, pltpu.VMEM((rows, d_model), BF16), pltpu.VMEM((2, d_model, 2 * fc), BF16))
    pl.run_scoped(
        phase_down,
        pltpu.VMEM((ffn, d_q), BF16),
        pltpu.VMEM((2 * n_x, cap, d_q), BF16),
        pltpu.VMEM((4, tok, d_q), F32),
        pltpu.VMEM((2 * n_x, tok, cap), BF16),
        pltpu.VMEM((n_x * cap, d_q), BF16),
    )

    def drain_gu(k, carry):
        wait_for(gu_rows(k, 0), s_main.at[k])
        wait_for(gu_rows(k, 0), s_a.at[k])
        wait_for(gu_rows(k, 0), s_b.at[k])

        @pl.when(jnp.logical_not(lead))
        def _():
            wait_for(gu_rows(k, 0), s_c.at[k])

        return carry

    lax.fori_loop(0, n_k, drain_gu, 0)

    def drain_wd(m, carry):
        wait_for(wd_rows(0, m), t_main.at[m])
        wait_for(wd_rows(0, m), t_a.at[m])
        wait_for(wd_rows(0, m), t_b.at[m])

        @pl.when(jnp.logical_not(lead))
        def _():
            wait_for(wd_rows(0, m), t_c.at[m])

        return carry

    lax.fori_loop(0, n_w, drain_wd, 0)


def solution(mesh):
    n_group, n_y = mesh.shape["expert"], mesh.shape["data"]
    assert n_y == 4 and n_group % 2 == 0
    n_x = n_group // 2
    tok_spec = P(("rep", "expert", "data"), None)
    wide_spec = P("expert", "data", None)
    down_spec = P("expert", None, "data")

    def device_step(x_loc, idx_loc, gate_loc, wg_loc, wu_loc, wd_loc):
        tok, d_model = x_loc.shape
        n_local, d_q, ffn = wg_loc.shape
        assert n_local == 1 and n_group == 8
        cap = capacity_rows(tok, idx_loc.shape[1], n_group)
        fc = pick(ffn, (384, 256, 128))
        n_k, n_w, n_j = ffn // fc, pick(ffn // 16, (3, 2, 1)), pick(d_model // 128, (3, 2, 1))
        rows = 2 * n_x * cap
        tile = pick(rows, (640, 48, 8))
        dims = (n_x, tok, d_model, d_q, ffn, cap, fc, n_k, n_w, n_j, tile)
        hbm = pl.BlockSpec(memory_space=pl.ANY)
        vmem = pl.BlockSpec(memory_space=pltpu.VMEM)
        dma = pltpu.SemaphoreType.DMA
        shape = jax.ShapeDtypeStruct
        outs = pl.pallas_call(
            functools.partial(moe_kernel, dims),
            name="moe_layer",
            out_shape=[
                shape((tok, d_model), BF16),
                shape((tok, d_model), BF16),
                shape((rows, d_model), BF16),
                shape((n_k, d_model, 2 * fc), BF16),
                shape((4, ffn, d_q), BF16),
                shape((4, 2, n_x * cap, d_q), BF16),
            ],
            in_specs=[vmem, vmem, hbm, hbm, hbm, hbm],
            out_specs=[hbm] * 6,
            scratch_shapes=[
                pltpu.VMEM((rows, ffn), BF16),
                pltpu.VMEM((8, tok), F32),
                pltpu.VMEM((8, tok), F32),
                pltpu.VMEM((tok, 128), F32),
                pltpu.VMEM((tok, 128), F32),
                dma((n_j + 1,)), dma((n_j + 1,)), dma((n_x - 1,)), dma, dma((n_x - 1, n_j)), dma, dma((n_j + 1,)), dma((2,)),
                dma((n_k,)), dma((n_k,)), dma((n_k,)), dma((n_k,)), dma((4, n_k)), dma((2,)),
                dma((n_w,)), dma((n_w,)), dma((n_w,)), dma((n_w,)), dma((4, n_w)), dma((n_w,)),
                dma((2 * n_x,)), dma((4, 2)), dma,
            ],
            compiler_params=pltpu.CompilerParams(collective_id=0, has_side_effects=True, vmem_limit_bytes=67_043_328),
        )(idx_loc, gate_loc, x_loc, wg_loc.reshape(d_q, ffn), wu_loc.reshape(d_q, ffn), wd_loc.reshape(ffn, d_q))
        return outs[0]

    return jax.shard_map(device_step, mesh=mesh, in_specs=(tok_spec, tok_spec, tok_spec, wide_spec, wide_spec, down_spec), out_specs=tok_spec, check_vma=False)
```

```python
import functools

import jax
import jax.numpy as jnp
from jax import lax
from jax.experimental import pallas as pl
from jax.experimental.pallas import tpu as pltpu
from jax.sharding import PartitionSpec as P

MESH = pl.DeviceIdType.MESH
F32 = jnp.float32
BF16 = jnp.bfloat16
LEAD = 4
EARLY = 11
DOWN_STEP = 12
LAG = 3


def capacity_rows(tok_rows, top_k, n_exp):
    return max(8, ((5 * top_k * tok_rows) // (4 * n_exp) + 7) // 8 * 8)


def pick(total, options):
    return next(c for c in options if total % c == 0)


def moe_kernel(dims, idx_ref, gate_ref, x_ref, wg_ref, wu_ref, wd_ref, y_ref, xpar_ref, xrows_ref, gu_ref, wdb_ref, back_ref,
               h, keyt, keyt_par, keyc, gate_e,
               s_x, r_x, s_own, r_own, s_par, r_par, l_loc, l_x,
               s_main, s_a, s_b, s_c, r_gu, l_w,
               t_main, t_a, t_b, t_c, r_wd, l_wd, s_ret, r_back, l_back):
    n_x, tok, d_model, d_q, ffn, cap, fc, n_k, n_w, n_j, tile = dims
    rows = 2 * n_x * cap
    wk = d_q // n_w
    xc = d_model // n_j
    p = lax.axis_index("expert")
    q = lax.axis_index("data")
    cx, cc = p // 2, p % 2
    half = q // 2
    inner = q + 1 - 2 * (q % 2)
    outer = 3 - q
    lead = cc == half

    def dev(x, y, c):
        return {"expert": 2 * x + c, "data": y}

    def quarter(i):
        base = q + (i // 2) * (inner - q)
        return base + (i % 2) * (3 - 2 * base)

    partner = dev(cx, q, 1 - cc)
    inner_dev = dev(cx, inner, cc)
    outer_dev = dev(cx, outer, 1 - cc)
    mirror = dev(cx, outer, cc)

    def remote(src, dst, send, recv, device):
        return pltpu.make_async_remote_copy(src_ref=src, dst_ref=dst, send_sem=send, recv_sem=recv, device_id=device, device_id_type=MESH)

    def wait_for(ref, sem):
        pltpu.make_async_copy(ref, ref, sem).wait()

    barrier = pltpu.get_barrier_semaphore()
    peers = [partner, inner_dev, outer_dev]
    peers += [dev((cx + d) % n_x, q, cc) for d in range(1, n_x)]
    peers += [dev((cx + d) % n_x, outer, cc) for d in range(n_x)]
    for peer in peers:
        pl.semaphore_signal(barrier, inc=1, device_id=peer, device_id_type=MESH)
    pl.semaphore_wait(barrier, len(peers))

    def gu_rows(k, i):
        return gu_ref.at[k, pl.ds(quarter(i) * d_q, d_q), :]

    def send_own_gu(k, device, send, recv):
        src = pl.ds(pl.multiple_of(k * fc, 128), fc)
        for w_ref, c0 in ((wg_ref, 0), (wu_ref, fc)):
            remote(w_ref.at[:, src], gu_ref.at[k, pl.ds(q * d_q, d_q), pl.ds(c0, fc)], send, recv, device).start()

    def pass_gu(k, i, device, send, i_there):
        remote(gu_rows(k, i), gu_rows(k, i), send, r_gu.at[i_there, k], device).start()

    def send_block(j):
        cols = pl.ds(j * xc, xc)
        remote(x_ref.at[:, cols], xpar_ref.at[:, cols], s_x.at[j], r_x.at[j], mirror).start()

    def each(count, body):
        lax.fori_loop(0, count, lambda k, carry: (body(k), carry)[1], 0)

    send_block(0)
    early = min(EARLY, n_k)

    @pl.when(lead)
    def _():
        each(early, lambda k: send_own_gu(k, inner_dev, s_main.at[k], r_gu.at[2, k]))

    own_x = pltpu.make_async_copy(x_ref, h.at[pl.ds(0, tok), pl.ds(d_model, d_model)], l_x.at[0])
    own_x.start()
    expert = lax.broadcasted_iota(jnp.int32, (128, tok), 0)
    first = expert == idx_ref[0:1, :]
    second = expert == idx_ref[1:2, :]
    chosen = jnp.logical_or(first, second)
    before = lax.broadcasted_iota(jnp.int32, (tok, tok), 0) < lax.broadcasted_iota(jnp.int32, (tok, tok), 1)
    slot = jnp.dot(chosen.astype(F32).astype(BF16), before.astype(F32).astype(BF16), preferred_element_type=F32)
    key = jnp.where(jnp.logical_and(chosen, slot < cap), slot, -1.0)
    keyt[...] = key[:8, :]
    keyc[...] = key.T
    gate_e[...] = (jnp.where(first, gate_ref[0:1, :], 0.0) + jnp.where(second, gate_ref[1:2, :], 0.0)).T
    send_key = remote(keyt, keyt_par, s_x.at[n_j], r_x.at[n_j], mirror)
    send_key.start()
    for j in range(1, n_j):
        send_block(j)

    @pl.when(jnp.logical_not(lead))
    def _():
        each(n_k, lambda k: send_own_gu(k, outer_dev, s_main.at[k], r_gu.at[1, k]))


    slots = lax.broadcasted_iota(jnp.int32, (cap, tok), 0).astype(F32)

    def select(keys, d):
        e = 2 * lax.rem(cx + d, n_x) + half
        return (slots == keys[pl.ds(e, 1), :]).astype(F32).astype(BF16)

    own_x.wait()

    def own_rows(t, carry):
        d = lax.rem(t + 1, n_x)
        pick_rows = select(keyt, d)
        stage = h.at[pl.ds(pl.multiple_of(t * cap, 8), cap), pl.ds(0, d_model)]
        for j in range(n_j):
            got = jnp.dot(pick_rows, h[pl.ds(0, tok), pl.ds(d_model + j * xc, xc)], preferred_element_type=F32)
            h[pl.ds(pl.multiple_of(t * cap, 8), cap), pl.ds(j * xc, xc)] = got.astype(BF16)
        dst = xrows_ref.at[pl.ds(pl.multiple_of(cx * 2 * cap, 8), cap), :]

        @pl.when(t < n_x - 1)
        def _():
            remote(stage, dst, s_own.at[t], r_own, dev(lax.rem(cx + d, n_x), q, cc)).start()

        @pl.when(t == n_x - 1)
        def _():
            pltpu.make_async_copy(stage, dst, l_loc.at[n_j]).start()

        return carry

    lax.fori_loop(0, n_x, own_rows, 0)

    def start_own_pass(k, carry):
        @pl.when(lead)
        def _():
            send_own_gu(k, partner, s_a.at[k], r_gu.at[0, k])

        return carry

    lax.fori_loop(0, n_k, start_own_pass, 0)

    send_key.wait()

    def par_cols(j, carry):
        cols = pl.ds(pl.multiple_of(j * xc, 128), xc)
        wait_for(xpar_ref.at[:, cols], r_x.at[j])
        here = pl.ds(pl.multiple_of(d_model + j * xc, 128), xc)
        load = pltpu.make_async_copy(xpar_ref.at[:, cols], h.at[pl.ds(tok, tok), here], l_x.at[1])
        load.start()
        load.wait()

        def par_rows(t, carry2):
            d = lax.rem(t + 1, n_x)
            r0 = pl.multiple_of((n_x + t) * cap, 8)
            got = jnp.dot(select(keyt_par, d), h[pl.ds(tok, tok), here], preferred_element_type=F32)
            h[pl.ds(r0, cap), cols] = got.astype(BF16)
            stage = h.at[pl.ds(r0, cap), cols]
            dst = xrows_ref.at[pl.ds(pl.multiple_of((cx * 2 + 1) * cap, 8), cap), cols]

            @pl.when(t < n_x - 1)
            def _():
                remote(stage, dst, s_par.at[t, j], r_par, dev(lax.rem(cx + d, n_x), q, cc)).start()

            @pl.when(t == n_x - 1)
            def _():
                pltpu.make_async_copy(stage, dst, l_loc.at[j]).start()

            return carry2

        return lax.fori_loop(0, n_x, par_rows, carry)

    lax.fori_loop(0, n_j, par_cols, 0)

    def ahead(k):
        @pl.when(lead)
        def _():
            wait_for(gu_rows(k, 2), r_gu.at[2, k])
            pass_gu(k, 2, partner, s_b.at[k], 2)

        @pl.when(jnp.logical_not(lead))
        def _():
            wait_for(gu_rows(k, 1), r_gu.at[1, k])
            pass_gu(k, 1, inner_dev, s_a.at[k], 3)
            pass_gu(k, 1, partner, s_b.at[k], 1)

    def wd_rows(i, m):
        return wdb_ref.at[quarter(i), pl.ds(pl.multiple_of(m * wk, 8), wk), :]

    def send_own_wd(m, device, send, recv):
        src = wd_ref.at[pl.ds(pl.multiple_of(m * wk, 8), wk), :]
        remote(src, wd_rows(0, m), send, recv, device).start()

    def phase_up(xr, wbuf):
        def gather_chunk(k, slot):
            @pl.when(lead)
            def _():
                wait_for(gu_rows(k, 1), r_gu.at[1, k])
                wait_for(gu_rows(k, 3), r_gu.at[3, k])
                src = pl.ds(pl.multiple_of(k * fc, 128), fc)
                for w_ref, c0 in ((wg_ref, 0), (wu_ref, fc)):
                    pltpu.make_async_copy(w_ref.at[:, src], wbuf.at[slot, pl.ds(q * d_q, d_q), pl.ds(c0, fc)], l_w.at[slot]).start()
                for i in (1, 2, 3):
                    pltpu.make_async_copy(gu_rows(k, i), wbuf.at[slot, pl.ds(quarter(i) * d_q, d_q), :], l_w.at[slot]).start()

            @pl.when(jnp.logical_not(lead))
            def _():
                wait_for(gu_rows(k, 3), r_gu.at[3, k])
                pass_gu(k, 3, partner, s_c.at[k], 3)
                wait_for(gu_rows(k, 0), r_gu.at[0, k])
                wait_for(gu_rows(k, 2), r_gu.at[2, k])
                pltpu.make_async_copy(gu_ref.at[k], wbuf.at[slot], l_w.at[slot]).start()

        for k in range(LEAD):
            ahead(k)

        wait_for(xrows_ref.at[pl.ds(0, (n_x - 1) * cap), :], r_own)
        wait_for(xrows_ref.at[pl.ds(0, (n_x - 1) * cap), :], r_par)
        wait_for(xrows_ref.at[pl.ds(0, cap), :], l_loc.at[n_j])
        for j in range(n_j):
            wait_for(xrows_ref.at[pl.ds(0, cap), pl.ds(0, xc)], l_loc.at[j])
        load = pltpu.make_async_copy(xrows_ref, xr, l_x.at[0])
        load.start()

        def drain(t, carry):
            wait_for(xrows_ref.at[pl.ds(0, cap), :], s_own.at[t])

            def inner_drain(j, carry2):
                wait_for(xrows_ref.at[pl.ds(0, cap), pl.ds(0, xc)], s_par.at[t, j])
                return carry2

            return lax.fori_loop(0, n_j, inner_drain, carry)

        lax.fori_loop(0, n_x - 1, drain, 0)
        for j in range(n_j):
            wait_for(xpar_ref.at[:, pl.ds(0, xc)], s_x.at[j])

        def start_wd(m, carry):
            @pl.when(jnp.logical_not(lead))
            def _():
                send_own_wd(m, outer_dev, t_main.at[m], r_wd.at[1, m])

            @pl.when(lead)
            def _():
                send_own_wd(m, partner, t_a.at[m], r_wd.at[0, m])

            return carry

        lax.fori_loop(0, n_w, start_wd, 0)
        gather_chunk(0, 0)
        load.wait()

        def step(k, carry):
            slot = lax.rem(k, 2)

            @pl.when(k + LEAD < n_k)
            def _():
                ahead(k + LEAD)

            @pl.when(jnp.logical_and(lead, jnp.logical_and(k >= 2, k - 2 + early < n_k)))
            def _():
                send_own_gu(k - 2 + early, inner_dev, s_main.at[k - 2 + early], r_gu.at[2, k - 2 + early])

            @pl.when(jnp.logical_and(k == min(DOWN_STEP, n_k - 1), lead))
            def _():
                def start_near(m, carry2):
                    send_own_wd(m, inner_dev, t_main.at[m], r_wd.at[2, m])
                    return carry2

                lax.fori_loop(0, n_w, start_near, 0)

            @pl.when(k + 1 < n_k)
            def _():
                gather_chunk(k + 1, lax.rem(k + 1, 2))

            wait_for(wbuf.at[slot], l_w.at[slot])

            def row_tile(r, carry2):
                r0 = pl.multiple_of(r * tile, 8)
                both = jnp.dot(xr[pl.ds(r0, tile), :], wbuf[slot], preferred_element_type=F32)
                act = jax.nn.silu(both[:, :fc]) * both[:, fc:]
                h[pl.ds(r0, tile), pl.ds(pl.multiple_of(k * fc, 128), fc)] = act.astype(BF16)
                return carry2

            lax.fori_loop(0, rows // tile, row_tile, 0)
            return carry

        lax.fori_loop(0, n_k, step, 0)

    def phase_down(wdv, stage, acc, cmat, backv):
        t_tile = min(512, tok)
        parts = 4 * n_w
        n_blocks = 2 * n_x

        def ret_dst(u):
            return back_ref.at[quarter(u // n_w), u % n_w, half, pl.ds(pl.multiple_of(cx * cap, 8), cap), :]

        def take(i, m):
            @pl.when(jnp.logical_not(jnp.logical_and(lead, i == 0)))
            def _():
                wait_for(wd_rows(i, m), r_wd.at[i, m])

                @pl.when(jnp.logical_and(lead, i == 2))
                def _():
                    remote(wd_rows(2, m), wd_rows(2, m), t_b.at[m], r_wd.at[2, m], partner).start()

                @pl.when(jnp.logical_and(jnp.logical_not(lead), i == 1))
                def _():
                    remote(wd_rows(1, m), wd_rows(1, m), t_b.at[m], r_wd.at[1, m], partner).start()

                @pl.when(jnp.logical_and(jnp.logical_not(lead), i == 3))
                def _():
                    remote(wd_rows(3, m), wd_rows(3, m), t_c.at[m], r_wd.at[3, m], partner).start()

        def load_part(u):
            i, m = u // n_w, u % n_w
            dst = wdv.at[lax.rem(u, 2)]
            sem = l_wd.at[lax.rem(u, 2)]

            @pl.when(jnp.logical_and(lead, i == 0))
            def _():
                pltpu.make_async_copy(wd_ref.at[pl.ds(pl.multiple_of(m * wk, 8), wk), :], dst, sem).start()

            @pl.when(jnp.logical_not(jnp.logical_and(lead, i == 0)))
            def _():
                pltpu.make_async_copy(wd_rows(i, m), dst, sem).start()

        def combine(qt, m, g, add, buf):
            def tok_tile(r, carry):
                r0 = pl.multiple_of(r * t_tile, 8)
                gates = gate_e[pl.ds(r0, t_tile), :]
                lanes = lax.broadcasted_iota(jnp.int32, (t_tile, 128), 1)
                total = None
                for x in range(n_x):
                    e = 2 * x + g
                    rows_x = jnp.dot(cmat[e, pl.ds(r0, t_tile), :], backv[buf, pl.ds(x * cap, cap), :], preferred_element_type=F32)
                    gate_x = jnp.sum(jnp.where(lanes == e, gates, 0.0), axis=1, keepdims=True)
                    total = gate_x * rows_x if total is None else total + gate_x * rows_x
                if add:
                    total = total + acc[qt * n_w + m, pl.ds(r0, t_tile), :]
                acc[qt * n_w + m, pl.ds(r0, t_tile), :] = total
                return carry

            lax.fori_loop(0, tok // t_tile, tok_tile, 0)

        def add_up(u):
            i, m = u // n_w, u % n_w
            here, there = quarter(i), 3 - quarter(i)
            wait_for(back_ref.at[0, 0, 0, pl.ds(0, (n_x - 1) * cap), :], r_back.at[here, m, half])
            first_load = pltpu.make_async_copy(back_ref.at[here, m, half], backv.at[0], l_back.at[0])
            first_load.start()
            wait_for(back_ref.at[0, 0, 0], r_back.at[there, m, 1 - half])
            second_load = pltpu.make_async_copy(back_ref.at[there, m, 1 - half], backv.at[1], l_back.at[1])
            second_load.start()

            def both(add):
                first_load.wait()
                combine(here, m, half, add, 0)
                second_load.wait()
                combine(there, m, 1 - half, add, 1)

            @pl.when(i % 2 == 0)
            def _():
                both(False)

            @pl.when(i % 2 == 1)
            def _():
                both(True)

        take(jnp.int32(0), jnp.int32(0))
        load_part(jnp.int32(0))

        slot_lane = lax.broadcasted_iota(jnp.int32, (tok, cap), 1).astype(F32)
        for e in range(2 * n_x):
            cmat[e] = (slot_lane == keyc[:, e:e + 1]).astype(F32).astype(BF16)

        def part(u, carry):
            i, m = u // n_w, u % n_w
            slot = lax.rem(u, LAG)

            @pl.when(u >= 2 * n_w)
            def _():
                take(i, m)
                load_part(u)

            @pl.when(u == 1)
            def _():
                each(n_w - 2, lambda k: take(jnp.int32(0), k + 2))

                @pl.when(jnp.logical_not(lead))
                def _():
                    each(n_w, lambda k: take(jnp.int32(1), k))

            @pl.when(jnp.logical_and(u == n_w - 1, lead))
            def _():
                each(n_w, lambda k: take(jnp.int32(1), k))

            @pl.when(jnp.logical_and(u == n_w + 1, jnp.logical_not(lead)))
            def _():
                each(n_w, lambda k: remote(wd_rows(1, k), wd_rows(1, k), t_a.at[k], r_wd.at[3, k], inner_dev).start())

            @pl.when(jnp.logical_and(u >= 1, u + 1 < 2 * n_w))
            def _():
                load_part(u + 1)

            wait_for(wdv.at[0], l_wd.at[lax.rem(u, 2)])

            def block(t, carry2):
                s = (t // n_x + 1 - cc) % 2
                x_src = lax.rem(cx + 1 + t % n_x, n_x)
                r0 = pl.multiple_of((x_src * 2 + s) * cap, 8)
                out = lax.dot_general(h[pl.ds(r0, cap), :], wdv[lax.rem(u, 2)], (((1,), (1,)), ((), ())), preferred_element_type=F32)

                @pl.when(u >= LAG)
                def _():
                    wait_for(stage.at[0, 0], s_ret.at[slot, t])

                stage[slot, t] = out.astype(BF16)
                local = jnp.logical_and(s == 0, t % n_x == n_x - 1)

                @pl.when(jnp.logical_not(local))
                def _():
                    remote(stage.at[slot, t], ret_dst(u), s_ret.at[slot, t], r_back.at[quarter(i), m, half], dev(x_src, q + s * (outer - q), cc)).start()

                @pl.when(local)
                def _():
                    pltpu.make_async_copy(stage.at[slot, t], ret_dst(u), s_ret.at[slot, t]).start()

                return carry2

            lax.fori_loop(0, n_blocks, block, 0)

            @pl.when(u == 0)
            def _():
                take(0, jnp.int32(1))
                load_part(jnp.int32(1))

            @pl.when(u >= LAG)
            def _():
                add_up(u - LAG)

            return carry

        lax.fori_loop(0, parts, part, 0)

        x_here = h.at[pl.ds(0, tok), pl.ds(0, d_model)]
        load = pltpu.make_async_copy(x_ref, x_here, l_x.at[0])
        load.start()

        def rest(k):
            u = parts - LAG + k
            each(n_blocks, lambda t: wait_for(stage.at[0, 0], s_ret.at[lax.rem(u, LAG), t]))
            add_up(u)

        each(LAG, rest)
        load.wait()

        def finish(r, carry):
            r0 = pl.multiple_of(r * t_tile, 8)
            for c in range(4 * n_w):
                cols = pl.ds(c * wk, wk)
                total = h[pl.ds(r0, t_tile), cols].astype(F32) + acc[c, pl.ds(r0, t_tile), :]
                h[pl.ds(r0, t_tile), cols] = total.astype(BF16)
            return carry

        lax.fori_loop(0, tok // t_tile, finish, 0)
        store = pltpu.make_async_copy(x_here, y_ref, l_x.at[0])
        store.start()
        store.wait()

    pl.run_scoped(phase_up, pltpu.VMEM((rows, d_model), BF16), pltpu.VMEM((2, d_model, 2 * fc), BF16))
    pl.run_scoped(
        phase_down,
        pltpu.VMEM((2, wk, ffn), BF16),
        pltpu.VMEM((LAG, 2 * n_x, cap, wk), BF16),
        pltpu.VMEM((4 * n_w, tok, wk), F32),
        pltpu.VMEM((2 * n_x, tok, cap), BF16),
        pltpu.VMEM((2, n_x * cap, wk), BF16),
    )

    def drain_gu(k, carry):
        wait_for(gu_rows(k, 0), s_main.at[k])
        wait_for(gu_rows(k, 0), s_a.at[k])
        wait_for(gu_rows(k, 0), s_b.at[k])

        @pl.when(jnp.logical_not(lead))
        def _():
            wait_for(gu_rows(k, 0), s_c.at[k])

        return carry

    lax.fori_loop(0, n_k, drain_gu, 0)

    def drain_wd(m, carry):
        wait_for(wd_rows(0, m), t_main.at[m])
        wait_for(wd_rows(0, m), t_a.at[m])
        wait_for(wd_rows(0, m), t_b.at[m])

        @pl.when(jnp.logical_not(lead))
        def _():
            wait_for(wd_rows(0, m), t_c.at[m])

        return carry

    lax.fori_loop(0, n_w, drain_wd, 0)


def solution(mesh):
    n_group, n_y = mesh.shape["expert"], mesh.shape["data"]
    assert n_y == 4 and n_group % 2 == 0
    n_x = n_group // 2
    tok_spec = P(("rep", "expert", "data"), None)
    wide_spec = P("expert", "data", None)
    down_spec = P("expert", None, "data")

    def device_step(x_loc, idx_loc, gate_loc, wg_loc, wu_loc, wd_loc):
        tok, d_model = x_loc.shape
        n_local, d_q, ffn = wg_loc.shape
        assert n_local == 1 and n_group == 8
        cap = capacity_rows(tok, idx_loc.shape[1], n_group)
        fc = pick(ffn, (384, 256, 128))
        n_k, n_w, n_j = ffn // fc, pick(d_q // 8, (3, 2, 1)), pick(d_model // 128, (3, 2, 1))
        rows = 2 * n_x * cap
        tile = pick(rows, (640, 48, 8))
        dims = (n_x, tok, d_model, d_q, ffn, cap, fc, n_k, n_w, n_j, tile)
        hbm = pl.BlockSpec(memory_space=pl.ANY)
        vmem = pl.BlockSpec(memory_space=pltpu.VMEM)
        dma = pltpu.SemaphoreType.DMA
        shape = jax.ShapeDtypeStruct
        outs = pl.pallas_call(
            functools.partial(moe_kernel, dims),
            name="moe_layer",
            out_shape=[
                shape((tok, d_model), BF16),
                shape((tok, d_model), BF16),
                shape((rows, d_model), BF16),
                shape((n_k, d_model, 2 * fc), BF16),
                shape((4, d_q, ffn), BF16),
                shape((4, n_w, 2, n_x * cap, d_q // n_w), BF16),
            ],
            in_specs=[vmem, vmem, hbm, hbm, hbm, hbm],
            out_specs=[hbm] * 6,
            scratch_shapes=[
                pltpu.VMEM((rows, ffn), BF16),
                pltpu.VMEM((8, tok), F32),
                pltpu.VMEM((8, tok), F32),
                pltpu.VMEM((tok, 128), F32),
                pltpu.VMEM((tok, 128), F32),
                dma((n_j + 1,)), dma((n_j + 1,)), dma((n_x - 1,)), dma, dma((n_x - 1, n_j)), dma, dma((n_j + 1,)), dma((2,)),
                dma((n_k,)), dma((n_k,)), dma((n_k,)), dma((n_k,)), dma((4, n_k)), dma((2,)),
                dma((n_w,)), dma((n_w,)), dma((n_w,)), dma((n_w,)), dma((4, n_w)), dma((2,)),
                dma((LAG, 2 * n_x)), dma((4, n_w, 2)), dma((2,)),
            ],
            compiler_params=pltpu.CompilerParams(collective_id=0, has_side_effects=True, vmem_limit_bytes=67_043_328),
        )(idx_loc.T, gate_loc.T, x_loc, wg_loc.reshape(d_q, ffn), wu_loc.reshape(d_q, ffn), wd_loc.reshape(ffn, d_q).T)
        return outs[0]

    return jax.shard_map(device_step, mesh=mesh, in_specs=(tok_spec, tok_spec, tok_spec, wide_spec, wide_spec, down_spec), out_specs=tok_spec, check_vma=False)
```

```python
import functools

import jax
import jax.numpy as jnp
from jax import lax
from jax.experimental import pallas as pl
from jax.experimental.pallas import tpu as pltpu
from jax.sharding import PartitionSpec as P

MESH = pl.DeviceIdType.MESH
F32 = jnp.float32
BF16 = jnp.bfloat16
LEAD_FIRST = 3
LEAD = 5
EARLY = 13
LATE_STEP = 4
DOWN_STEP = 12
STAGES = 3


def capacity_rows(tok_rows, top_k, n_exp):
    return max(8, ((5 * top_k * tok_rows) // (4 * n_exp) + 7) // 8 * 8)


def pick(total, options):
    return next(c for c in options if total % c == 0)


def moe_kernel(dims, idx_ref, gate_ref, x_ref, wg_ref, wu_ref, wd_ref, y_ref, xpar_ref, xrows_ref, gu_ref, wdb_ref, back_ref,
               h, keyt, keyt_par, keyc, gate_e,
               s_x, r_x, s_own, r_own, s_par, r_par, l_loc, l_x,
               s_main, s_a, s_b, s_c, r_gu, l_w,
               t_main, t_a, t_b, t_c, r_wd, l_wd, s_ret, l_ret, r_back, l_back):
    n_x, tok, d_model, d_q, ffn, cap, fc, n_k, n_j, tile = dims
    rows = 2 * n_x * cap
    wk = d_q // 9 * 4
    rest = d_q - 2 * wk
    xc = d_model // n_j
    p = lax.axis_index("expert")
    q = lax.axis_index("data")
    cx, cc = p // 2, p % 2
    half = q // 2
    inner = q + 1 - 2 * (q % 2)
    outer = 3 - q
    lead = cc == half

    def dev(x, y, c):
        return {"expert": 2 * x + c, "data": y}

    def quarter(i):
        base = q + (i // 2) * (inner - q)
        return base + (i % 2) * (3 - 2 * base)

    partner = dev(cx, q, 1 - cc)
    inner_dev = dev(cx, inner, cc)
    outer_dev = dev(cx, outer, 1 - cc)
    mirror = dev(cx, outer, cc)

    def remote(src, dst, send, recv, device):
        return pltpu.make_async_remote_copy(src_ref=src, dst_ref=dst, send_sem=send, recv_sem=recv, device_id=device, device_id_type=MESH)

    def wait_for(ref, sem):
        pltpu.make_async_copy(ref, ref, sem).wait()

    barrier = pltpu.get_barrier_semaphore()
    peers = [partner, inner_dev, outer_dev]
    peers += [dev((cx + d) % n_x, q, cc) for d in range(1, n_x)]
    peers += [dev((cx + d) % n_x, outer, cc) for d in range(n_x)]
    for peer in peers:
        pl.semaphore_signal(barrier, inc=1, device_id=peer, device_id_type=MESH)
    pl.semaphore_wait(barrier, len(peers))

    def gu_rows(k, i):
        return gu_ref.at[k, pl.ds(quarter(i) * d_q, d_q), :]

    def send_own_gu(k, device, send, recv):
        src = pl.ds(pl.multiple_of(k * fc, 128), fc)
        for w_ref, c0 in ((wg_ref, 0), (wu_ref, fc)):
            remote(w_ref.at[:, src], gu_ref.at[k, pl.ds(q * d_q, d_q), pl.ds(c0, fc)], send, recv, device).start()

    def pass_gu(k, i, device, send, i_there):
        remote(gu_rows(k, i), gu_rows(k, i), send, r_gu.at[i_there, k], device).start()

    def send_block(j):
        cols = pl.ds(j * xc, xc)
        remote(x_ref.at[:, cols], xpar_ref.at[:, cols], s_x.at[j], r_x.at[j], mirror).start()

    def each(count, body):
        lax.fori_loop(0, count, lambda k, carry: (body(k), carry)[1], 0)

    send_block(0)
    early = min(EARLY, n_k)

    @pl.when(lead)
    def _():
        each(early, lambda k: send_own_gu(k, inner_dev, s_main.at[k], r_gu.at[2, k]))

    own_x = pltpu.make_async_copy(x_ref, h.at[pl.ds(0, tok), pl.ds(d_model, d_model)], l_x.at[0])
    own_x.start()
    expert = lax.broadcasted_iota(jnp.int32, (128, tok), 0)
    first = expert == idx_ref[0:1, :]
    second = expert == idx_ref[1:2, :]
    chosen = jnp.logical_or(first, second)
    before = lax.broadcasted_iota(jnp.int32, (tok, tok), 0) < lax.broadcasted_iota(jnp.int32, (tok, tok), 1)
    slot = jnp.dot(chosen.astype(F32).astype(BF16), before.astype(F32).astype(BF16), preferred_element_type=F32)
    key = jnp.where(jnp.logical_and(chosen, slot < cap), slot, -1.0)
    keyt[...] = key[:8, :]
    keyc[...] = key.T
    gate_e[...] = (jnp.where(first, gate_ref[0:1, :], 0.0) + jnp.where(second, gate_ref[1:2, :], 0.0)).T
    send_key = remote(keyt, keyt_par, s_x.at[n_j], r_x.at[n_j], mirror)
    send_key.start()
    for j in range(1, n_j):
        send_block(j)

    @pl.when(jnp.logical_not(lead))
    def _():
        each(n_k, lambda k: send_own_gu(k, outer_dev, s_main.at[k], r_gu.at[1, k]))


    slots = lax.broadcasted_iota(jnp.int32, (cap, tok), 0).astype(F32)

    def select(keys, d):
        e = 2 * lax.rem(cx + d, n_x) + half
        return (slots == keys[pl.ds(e, 1), :]).astype(F32).astype(BF16)

    own_x.wait()

    def own_rows(t, carry):
        d = lax.rem(t + 1, n_x)
        pick_rows = select(keyt, d)
        stage = h.at[pl.ds(pl.multiple_of(t * cap, 8), cap), pl.ds(0, d_model)]
        for j in range(n_j):
            got = jnp.dot(pick_rows, h[pl.ds(0, tok), pl.ds(d_model + j * xc, xc)], preferred_element_type=F32)
            h[pl.ds(pl.multiple_of(t * cap, 8), cap), pl.ds(j * xc, xc)] = got.astype(BF16)
        dst = xrows_ref.at[pl.ds(pl.multiple_of(cx * 2 * cap, 8), cap), :]

        @pl.when(t < n_x - 1)
        def _():
            remote(stage, dst, s_own.at[t], r_own, dev(lax.rem(cx + d, n_x), q, cc)).start()

        @pl.when(t == n_x - 1)
        def _():
            pltpu.make_async_copy(stage, dst, l_loc.at[n_j]).start()

        return carry

    lax.fori_loop(0, n_x, own_rows, 0)

    def start_own_pass(k, carry):
        @pl.when(lead)
        def _():
            send_own_gu(k, partner, s_a.at[k], r_gu.at[0, k])

        return carry

    lax.fori_loop(0, n_k, start_own_pass, 0)

    send_key.wait()

    def par_cols(j, carry):
        cols = pl.ds(pl.multiple_of(j * xc, 128), xc)
        wait_for(xpar_ref.at[:, cols], r_x.at[j])
        here = pl.ds(pl.multiple_of(d_model + j * xc, 128), xc)
        load = pltpu.make_async_copy(xpar_ref.at[:, cols], h.at[pl.ds(tok, tok), here], l_x.at[1])
        load.start()
        load.wait()

        def par_rows(t, carry2):
            d = lax.rem(t + 1, n_x)
            r0 = pl.multiple_of((n_x + t) * cap, 8)
            got = jnp.dot(select(keyt_par, d), h[pl.ds(tok, tok), here], preferred_element_type=F32)
            h[pl.ds(r0, cap), cols] = got.astype(BF16)
            stage = h.at[pl.ds(r0, cap), cols]
            dst = xrows_ref.at[pl.ds(pl.multiple_of((cx * 2 + 1) * cap, 8), cap), cols]

            @pl.when(t < n_x - 1)
            def _():
                remote(stage, dst, s_par.at[t, j], r_par, dev(lax.rem(cx + d, n_x), q, cc)).start()

            @pl.when(t == n_x - 1)
            def _():
                pltpu.make_async_copy(stage, dst, l_loc.at[j]).start()

            return carry2

        return lax.fori_loop(0, n_x, par_rows, carry)

    lax.fori_loop(0, n_j, par_cols, 0)

    def ahead(k):
        @pl.when(lead)
        def _():
            wait_for(gu_rows(k, 2), r_gu.at[2, k])
            pass_gu(k, 2, partner, s_b.at[k], 2)

        @pl.when(jnp.logical_not(lead))
        def _():
            wait_for(gu_rows(k, 1), r_gu.at[1, k])
            pass_gu(k, 1, inner_dev, s_a.at[k], 3)
            pass_gu(k, 1, partner, s_b.at[k], 1)

    def part_rows(m):
        return pl.ds(2 * wk, d_q - 2 * wk) if isinstance(m, int) and m == 2 else pl.ds(m * wk if isinstance(m, int) else pl.multiple_of(m * wk, 8), wk)

    def wd_rows(i, m):
        return wdb_ref.at[quarter(i), part_rows(m), :]

    def send_own_wd(m, device, send, recv):
        remote(wd_ref.at[part_rows(m), :], wd_rows(0, m), send, recv, device).start()

    def phase_up(xr, wbuf):
        def gather_chunk(k, slot):
            @pl.when(lead)
            def _():
                wait_for(gu_rows(k, 1), r_gu.at[1, k])
                wait_for(gu_rows(k, 3), r_gu.at[3, k])
                src = pl.ds(pl.multiple_of(k * fc, 128), fc)
                for w_ref, c0 in ((wg_ref, 0), (wu_ref, fc)):
                    pltpu.make_async_copy(w_ref.at[:, src], wbuf.at[slot, pl.ds(q * d_q, d_q), pl.ds(c0, fc)], l_w.at[slot]).start()
                for i in (1, 2, 3):
                    pltpu.make_async_copy(gu_rows(k, i), wbuf.at[slot, pl.ds(quarter(i) * d_q, d_q), :], l_w.at[slot]).start()

            @pl.when(jnp.logical_not(lead))
            def _():
                wait_for(gu_rows(k, 3), r_gu.at[3, k])
                pass_gu(k, 3, partner, s_c.at[k], 3)
                wait_for(gu_rows(k, 0), r_gu.at[0, k])
                wait_for(gu_rows(k, 2), r_gu.at[2, k])
                pltpu.make_async_copy(gu_ref.at[k], wbuf.at[slot], l_w.at[slot]).start()

        for k in range(min(LEAD_FIRST, n_k)):
            ahead(k)

        wait_for(xrows_ref.at[pl.ds(0, (n_x - 1) * cap), :], r_own)
        wait_for(xrows_ref.at[pl.ds(0, (n_x - 1) * cap), :], r_par)
        wait_for(xrows_ref.at[pl.ds(0, cap), :], l_loc.at[n_j])
        for j in range(n_j):
            wait_for(xrows_ref.at[pl.ds(0, cap), pl.ds(0, xc)], l_loc.at[j])
        load = pltpu.make_async_copy(xrows_ref, xr, l_x.at[0])
        load.start()

        def drain(t, carry):
            wait_for(xrows_ref.at[pl.ds(0, cap), :], s_own.at[t])

            def inner_drain(j, carry2):
                wait_for(xrows_ref.at[pl.ds(0, cap), pl.ds(0, xc)], s_par.at[t, j])
                return carry2

            return lax.fori_loop(0, n_j, inner_drain, carry)

        lax.fori_loop(0, n_x - 1, drain, 0)
        for j in range(n_j):
            wait_for(xpar_ref.at[:, pl.ds(0, xc)], s_x.at[j])

        @pl.when(lead)
        def _():
            for m in range(3):
                send_own_wd(m, partner, t_a.at[m], r_wd.at[0, m])

        @pl.when(jnp.logical_not(lead))
        def _():
            for m in range(3):
                send_own_wd(m, outer_dev, t_main.at[m], r_wd.at[1, m])

        gather_chunk(0, 0)
        for k in range(min(LEAD_FIRST, n_k), min(LEAD, n_k)):
            ahead(k)
        load.wait()

        def step(k, carry):
            slot = lax.rem(k, 2)

            @pl.when(k + LEAD < n_k)
            def _():
                ahead(k + LEAD)

            late = k - min(LATE_STEP, n_k - 1) + early

            @pl.when(jnp.logical_and(lead, jnp.logical_and(late >= early, late < n_k)))
            def _():
                send_own_gu(late, inner_dev, s_main.at[late], r_gu.at[2, late])

            @pl.when(jnp.logical_and(k == min(DOWN_STEP, n_k - 1), lead))
            def _():
                for m in range(3):
                    send_own_wd(m, inner_dev, t_main.at[m], r_wd.at[2, m])

            @pl.when(k + 1 < n_k)
            def _():
                gather_chunk(k + 1, lax.rem(k + 1, 2))

            wait_for(wbuf.at[slot], l_w.at[slot])

            def row_tile(r, carry2):
                r0 = pl.multiple_of(r * tile, 8)
                both = jnp.dot(xr[pl.ds(r0, tile), :], wbuf[slot], preferred_element_type=F32)
                act = jax.nn.silu(both[:, :fc]) * both[:, fc:]
                h[pl.ds(r0, tile), pl.ds(pl.multiple_of(k * fc, 128), fc)] = act.astype(BF16)
                return carry2

            lax.fori_loop(0, rows // tile, row_tile, 0)
            return carry

        lax.fori_loop(0, n_k, step, 0)

    def phase_down(wdv, stage, acc, cmat, backv):
        t_tile = min(512, tok)
        n_blocks = 2 * n_x
        last = 8

        def chunk(u, other):
            qt = quarter(u // 2)
            return (1 - u // last) * (2 * (qt + other * (3 - 2 * qt)) + u % 2) + u // last * last

        def take(i, m):
            @pl.when(jnp.logical_not(jnp.logical_and(lead, i == 0)))
            def _():
                wait_for(wd_rows(i, m), r_wd.at[i, m])

                @pl.when(jnp.logical_and(lead, i == 2))
                def _():
                    remote(wd_rows(i, m), wd_rows(i, m), t_b.at[m], r_wd.at[i, m], partner).start()

                @pl.when(jnp.logical_and(jnp.logical_not(lead), i == 1))
                def _():
                    remote(wd_rows(i, m), wd_rows(i, m), t_b.at[m], r_wd.at[i, m], partner).start()

                @pl.when(jnp.logical_and(jnp.logical_not(lead), i == 3))
                def _():
                    remote(wd_rows(i, m), wd_rows(i, m), t_c.at[m], r_wd.at[i, m], partner).start()

        def load(i, m, dst, sem):
            @pl.when(jnp.logical_and(lead, i == 0))
            def _():
                pltpu.make_async_copy(wd_ref.at[part_rows(m), :], dst, sem).start()

            @pl.when(jnp.logical_not(jnp.logical_and(lead, i == 0)))
            def _():
                pltpu.make_async_copy(wd_rows(i, m), dst, sem).start()

        def load_main(u):
            load(u // 2, u % 2, wdv.at[u % 2], l_wd.at[u % 2])

        def load_rest(i):
            load(i, 2, wdv.at[2, pl.ds(pl.multiple_of(quarter(i) * rest, 8), rest), :], l_wd.at[2])

        def combine(c, g, add, buf):
            def tok_tile(r, carry):
                r0 = pl.multiple_of(r * t_tile, 8)
                gates = gate_e[pl.ds(r0, t_tile), :]
                lanes = lax.broadcasted_iota(jnp.int32, (t_tile, 128), 1)
                total = None
                for x in range(n_x):
                    e = 2 * x + g
                    rows_x = jnp.dot(cmat[e, pl.ds(r0, t_tile), :], backv[buf, pl.ds(x * cap, cap), :], preferred_element_type=F32)
                    gate_x = jnp.sum(jnp.where(lanes == e, gates, 0.0), axis=1, keepdims=True)
                    total = gate_x * rows_x if total is None else total + gate_x * rows_x
                if add:
                    total = total + acc[c, pl.ds(r0, t_tile), :]
                acc[c, pl.ds(r0, t_tile), :] = total
                return carry

            lax.fori_loop(0, tok // t_tile, tok_tile, 0)

        def add_up(u):
            here, there = chunk(u, 0), chunk(u, 1)
            wait_for(stage.at[0, 0], l_ret.at[lax.rem(u, STAGES)])
            wait_for(back_ref.at[0, 0, pl.ds(0, (n_x - 1) * cap), :], r_back.at[here, half])
            first_load = pltpu.make_async_copy(back_ref.at[here, half], backv.at[0], l_back.at[0])
            first_load.start()
            wait_for(back_ref.at[0, 0], r_back.at[there, 1 - half])
            second_load = pltpu.make_async_copy(back_ref.at[there, 1 - half], backv.at[1], l_back.at[1])
            second_load.start()

            def both(add_first, add_second):
                first_load.wait()
                combine(here, half, add_first, 0)
                second_load.wait()
                combine(there, 1 - half, add_second, 1)

            @pl.when(jnp.logical_and(u < last, u // 2 % 2 == 0))
            def _():
                both(False, False)

            @pl.when(jnp.logical_and(u < last, u // 2 % 2 == 1))
            def _():
                both(True, True)

            @pl.when(u == last)
            def _():
                both(False, True)

        slot_lane = lax.broadcasted_iota(jnp.int32, (tok, cap), 1).astype(F32)
        for e in range(2 * n_x):
            cmat[e] = (slot_lane == keyc[:, e:e + 1]).astype(F32).astype(BF16)

        take(0, 0)
        load_main(0)

        def part(u, carry):
            slot = lax.rem(u, STAGES)
            buf = (1 - u // last) * (u % 2) + u // last * 2

            @pl.when(jnp.logical_and(u >= 4, u < last))
            def _():
                take(u // 2, u % 2)
                load_main(u)

            @pl.when(u == 0)
            def _():
                take(0, 1)
                load_main(u + 1)
                take(0, 2)
                load_rest(0)

            @pl.when(jnp.logical_and(u == 1, jnp.logical_not(lead)))
            def _():
                for m in range(3):
                    take(1, m)
                for m in range(3):
                    remote(wd_rows(1, m), wd_rows(1, m), t_a.at[m], r_wd.at[3, m], inner_dev).start()

            @pl.when(jnp.logical_and(u == 1, lead))
            def _():
                for m in range(3):
                    take(1, m)

            @pl.when(jnp.logical_and(u >= 1, u <= 2))
            def _():
                load_main(u + 1)

            @pl.when(u == 2)
            def _():
                load_rest(1)

            @pl.when(u == 6)
            def _():
                take(2, 2)
                load_rest(2)

            @pl.when(u < last)
            def _():
                wait_for(wdv.at[0], l_wd.at[u % 2])

            @pl.when(u == last)
            def _():
                load_rest(3)
                wait_for(wdv.at[2], l_wd.at[2])

            def block(t, carry2):
                s = (t // n_x + 1 - cc) % 2
                x_src = lax.rem(cx + 1 + t % n_x, n_x)
                r0 = pl.multiple_of((x_src * 2 + s) * cap, 8)
                local = jnp.logical_and(s == 0, t % n_x == n_x - 1)

                @pl.when(jnp.logical_and(u == last - 1, t == n_x))
                def _():
                    take(3, 2)

                out = lax.dot_general(h[pl.ds(r0, cap), :], wdv[buf], (((1,), (1,)), ((), ())), preferred_element_type=F32)

                @pl.when(jnp.logical_and(u >= STAGES, jnp.logical_not(local)))
                def _():
                    wait_for(stage.at[0, 0], s_ret.at[slot, t])

                stage[slot, t] = out.astype(BF16)
                dst = back_ref.at[chunk(u, 0), half, pl.ds(pl.multiple_of(cx * cap, 8), cap), :]

                @pl.when(jnp.logical_not(local))
                def _():
                    remote(stage.at[slot, t], dst, s_ret.at[slot, t], r_back.at[chunk(u, 0), half], dev(x_src, q + s * (outer - q), cc)).start()

                @pl.when(local)
                def _():
                    pltpu.make_async_copy(stage.at[slot, t], dst, l_ret.at[slot]).start()

                return carry2

            lax.fori_loop(0, n_blocks, block, 0)

            def adds(v, carry2):
                add_up(v)
                return carry2

            @pl.when(jnp.logical_and(u >= 2, u < last - 1))
            def _():
                lax.fori_loop(u - 2, u - 1 + u // 6, adds, 0)

            return carry

        lax.fori_loop(0, last + 1, part, 0)

        x_here = h.at[pl.ds(0, tok), pl.ds(0, d_model)]
        x_load = pltpu.make_async_copy(x_ref, x_here, l_x.at[0])
        x_load.start()
        each(last - 5, lambda k: add_up(k + 6))
        x_load.wait()

        def finish(r, carry):
            r0 = pl.multiple_of(r * t_tile, 8)

            def put(c0, width, extra):
                cols = pl.ds(c0, width)
                h[pl.ds(r0, t_tile), cols] = (h[pl.ds(r0, t_tile), cols].astype(F32) + extra).astype(BF16)

            for qt in range(4):
                for m in range(2):
                    put(qt * d_q + m * wk, wk, acc[2 * qt + m, pl.ds(r0, t_tile), :])
                put(qt * d_q + 2 * wk, rest, acc[last, pl.ds(r0, t_tile), pl.ds(qt * rest, rest)])
            return carry

        lax.fori_loop(0, tok // t_tile, finish, 0)
        store = pltpu.make_async_copy(x_here, y_ref, l_x.at[0])
        store.start()

        def sent(k, carry):
            u = last - STAGES + 1 + k

            def sent_block(t, carry2):
                s = (t // n_x + 1 - cc) % 2

                @pl.when(jnp.logical_not(jnp.logical_and(s == 0, t % n_x == n_x - 1)))
                def _():
                    wait_for(stage.at[0, 0], s_ret.at[lax.rem(u, STAGES), t])

                return carry2

            return lax.fori_loop(0, n_blocks, sent_block, carry)

        lax.fori_loop(0, STAGES, sent, 0)
        store.wait()

    pl.run_scoped(phase_up, pltpu.VMEM((rows, d_model), BF16), pltpu.VMEM((2, d_model, 2 * fc), BF16))
    pl.run_scoped(
        phase_down,
        pltpu.VMEM((3, wk, ffn), BF16),
        pltpu.VMEM((STAGES, 2 * n_x, cap, wk), BF16),
        pltpu.VMEM((9, tok, wk), F32),
        pltpu.VMEM((2 * n_x, tok, cap), BF16),
        pltpu.VMEM((2, n_x * cap, wk), BF16),
    )

    def drain_gu(k, carry):
        wait_for(gu_rows(k, 0), s_main.at[k])
        wait_for(gu_rows(k, 0), s_a.at[k])
        wait_for(gu_rows(k, 0), s_b.at[k])

        @pl.when(jnp.logical_not(lead))
        def _():
            wait_for(gu_rows(k, 0), s_c.at[k])

        return carry

    lax.fori_loop(0, n_k, drain_gu, 0)

    for m in range(3):
        for sem in (t_main, t_a, t_b):
            wait_for(wd_rows(0, m), sem.at[m])

    @pl.when(jnp.logical_not(lead))
    def _():
        for m in range(3):
            wait_for(wd_rows(0, m), t_c.at[m])


def solution(mesh):
    n_group, n_y = mesh.shape["expert"], mesh.shape["data"]
    assert n_y == 4 and n_group % 2 == 0
    n_x = n_group // 2
    tok_spec = P(("rep", "expert", "data"), None)
    wide_spec = P("expert", "data", None)
    down_spec = P("expert", None, "data")

    def device_step(x_loc, idx_loc, gate_loc, wg_loc, wu_loc, wd_loc):
        tok, d_model = x_loc.shape
        n_local, d_q, ffn = wg_loc.shape
        assert n_local == 1 and n_group == 8 and d_q % 72 == 0
        cap = capacity_rows(tok, idx_loc.shape[1], n_group)
        fc = pick(ffn, (384, 256, 128))
        n_k, n_j = ffn // fc, pick(d_model // 128, (3, 2, 1))
        rows = 2 * n_x * cap
        tile = pick(rows, (640, 48, 8))
        dims = (n_x, tok, d_model, d_q, ffn, cap, fc, n_k, n_j, tile)
        hbm = pl.BlockSpec(memory_space=pl.ANY)
        vmem = pl.BlockSpec(memory_space=pltpu.VMEM)
        dma = pltpu.SemaphoreType.DMA
        shape = jax.ShapeDtypeStruct
        outs = pl.pallas_call(
            functools.partial(moe_kernel, dims),
            name="moe_layer",
            out_shape=[
                shape((tok, d_model), BF16),
                shape((tok, d_model), BF16),
                shape((rows, d_model), BF16),
                shape((n_k, d_model, 2 * fc), BF16),
                shape((4, d_q, ffn), BF16),
                shape((9, 2, n_x * cap, d_q // 9 * 4), BF16),
            ],
            in_specs=[vmem, vmem, hbm, hbm, hbm, hbm],
            out_specs=[hbm] * 6,
            scratch_shapes=[
                pltpu.VMEM((rows, ffn), BF16),
                pltpu.VMEM((8, tok), F32),
                pltpu.VMEM((8, tok), F32),
                pltpu.VMEM((tok, 128), F32),
                pltpu.VMEM((tok, 128), F32),
                dma((n_j + 1,)), dma((n_j + 1,)), dma((n_x - 1,)), dma, dma((n_x - 1, n_j)), dma, dma((n_j + 1,)), dma((2,)),
                dma((n_k,)), dma((n_k,)), dma((n_k,)), dma((n_k,)), dma((4, n_k)), dma((2,)),
                dma((3,)), dma((3,)), dma((3,)), dma((3,)), dma((4, 3)), dma((3,)),
                dma((STAGES, 2 * n_x)), dma((STAGES,)), dma((9, 2)), dma((2,)),
            ],
            compiler_params=pltpu.CompilerParams(collective_id=0, has_side_effects=True, vmem_limit_bytes=67_043_328),
        )(idx_loc.T, gate_loc.T, x_loc, wg_loc.reshape(d_q, ffn), wu_loc.reshape(d_q, ffn), wd_loc.reshape(ffn, d_q).T)
        return outs[0]

    return jax.shard_map(device_step, mesh=mesh, in_specs=(tok_spec, tok_spec, tok_spec, wide_spec, wide_spec, down_spec), out_specs=tok_spec, check_vma=False)
```

```python
import functools

import jax
import jax.numpy as jnp
from jax import lax
from jax.experimental import pallas as pl
from jax.experimental.pallas import tpu as pltpu
from jax.sharding import PartitionSpec as P

MESH = pl.DeviceIdType.MESH
F32 = jnp.float32
BF16 = jnp.bfloat16
LEAD = 2
EARLY = 13
LATE_STEP = 9
DOWN_STEP = 13
STAGES = 3


def capacity_rows(tok_rows, top_k, n_exp):
    return max(8, ((5 * top_k * tok_rows) // (4 * n_exp) + 7) // 8 * 8)


def pick(total, options):
    return next(c for c in options if total % c == 0)


def moe_kernel(dims, idx_ref, gate_ref, x_ref, wg_ref, wu_ref, wd_ref, y_ref, xpar_ref, xrows_ref, gu_ref, wdb_ref, back_ref, end_ref,
               h, keyt, keyt_par, tok_keys,
               s_x, r_x, s_own, r_own, s_par, r_par, l_loc, l_x,
               s_main, s_a, s_b, s_c, r_gu, l_w,
               t_main, t_a, t_b, t_c, r_wd, l_wd, s_ret, l_ret, r_back, r_end, l_back):
    n_x, tok, d_model, d_q, ffn, cap, fc, n_k, n_j, tile = dims
    rows = 2 * n_x * cap
    wk = d_q // 9 * 4
    rest = d_q - 2 * wk
    xc = d_model // n_j
    p = lax.axis_index("expert")
    q = lax.axis_index("data")
    cx, cc = p // 2, p % 2
    half = q // 2
    inner = q + 1 - 2 * (q % 2)
    outer = 3 - q
    lead = cc == half

    def dev(x, y, c):
        return {"expert": 2 * x + c, "data": y}

    def quarter(i):
        base = q + (i // 2) * (inner - q)
        return base + (i % 2) * (3 - 2 * base)

    partner = dev(cx, q, 1 - cc)
    inner_dev = dev(cx, inner, cc)
    outer_dev = dev(cx, outer, 1 - cc)
    mirror = dev(cx, outer, cc)

    def remote(src, dst, send, recv, device):
        return pltpu.make_async_remote_copy(src_ref=src, dst_ref=dst, send_sem=send, recv_sem=recv, device_id=device, device_id_type=MESH)

    def wait_for(ref, sem):
        pltpu.make_async_copy(ref, ref, sem).wait()

    barrier = pltpu.get_barrier_semaphore()
    peers = [partner, inner_dev, outer_dev]
    peers += [dev((cx + d) % n_x, q, cc) for d in range(1, n_x)]
    peers += [dev((cx + d) % n_x, outer, cc) for d in range(n_x)]
    for peer in peers:
        pl.semaphore_signal(barrier, inc=1, device_id=peer, device_id_type=MESH)
    pl.semaphore_wait(barrier, len(peers))

    def gu_rows(k, i):
        return gu_ref.at[k, pl.ds(quarter(i) * d_q, d_q), :]

    def send_own_gu(k, device, send, recv):
        src = pl.ds(pl.multiple_of(k * fc, 128), fc)
        for w_ref, c0 in ((wg_ref, 0), (wu_ref, fc)):
            remote(w_ref.at[:, src], gu_ref.at[k, pl.ds(q * d_q, d_q), pl.ds(c0, fc)], send, recv, device).start()

    def pass_gu(k, i, device, send, i_there):
        remote(gu_rows(k, i), gu_rows(k, i), send, r_gu.at[i_there, k], device).start()

    def send_block(j):
        cols = pl.ds(j * xc, xc)
        remote(x_ref.at[:, cols], xpar_ref.at[:, cols], s_x.at[j], r_x.at[j], mirror).start()

    def each(count, body):
        lax.fori_loop(0, count, lambda k, carry: (body(k), carry)[1], 0)

    send_block(0)
    early = min(EARLY, n_k)

    @pl.when(lead)
    def _():
        each(early, lambda k: send_own_gu(k, inner_dev, s_main.at[k], r_gu.at[2, k]))

    own_x = pltpu.make_async_copy(x_ref, h.at[pl.ds(0, tok), pl.ds(d_model, d_model)], l_x.at[0])
    own_x.start()
    expert = lax.broadcasted_iota(jnp.int32, (128, tok), 0)
    first = expert == idx_ref[0:1, :]
    second = expert == idx_ref[1:2, :]
    chosen = jnp.logical_or(first, second)
    before = lax.broadcasted_iota(jnp.int32, (tok, tok), 0) < lax.broadcasted_iota(jnp.int32, (tok, tok), 1)
    slot = jnp.dot(chosen.astype(F32).astype(BF16), before.astype(F32).astype(BF16), preferred_element_type=F32)
    key = jnp.where(jnp.logical_and(chosen, slot < cap), slot, -1.0)
    keyt[...] = key[:8, :]
    gates = jnp.where(expert - 8 == idx_ref[0:1, :], gate_ref[0:1, :], 0.0) + jnp.where(expert - 8 == idx_ref[1:2, :], gate_ref[1:2, :], 0.0)
    tok_keys[...] = jnp.where(expert < 8, key, gates).T
    send_key = remote(keyt, keyt_par, s_x.at[n_j], r_x.at[n_j], mirror)
    send_key.start()
    for j in range(1, n_j):
        send_block(j)

    @pl.when(jnp.logical_not(lead))
    def _():
        each(n_k, lambda k: send_own_gu(k, outer_dev, s_main.at[k], r_gu.at[1, k]))


    slots = lax.broadcasted_iota(jnp.int32, (cap, tok), 0).astype(F32)

    def select(keys, d):
        e = 2 * lax.rem(cx + d, n_x) + half
        return (slots == keys[pl.ds(e, 1), :]).astype(F32).astype(BF16)

    own_x.wait()

    def own_rows(t, carry):
        d = lax.rem(t + 1, n_x)
        pick_rows = select(keyt, d)
        stage = h.at[pl.ds(pl.multiple_of(t * cap, 8), cap), pl.ds(0, d_model)]
        for j in range(n_j):
            got = jnp.dot(pick_rows, h[pl.ds(0, tok), pl.ds(d_model + j * xc, xc)], preferred_element_type=F32)
            h[pl.ds(pl.multiple_of(t * cap, 8), cap), pl.ds(j * xc, xc)] = got.astype(BF16)
        dst = xrows_ref.at[pl.ds(pl.multiple_of(cx * cap, 8), cap), :]

        @pl.when(t < n_x - 1)
        def _():
            remote(stage, dst, s_own.at[t], r_own, dev(lax.rem(cx + d, n_x), q, cc)).start()

        @pl.when(t == n_x - 1)
        def _():
            pltpu.make_async_copy(stage, dst, l_loc.at[n_j]).start()

        return carry

    lax.fori_loop(0, n_x, own_rows, 0)

    def start_own_pass(k, carry):
        @pl.when(lead)
        def _():
            send_own_gu(k, partner, s_a.at[k], r_gu.at[0, k])

        return carry

    lax.fori_loop(0, n_k, start_own_pass, 0)

    send_key.wait()

    def par_cols(j, carry):
        cols = pl.ds(pl.multiple_of(j * xc, 128), xc)
        with jax.named_scope("par_wait"):
            wait_for(xpar_ref.at[:, cols], r_x.at[j])
        here = pl.ds(pl.multiple_of(d_model + j * xc, 128), xc)
        load = pltpu.make_async_copy(xpar_ref.at[:, cols], h.at[pl.ds(tok, tok), here], l_x.at[1])
        load.start()
        load.wait()

        def par_rows(t, carry2):
            d = lax.rem(t + 1, n_x)
            r0 = pl.multiple_of((n_x + t) * cap, 8)
            got = jnp.dot(select(keyt_par, d), h[pl.ds(tok, tok), here], preferred_element_type=F32)
            h[pl.ds(r0, cap), cols] = got.astype(BF16)
            stage = h.at[pl.ds(r0, cap), cols]
            dst = xrows_ref.at[pl.ds(pl.multiple_of((n_x + cx) * cap, 8), cap), cols]

            @pl.when(t < n_x - 1)
            def _():
                remote(stage, dst, s_par.at[t, j], r_par, dev(lax.rem(cx + d, n_x), q, cc)).start()

            @pl.when(t == n_x - 1)
            def _():
                pltpu.make_async_copy(stage, dst, l_loc.at[j]).start()

            return carry2

        return lax.fori_loop(0, n_x, par_rows, carry)

    lax.fori_loop(0, n_j, par_cols, 0)

    def ahead(k):
        @pl.when(lead)
        def _():
            wait_for(gu_rows(k, 2), r_gu.at[2, k])
            pass_gu(k, 2, partner, s_b.at[k], 2)

        @pl.when(jnp.logical_not(lead))
        def _():
            wait_for(gu_rows(k, 1), r_gu.at[1, k])
            pass_gu(k, 1, inner_dev, s_a.at[k], 3)
            pass_gu(k, 1, partner, s_b.at[k], 1)

    def part_rows(m):
        return pl.ds(2 * wk, d_q - 2 * wk) if isinstance(m, int) and m == 2 else pl.ds(m * wk if isinstance(m, int) else pl.multiple_of(m * wk, 8), wk)

    def wd_rows(i, m):
        return wdb_ref.at[quarter(i), part_rows(m), :]

    def send_own_wd(m, device, send, recv):
        remote(wd_ref.at[part_rows(m), :], wd_rows(0, m), send, recv, device).start()

    def phase_up(xr, wbuf):
        def gather_chunk(k, slot):
            @pl.when(lead)
            def _():
                wait_for(gu_rows(k, 1), r_gu.at[1, k])
                wait_for(gu_rows(k, 3), r_gu.at[3, k])
                src = pl.ds(pl.multiple_of(k * fc, 128), fc)
                for w_ref, c0 in ((wg_ref, 0), (wu_ref, fc)):
                    pltpu.make_async_copy(w_ref.at[:, src], wbuf.at[slot, pl.ds(q * d_q, d_q), pl.ds(c0, fc)], l_w.at[slot]).start()
                for i in (1, 2, 3):
                    pltpu.make_async_copy(gu_rows(k, i), wbuf.at[slot, pl.ds(quarter(i) * d_q, d_q), :], l_w.at[slot]).start()

            @pl.when(jnp.logical_not(lead))
            def _():
                wait_for(gu_rows(k, 3), r_gu.at[3, k])
                pass_gu(k, 3, partner, s_c.at[k], 3)
                wait_for(gu_rows(k, 0), r_gu.at[0, k])
                wait_for(gu_rows(k, 2), r_gu.at[2, k])
                pltpu.make_async_copy(gu_ref.at[k], wbuf.at[slot], l_w.at[slot]).start()

        with jax.named_scope("ahead_first"):
            for k in range(LEAD):
                ahead(k)

        with jax.named_scope("rows_wait"):
            wait_for(xrows_ref.at[pl.ds(0, (n_x - 1) * cap), :], r_own)
            wait_for(xrows_ref.at[pl.ds(0, (n_x - 1) * cap), :], r_par)
            wait_for(xrows_ref.at[pl.ds(0, cap), :], l_loc.at[n_j])
            for j in range(n_j):
                wait_for(xrows_ref.at[pl.ds(0, cap), pl.ds(0, xc)], l_loc.at[j])
        load = pltpu.make_async_copy(xrows_ref, xr, l_x.at[0])
        load.start()

        def drain(t, carry):
            wait_for(xrows_ref.at[pl.ds(0, cap), :], s_own.at[t])

            def inner_drain(j, carry2):
                wait_for(xrows_ref.at[pl.ds(0, cap), pl.ds(0, xc)], s_par.at[t, j])
                return carry2

            return lax.fori_loop(0, n_j, inner_drain, carry)

        lax.fori_loop(0, n_x - 1, drain, 0)
        for j in range(n_j):
            wait_for(xpar_ref.at[:, pl.ds(0, xc)], s_x.at[j])

        @pl.when(lead)
        def _():
            for m in range(3):
                send_own_wd(m, partner, t_a.at[m], r_wd.at[0, m])

        @pl.when(jnp.logical_not(lead))
        def _():
            for m in range(3):
                send_own_wd(m, outer_dev, t_main.at[m], r_wd.at[1, m])

        with jax.named_scope("first_chunk"):
            gather_chunk(0, 0)
            load.wait()

        def step(k, carry):
            slot = lax.rem(k, 2)

            @pl.when(k + LEAD < n_k)
            def _():
                with jax.named_scope("ahead"):
                    ahead(k + LEAD)

            late = k - min(LATE_STEP, n_k - 1) + early

            @pl.when(jnp.logical_and(lead, jnp.logical_and(late >= early, late < n_k)))
            def _():
                send_own_gu(late, inner_dev, s_main.at[late], r_gu.at[2, late])

            @pl.when(jnp.logical_and(k == min(DOWN_STEP, n_k - 1), lead))
            def _():
                for m in range(3):
                    send_own_wd(m, inner_dev, t_main.at[m], r_wd.at[2, m])

            with jax.named_scope("wload"):
                wait_for(wbuf.at[slot], l_w.at[slot])

            def row_tile(r, carry2):
                @pl.when(jnp.logical_and(r == 1, k + 1 < n_k))
                def _():
                    with jax.named_scope("gather"):
                        gather_chunk(k + 1, lax.rem(k + 1, 2))

                r0 = pl.multiple_of(r * tile, 8)
                both = jnp.dot(xr[pl.ds(r0, tile), :], wbuf[slot], preferred_element_type=F32)
                act = jax.nn.silu(both[:, :fc]) * both[:, fc:]
                h[pl.ds(r0, tile), pl.ds(pl.multiple_of(k * fc, 128), fc)] = act.astype(BF16)
                return carry2

            with jax.named_scope("mm"):
                lax.fori_loop(0, rows // tile, row_tile, 0)
            return carry

        lax.fori_loop(0, n_k, step, 0)

    def phase_down(wdv, stage, stage_end, acc, cmat, backv, backe, y):
        t_tile = min(512, tok)
        mixed, last = 6, 9

        def place(u):
            v = u - u // 7
            return v // 2, v % 2

        def chunk(u, other):
            i, m = place(u)
            qt = quarter(i)
            is_mixed = u // 6 - u // 7
            return (1 - is_mixed) * (2 * (qt + other * (3 - 2 * qt)) + m) + is_mixed * 8

        def take(i, m):
            @pl.when(jnp.logical_not(jnp.logical_and(lead, i == 0)))
            def _():
                wait_for(wd_rows(i, m), r_wd.at[i, m])

                @pl.when(jnp.logical_and(lead, i == 2))
                def _():
                    remote(wd_rows(i, m), wd_rows(i, m), t_b.at[m], r_wd.at[i, m], partner).start()

                @pl.when(jnp.logical_and(jnp.logical_not(lead), i == 1))
                def _():
                    remote(wd_rows(i, m), wd_rows(i, m), t_b.at[m], r_wd.at[i, m], partner).start()

                @pl.when(jnp.logical_and(jnp.logical_not(lead), i == 3))
                def _():
                    remote(wd_rows(i, m), wd_rows(i, m), t_c.at[m], r_wd.at[i, m], partner).start()

        def load(i, m, dst, sem):
            @pl.when(jnp.logical_and(lead, i == 0))
            def _():
                pltpu.make_async_copy(wd_ref.at[part_rows(m), :], dst, sem).start()

            @pl.when(jnp.logical_not(jnp.logical_and(lead, i == 0)))
            def _():
                pltpu.make_async_copy(wd_rows(i, m), dst, sem).start()

        def load_main(u):
            i, m = place(u)
            load(i, m, wdv.at[m], l_wd.at[m])

        def load_rest(i):
            load(i, 2, wdv.at[2, pl.ds(pl.multiple_of(quarter(i) * rest, 8), rest), :], l_wd.at[2])

        def combine(g, rows_of, old_of, put):
            def tok_tile(r, carry):
                r0 = pl.multiple_of(r * t_tile, 8)
                gates = tok_keys[pl.ds(r0, t_tile), :]
                lanes = lax.broadcasted_iota(jnp.int32, (t_tile, 128), 1)
                total = old_of(r0)
                for x in range(n_x):
                    e = 2 * x + g
                    rows_x = jnp.dot(cmat[e, pl.ds(r0, t_tile), :], rows_of(x), preferred_element_type=F32)
                    gate_x = jnp.sum(jnp.where(lanes == e + 8, gates, 0.0), axis=1, keepdims=True)
                    total = gate_x * rows_x if total is None else total + gate_x * rows_x
                put(r0, total)
                return carry

            lax.fori_loop(0, tok // t_tile, tok_tile, 0)

        def combine_main(a, g, add, buf):
            def put(r0, total):
                acc[a, pl.ds(r0, t_tile), :] = total

            combine(g, lambda x: backv[buf, pl.ds(x * cap, cap), :], lambda r0: acc[a, pl.ds(r0, t_tile), :] if add else None, put)

        def to_y(c0, width, extra_of):
            cols = pl.ds(c0, width)

            def tok_tile(r, carry):
                r0 = pl.multiple_of(r * t_tile, 8)
                y[pl.ds(r0, t_tile), cols] = (y[pl.ds(r0, t_tile), cols].astype(F32) + extra_of(r0)).astype(BF16)
                return carry

            lax.fori_loop(0, tok // t_tile, tok_tile, 0)

        def fetch(u):
            here, there = chunk(u, 0), chunk(u, 1)
            wait_for(stage.at[0, 0, pl.ds(0, cap), :], l_ret.at[lax.rem(u, STAGES)])
            wait_for(back_ref.at[0, 0, pl.ds(0, (n_x - 1) * cap), :], r_back.at[here, half])
            pltpu.make_async_copy(back_ref.at[here, half], backv.at[0], l_back.at[0]).start()
            wait_for(back_ref.at[0, 0], r_back.at[there, 1 - half])
            pltpu.make_async_copy(back_ref.at[there, 1 - half], backv.at[1], l_back.at[1]).start()

        def add_up(u):
            here, there = chunk(u, 0), chunk(u, 1)
            i, m = place(u)
            is_mixed = u // 6 - u // 7
            held_here = (1 - is_mixed) * (2 * (i % 2) + m) + is_mixed * 4
            held_there = (1 - is_mixed) * (2 - 2 * (i % 2) + m) + is_mixed * 4

            def both(add_first, add_second):
                wait_for(backv.at[0], l_back.at[0])
                combine_main(held_here, half, add_first, 0)
                wait_for(backv.at[1], l_back.at[1])
                combine_main(held_there, 1 - half, add_second, 1)

            @pl.when(u == mixed)
            def _():
                both(False, True)

            @pl.when(jnp.logical_and(u != mixed, i % 2 == 0))
            def _():
                both(False, False)

            @pl.when(jnp.logical_and(u != mixed, i % 2 == 1))
            def _():
                both(True, True)
                for c in range(8):

                    for c_done, held in ((here, held_here), (there, held_there)):

                        @pl.when(c_done == c)
                        def _(c=c, held=held):
                            to_y(c // 2 * d_q + c % 2 * wk, wk, lambda r0: acc[held, pl.ds(r0, t_tile), :])

        def add_end():
            wait_for(stage_end.at[0, pl.ds(0, cap), :], l_ret.at[STAGES])
            wait_for(end_ref.at[0, pl.ds(0, (n_x - 1) * cap), :], r_end.at[half])
            first_load = pltpu.make_async_copy(end_ref.at[half], backe.at[0], l_back.at[0])
            first_load.start()
            wait_for(end_ref.at[0], r_end.at[1 - half])
            second_load = pltpu.make_async_copy(end_ref.at[1 - half], backe.at[1], l_back.at[1])
            second_load.start()
            for buf, g, load_end in ((0, half, first_load), (1, 1 - half, second_load)):
                load_end.wait()

                def put(r0, total, buf=buf):
                    acc[buf, pl.ds(r0, t_tile), pl.ds(0, rest)] = total

                combine(g, lambda x, buf=buf: backe[buf, pl.ds(x * cap, cap), :], lambda r0: None, put)

        slot_lane = lax.broadcasted_iota(jnp.int32, (tok, cap), 1).astype(F32)
        for e in range(2 * n_x):
            cmat[e] = (slot_lane == tok_keys[:, e:e + 1]).astype(F32).astype(BF16)

        x_load = pltpu.make_async_copy(x_ref, y, l_x.at[0])
        x_load.start()
        take(0, 0)
        load_main(0)
        wdv[2, pl.ds(pl.multiple_of(quarter(3) * rest, 8), rest), :] = jnp.zeros((rest, ffn), BF16)
        x_load.wait()

        def group_of(t):
            return (t + 1 - cc) % 2

        def send_back(t, out_ref, dst, send, recv, local_sem):
            s = group_of(t)
            for d in range(n_x):
                x_src = lax.rem(cx + 1 + d, n_x)
                src = out_ref.at[pl.ds(pl.multiple_of(x_src * cap, 8), cap), :]

                def go(src=src, x_src=x_src, d=d):
                    remote(src, dst, send.at[t * n_x + d], recv, dev(x_src, q + s * (outer - q), cc)).start()

                if d < n_x - 1:
                    go()
                else:
                    pl.when(s == 1)(go)

                    @pl.when(s == 0)
                    def _(src=src):
                        pltpu.make_async_copy(src, dst, local_sem).start()

        def sent_back(t, ref, send):
            for d in range(n_x - 1):
                wait_for(ref, send.at[t * n_x + d])

            @pl.when(group_of(t) == 1)
            def _():
                wait_for(ref, send.at[t * n_x + n_x - 1])

        g_tile = n_x * cap // 2

        def group_rows(t, r):
            return h[pl.ds(pl.multiple_of((group_of(t) * 2 + r) * g_tile, 8), g_tile), :]

        def times(left, right):
            return lax.dot_general(left, right, (((1,), (1,)), ((), ())), preferred_element_type=F32).astype(BF16)

        my_rows = pl.ds(pl.multiple_of(cx * cap, 8), cap)

        def part(u, carry):
            i, m = place(u)
            slot = lax.rem(u, STAGES)
            is_mixed = u // 6 - u // 7
            buf = (1 - is_mixed) * m + is_mixed * 2
            other_core = jnp.logical_not(lead)

            @pl.when(u == 0)
            def _():
                take(0, 1)
                load_main(u + 1)
                take(0, 2)
                load_rest(0)

            @pl.when(u == 1)
            def _():
                with jax.named_scope("take_outer"):
                    for k in range(3):
                        take(1, k)

            @pl.when(jnp.logical_and(u == 4, other_core))
            def _():
                for k in range(3):
                    remote(wd_rows(1, k), wd_rows(1, k), t_a.at[k], r_wd.at[3, k], inner_dev).start()

            @pl.when(jnp.logical_and(u >= 1, u <= 2))
            def _():
                load_main(u + 1)

            @pl.when(u == 2)
            def _():
                load_rest(1)

            @pl.when(jnp.logical_and(u == 3, lead))
            def _():
                take(2, 0)

            @pl.when(jnp.logical_and(u == 5, other_core))
            def _():
                with jax.named_scope("take_21b"):
                    take(2, 1)
                    load_main(u)

            @pl.when(jnp.logical_and(u == 5, lead))
            def _():
                take(2, 2)

            @pl.when(jnp.logical_or(u == 7, u == 8))
            def _():
                with jax.named_scope("take_late"):
                    take(3, m)
                    load_main(u)

            @pl.when(u != mixed)
            def _():
                with jax.named_scope("wdload"):
                    wait_for(wdv.at[0], l_wd.at[m])

            @pl.when(u == mixed)
            def _():
                with jax.named_scope("restload"):
                    wait_for(wdv.at[2, pl.ds(0, 3 * rest), :], l_wd.at[2])

            def middle():
                @pl.when(jnp.logical_and(u == 3, other_core))
                def _():
                    take(2, 0)

                @pl.when(u == 3)
                def _():
                    load_main(u + 1)

                @pl.when(jnp.logical_and(u == 4, lead))
                def _():
                    with jax.named_scope("take_21a"):
                        take(2, 1)
                        load_main(u + 1)

                @pl.when(jnp.logical_and(u == 5, other_core))
                def _():
                    take(2, 2)

                @pl.when(u == 5)
                def _():
                    load_rest(2)

                @pl.when(u == last - 1)
                def _():
                    take(3, 2)
                    load_rest(3)

                @pl.when(jnp.logical_and(u >= 2, u < last - 1))
                def _():
                    fetch(u - 2)

            def group(t, carry2):
                with jax.named_scope('middle'):
                    pl.when(t == 1)(middle)

                @pl.when(u >= STAGES)
                def _():
                    with jax.named_scope("sent_wait"):
                        sent_back(t, stage.at[0, 0, pl.ds(0, cap), :], s_ret.at[slot])

                def rows_of_group(r, carry3):
                    stage[slot, t, pl.ds(pl.multiple_of(r * g_tile, 8), g_tile), :] = times(group_rows(t, r), wdv[buf])
                    return carry3

                lax.fori_loop(0, 2, rows_of_group, 0)
                c = chunk(u, 0)
                send_back(t, stage.at[slot, t], back_ref.at[c, half, my_rows, :], s_ret.at[slot], r_back.at[c, half], l_ret.at[slot])
                return carry2

            with jax.named_scope("groups"):
                lax.fori_loop(0, 2, group, 0)

            @pl.when(jnp.logical_and(u >= 2, u < last - 1))
            def _():
                with jax.named_scope("add_up"):
                    add_up(u - 2)

            return carry

        lax.fori_loop(0, last, part, 0)
        wait_for(wdv.at[2, pl.ds(0, rest), :], l_wd.at[2])
        end_rows = pl.ds(pl.multiple_of(quarter(3) * rest, 8), rest)

        def end_group(t, carry):
            def rows_of_group(r, carry2):
                stage_end[t, pl.ds(pl.multiple_of(r * g_tile, 8), g_tile), :] = times(group_rows(t, r), wdv[2, end_rows, :])
                return carry2

            lax.fori_loop(0, 2, rows_of_group, 0)
            send_back(t, stage_end.at[t], end_ref.at[half, my_rows, :], s_ret.at[STAGES], r_end.at[half], l_ret.at[STAGES])
            return carry

        with jax.named_scope("end_groups"):
            lax.fori_loop(0, 2, end_group, 0)

        def add_later(k, carry):
            with jax.named_scope("fetch_tail"):
                fetch(k + 6)
            add_up(k + 6)
            return carry

        with jax.named_scope("add_tail"):
            lax.fori_loop(0, 3, add_later, 0)
        with jax.named_scope("add_end"):
            add_end()
        for qt in range(4):
            c0, held = qt * d_q + 2 * wk, pl.ds(qt * rest, rest)

            @pl.when(jnp.logical_and(quarter(3) != qt, quarter(2) != qt))
            def _(c0=c0, held=held):
                to_y(c0, rest, lambda r0: acc[4, pl.ds(r0, t_tile), held])

            for buf, i in ((0, 3), (1, 2)):

                @pl.when(quarter(i) == qt)
                def _(c0=c0, held=held, buf=buf):
                    to_y(c0, rest, lambda r0: acc[4, pl.ds(r0, t_tile), held] + acc[buf, pl.ds(r0, t_tile), pl.ds(0, rest)])

        store = pltpu.make_async_copy(y, y_ref, l_x.at[0])
        store.start()

        for k in range(STAGES):
            for t in range(2):
                sent_back(t, stage.at[0, 0, pl.ds(0, cap), :], s_ret.at[k])
        for t in range(2):
            sent_back(t, stage_end.at[0, pl.ds(0, cap), :], s_ret.at[STAGES])
        store.wait()

    pl.run_scoped(phase_up, pltpu.VMEM((rows, d_model), BF16), pltpu.VMEM((2, d_model, 2 * fc), BF16))
    pl.run_scoped(
        phase_down,
        pltpu.VMEM((3, wk, ffn), BF16),
        pltpu.VMEM((STAGES, 2, n_x * cap, wk), BF16),
        pltpu.VMEM((2, n_x * cap, rest), BF16),
        pltpu.VMEM((5, tok, wk), F32),
        pltpu.VMEM((2 * n_x, tok, cap), BF16),
        pltpu.VMEM((2, n_x * cap, wk), BF16),
        pltpu.VMEM((2, n_x * cap, rest), BF16),
        pltpu.VMEM((tok, d_model), BF16),
    )

    def drain_gu(k, carry):
        wait_for(gu_rows(k, 0), s_main.at[k])
        wait_for(gu_rows(k, 0), s_a.at[k])
        wait_for(gu_rows(k, 0), s_b.at[k])

        @pl.when(jnp.logical_not(lead))
        def _():
            wait_for(gu_rows(k, 0), s_c.at[k])

        return carry

    with jax.named_scope("drain"):
        lax.fori_loop(0, n_k, drain_gu, 0)

    for m in range(3):
        for sem in (t_main, t_a, t_b):
            wait_for(wd_rows(0, m), sem.at[m])

    @pl.when(jnp.logical_not(lead))
    def _():
        for m in range(3):
            wait_for(wd_rows(0, m), t_c.at[m])


def solution(mesh):
    n_group, n_y = mesh.shape["expert"], mesh.shape["data"]
    assert n_y == 4 and n_group % 2 == 0
    n_x = n_group // 2
    tok_spec = P(("rep", "expert", "data"), None)
    wide_spec = P("expert", "data", None)
    down_spec = P("expert", None, "data")

    def device_step(x_loc, idx_loc, gate_loc, wg_loc, wu_loc, wd_loc):
        tok, d_model = x_loc.shape
        n_local, d_q, ffn = wg_loc.shape
        assert n_local == 1 and n_group == 8 and d_q % 72 == 0
        cap = capacity_rows(tok, idx_loc.shape[1], n_group)
        fc = pick(ffn, (384, 256, 128))
        n_k, n_j = ffn // fc, pick(d_model // 128, (3, 2, 1))
        rows = 2 * n_x * cap
        tile = pick(rows, (1280, 48, 8))
        dims = (n_x, tok, d_model, d_q, ffn, cap, fc, n_k, n_j, tile)
        hbm = pl.BlockSpec(memory_space=pl.ANY)
        vmem = pl.BlockSpec(memory_space=pltpu.VMEM)
        dma = pltpu.SemaphoreType.DMA
        shape = jax.ShapeDtypeStruct
        outs = pl.pallas_call(
            functools.partial(moe_kernel, dims),
            name="moe_layer",
            out_shape=[
                shape((tok, d_model), BF16),
                shape((tok, d_model), BF16),
                shape((rows, d_model), BF16),
                shape((n_k, d_model, 2 * fc), BF16),
                shape((4, d_q, ffn), BF16),
                shape((9, 2, n_x * cap, d_q // 9 * 4), BF16),
                shape((2, n_x * cap, d_q // 9), BF16),
            ],
            in_specs=[vmem, vmem, hbm, hbm, hbm, hbm],
            out_specs=[hbm] * 7,
            scratch_shapes=[
                pltpu.VMEM((rows, ffn), BF16),
                pltpu.VMEM((8, tok), F32),
                pltpu.VMEM((8, tok), F32),
                pltpu.VMEM((tok, 128), F32),
                dma((n_j + 1,)), dma((n_j + 1,)), dma((n_x - 1,)), dma, dma((n_x - 1, n_j)), dma, dma((n_j + 1,)), dma((2,)),
                dma((n_k,)), dma((n_k,)), dma((n_k,)), dma((n_k,)), dma((4, n_k)), dma((2,)),
                dma((3,)), dma((3,)), dma((3,)), dma((3,)), dma((4, 3)), dma((3,)),
                dma((STAGES + 1, 2 * n_x)), dma((STAGES + 1,)), dma((9, 2)), dma((2,)), dma((2,)),
            ],
            compiler_params=pltpu.CompilerParams(collective_id=0, has_side_effects=True, vmem_limit_bytes=67_043_328),
        )(idx_loc.T, gate_loc.T, x_loc, wg_loc.reshape(d_q, ffn), wu_loc.reshape(d_q, ffn), wd_loc.reshape(ffn, d_q).T)
        return outs[0]

    return jax.shard_map(device_step, mesh=mesh, in_specs=(tok_spec, tok_spec, tok_spec, wide_spec, wide_spec, down_spec), out_specs=tok_spec, check_vma=False)
```

```python
import functools

import jax
import jax.numpy as jnp
from jax import lax
from jax.experimental import pallas as pl
from jax.experimental.pallas import tpu as pltpu
from jax.sharding import PartitionSpec as P

MESH = pl.DeviceIdType.MESH
F32 = jnp.float32
BF16 = jnp.bfloat16
LEAD = 2
DOWN_STEP = 13
STAGES = 3


def capacity_rows(tok_rows, top_k, n_exp):
    return max(8, ((5 * top_k * tok_rows) // (4 * n_exp) + 7) // 8 * 8)


def pick(total, options):
    return next(c for c in options if total % c == 0)


def moe_kernel(dims, idx_ref, gate_ref, x_ref, wg_ref, wu_ref, wd_ref, y_ref, xpar_ref, xrows_ref, gu_ref, wdb_ref, back_ref, end_ref,
               h, keyt, keyt_par, tok_keys,
               s_x, r_x, s_own, r_own, s_par, r_par, l_loc, l_x,
               s_main, s_a, s_b, s_c, r_gu, l_w,
               t_main, t_a, t_b, t_c, r_wd, l_wd, s_ret, l_ret, r_back, r_end, l_back):
    n_x, tok, d_model, d_q, ffn, cap, fc, n_k, n_j, tile = dims
    rows = 2 * n_x * cap
    wk = d_q // 9 * 4
    rest = d_q - 2 * wk
    xc = d_model // n_j
    p = lax.axis_index("expert")
    q = lax.axis_index("data")
    cx, cc = p // 2, p % 2
    half = q // 2
    inner = q + 1 - 2 * (q % 2)
    outer = 3 - q
    lead = cc == half

    def dev(x, y, c):
        return {"expert": 2 * x + c, "data": y}

    def quarter(i):
        base = q + (i // 2) * (inner - q)
        return base + (i % 2) * (3 - 2 * base)

    partner = dev(cx, q, 1 - cc)
    inner_dev = dev(cx, inner, cc)
    outer_dev = dev(cx, outer, 1 - cc)
    mirror = dev(cx, outer, cc)

    def remote(src, dst, send, recv, device):
        return pltpu.make_async_remote_copy(src_ref=src, dst_ref=dst, send_sem=send, recv_sem=recv, device_id=device, device_id_type=MESH)

    def wait_for(ref, sem):
        pltpu.make_async_copy(ref, ref, sem).wait()

    barrier = pltpu.get_barrier_semaphore()
    peers = [partner, inner_dev, outer_dev]
    peers += [dev((cx + d) % n_x, q, cc) for d in range(1, n_x)]
    peers += [dev((cx + d) % n_x, outer, cc) for d in range(n_x)]
    for peer in peers:
        pl.semaphore_signal(barrier, inc=1, device_id=peer, device_id_type=MESH)
    pl.semaphore_wait(barrier, len(peers))

    def gu_rows(k, i):
        return gu_ref.at[k, pl.ds(quarter(i) * d_q, d_q), :]

    def send_own_gu(k, device, send, recv):
        src = pl.ds(pl.multiple_of(k * fc, 128), fc)
        for w_ref, c0 in ((wg_ref, 0), (wu_ref, fc)):
            remote(w_ref.at[:, src], gu_ref.at[k, pl.ds(q * d_q, d_q), pl.ds(c0, fc)], send, recv, device).start()

    def pass_gu(k, i, device, send, i_there):
        remote(gu_rows(k, i), gu_rows(k, i), send, r_gu.at[i_there, k], device).start()

    def send_block(j):
        cols = pl.ds(j * xc, xc)
        remote(x_ref.at[:, cols], xpar_ref.at[:, cols], s_x.at[j], r_x.at[j], mirror).start()

    def each(count, body):
        lax.fori_loop(0, count, lambda k, carry: (body(k), carry)[1], 0)

    send_block(0)

    @pl.when(lead)
    def _():
        each(n_k, lambda k: send_own_gu(k, inner_dev, s_main.at[k], r_gu.at[2, k]))

    own_x = pltpu.make_async_copy(x_ref, h.at[pl.ds(0, tok), pl.ds(d_model, d_model)], l_x.at[0])
    own_x.start()
    expert = lax.broadcasted_iota(jnp.int32, (128, tok), 0)
    first = expert == idx_ref[0:1, :]
    second = expert == idx_ref[1:2, :]
    chosen = jnp.logical_or(first, second)
    before = lax.broadcasted_iota(jnp.int32, (tok, tok), 0) < lax.broadcasted_iota(jnp.int32, (tok, tok), 1)
    slot = jnp.dot(chosen.astype(F32).astype(BF16), before.astype(F32).astype(BF16), preferred_element_type=F32)
    key = jnp.where(jnp.logical_and(chosen, slot < cap), slot, -1.0)
    keyt[...] = key[:8, :]
    gates = jnp.where(expert - 8 == idx_ref[0:1, :], gate_ref[0:1, :], 0.0) + jnp.where(expert - 8 == idx_ref[1:2, :], gate_ref[1:2, :], 0.0)
    tok_keys[...] = jnp.where(expert < 8, key, gates).T
    send_key = remote(keyt, keyt_par, s_x.at[n_j], r_x.at[n_j], mirror)
    send_key.start()
    for j in range(1, n_j):
        send_block(j)

    @pl.when(jnp.logical_not(lead))
    def _():
        each(n_k, lambda k: send_own_gu(k, outer_dev, s_main.at[k], r_gu.at[1, k]))


    slots = lax.broadcasted_iota(jnp.int32, (cap, tok), 0).astype(F32)

    def select(keys, d):
        e = 2 * lax.rem(cx + d, n_x) + half
        return (slots == keys[pl.ds(e, 1), :]).astype(F32).astype(BF16)

    own_x.wait()

    def own_rows(t, carry):
        d = lax.rem(t + 1, n_x)
        pick_rows = select(keyt, d)
        stage = h.at[pl.ds(pl.multiple_of(t * cap, 8), cap), pl.ds(0, d_model)]
        for j in range(n_j):
            got = jnp.dot(pick_rows, h[pl.ds(0, tok), pl.ds(d_model + j * xc, xc)], preferred_element_type=F32)
            h[pl.ds(pl.multiple_of(t * cap, 8), cap), pl.ds(j * xc, xc)] = got.astype(BF16)
        dst = xrows_ref.at[pl.ds(pl.multiple_of(cx * cap, 8), cap), :]

        @pl.when(t < n_x - 1)
        def _():
            remote(stage, dst, s_own.at[t], r_own, dev(lax.rem(cx + d, n_x), q, cc)).start()

        @pl.when(t == n_x - 1)
        def _():
            pltpu.make_async_copy(stage, dst, l_loc.at[n_j]).start()

        return carry

    lax.fori_loop(0, n_x, own_rows, 0)

    def start_own_pass(k, carry):
        @pl.when(lead)
        def _():
            send_own_gu(k, partner, s_a.at[k], r_gu.at[0, k])

        return carry

    lax.fori_loop(0, n_k, start_own_pass, 0)

    send_key.wait()

    def par_cols(j, carry):
        cols = pl.ds(pl.multiple_of(j * xc, 128), xc)
        with jax.named_scope("par_wait"):
            wait_for(xpar_ref.at[:, cols], r_x.at[j])
        here = pl.ds(pl.multiple_of(d_model + j * xc, 128), xc)
        load = pltpu.make_async_copy(xpar_ref.at[:, cols], h.at[pl.ds(tok, tok), here], l_x.at[1])
        load.start()
        load.wait()

        def par_rows(t, carry2):
            d = lax.rem(t + 1, n_x)
            r0 = pl.multiple_of((n_x + t) * cap, 8)
            got = jnp.dot(select(keyt_par, d), h[pl.ds(tok, tok), here], preferred_element_type=F32)
            h[pl.ds(r0, cap), cols] = got.astype(BF16)
            stage = h.at[pl.ds(r0, cap), cols]
            dst = xrows_ref.at[pl.ds(pl.multiple_of((n_x + cx) * cap, 8), cap), cols]

            @pl.when(t < n_x - 1)
            def _():
                remote(stage, dst, s_par.at[t, j], r_par, dev(lax.rem(cx + d, n_x), q, cc)).start()

            @pl.when(t == n_x - 1)
            def _():
                pltpu.make_async_copy(stage, dst, l_loc.at[j]).start()

            return carry2

        return lax.fori_loop(0, n_x, par_rows, carry)

    lax.fori_loop(0, n_j, par_cols, 0)

    def ahead(k):
        @pl.when(lead)
        def _():
            wait_for(gu_rows(k, 2), r_gu.at[2, k])
            pass_gu(k, 2, partner, s_b.at[k], 2)

        @pl.when(jnp.logical_not(lead))
        def _():
            wait_for(gu_rows(k, 1), r_gu.at[1, k])
            pass_gu(k, 1, inner_dev, s_a.at[k], 3)
            pass_gu(k, 1, partner, s_b.at[k], 1)

    def part_rows(m):
        return pl.ds(2 * wk, d_q - 2 * wk) if isinstance(m, int) and m == 2 else pl.ds(m * wk if isinstance(m, int) else pl.multiple_of(m * wk, 8), wk)

    def wd_rows(i, m):
        return wdb_ref.at[quarter(i), part_rows(m), :]

    def send_own_wd(m, device, send, recv):
        remote(wd_ref.at[part_rows(m), :], wd_rows(0, m), send, recv, device).start()

    def phase_up(xr, wbuf):
        def gather_chunk(k, slot):
            @pl.when(lead)
            def _():
                wait_for(gu_rows(k, 1), r_gu.at[1, k])
                wait_for(gu_rows(k, 3), r_gu.at[3, k])
                src = pl.ds(pl.multiple_of(k * fc, 128), fc)
                for w_ref, c0 in ((wg_ref, 0), (wu_ref, fc)):
                    pltpu.make_async_copy(w_ref.at[:, src], wbuf.at[slot, pl.ds(q * d_q, d_q), pl.ds(c0, fc)], l_w.at[slot]).start()
                for i in (1, 2, 3):
                    pltpu.make_async_copy(gu_rows(k, i), wbuf.at[slot, pl.ds(quarter(i) * d_q, d_q), :], l_w.at[slot]).start()

            @pl.when(jnp.logical_not(lead))
            def _():
                wait_for(gu_rows(k, 3), r_gu.at[3, k])
                pass_gu(k, 3, partner, s_c.at[k], 3)
                wait_for(gu_rows(k, 0), r_gu.at[0, k])
                wait_for(gu_rows(k, 2), r_gu.at[2, k])
                pltpu.make_async_copy(gu_ref.at[k], wbuf.at[slot], l_w.at[slot]).start()

        with jax.named_scope("ahead_first"):
            for k in range(LEAD):
                ahead(k)

        with jax.named_scope("rows_wait"):
            wait_for(xrows_ref.at[pl.ds(0, (n_x - 1) * cap), :], r_own)
            wait_for(xrows_ref.at[pl.ds(0, (n_x - 1) * cap), :], r_par)
            wait_for(xrows_ref.at[pl.ds(0, cap), :], l_loc.at[n_j])
            for j in range(n_j):
                wait_for(xrows_ref.at[pl.ds(0, cap), pl.ds(0, xc)], l_loc.at[j])
        load = pltpu.make_async_copy(xrows_ref, xr, l_x.at[0])
        load.start()

        def drain(t, carry):
            wait_for(xrows_ref.at[pl.ds(0, cap), :], s_own.at[t])

            def inner_drain(j, carry2):
                wait_for(xrows_ref.at[pl.ds(0, cap), pl.ds(0, xc)], s_par.at[t, j])
                return carry2

            return lax.fori_loop(0, n_j, inner_drain, carry)

        lax.fori_loop(0, n_x - 1, drain, 0)
        for j in range(n_j):
            wait_for(xpar_ref.at[:, pl.ds(0, xc)], s_x.at[j])

        @pl.when(lead)
        def _():
            for m in range(3):
                send_own_wd(m, partner, t_a.at[m], r_wd.at[0, m])

        @pl.when(jnp.logical_not(lead))
        def _():
            for m in range(3):
                send_own_wd(m, outer_dev, t_main.at[m], r_wd.at[1, m])

        with jax.named_scope("first_chunk"):
            gather_chunk(0, 0)
            load.wait()

        def step(k, carry):
            slot = lax.rem(k, 2)

            @pl.when(k + LEAD < n_k)
            def _():
                with jax.named_scope("ahead"):
                    ahead(k + LEAD)

            @pl.when(jnp.logical_and(k == min(DOWN_STEP, n_k - 1), lead))
            def _():
                for m in range(3):
                    send_own_wd(m, inner_dev, t_main.at[m], r_wd.at[2, m])

            with jax.named_scope("wload"):
                wait_for(wbuf.at[slot], l_w.at[slot])

            def row_tile(r, carry2):
                @pl.when(jnp.logical_and(r == 1, k + 1 < n_k))
                def _():
                    with jax.named_scope("gather"):
                        gather_chunk(k + 1, lax.rem(k + 1, 2))

                r0 = pl.multiple_of(r * tile, 8)
                both = jnp.dot(xr[pl.ds(r0, tile), :], wbuf[slot], preferred_element_type=F32)
                act = jax.nn.silu(both[:, :fc]) * both[:, fc:]
                h[pl.ds(r0, tile), pl.ds(pl.multiple_of(k * fc, 128), fc)] = act.astype(BF16)
                return carry2

            with jax.named_scope("mm"):
                lax.fori_loop(0, rows // tile, row_tile, 0)
            return carry

        lax.fori_loop(0, n_k, step, 0)

    def phase_down(wdv, stage, stage_end, acc, cmat, backv, backe, y):
        t_tile = min(512, tok)
        mixed, last = 6, 9

        def place(u):
            v = u - u // 7
            return v // 2, v % 2

        def chunk(u, other):
            i, m = place(u)
            qt = quarter(i)
            is_mixed = u // 6 - u // 7
            return (1 - is_mixed) * (2 * (qt + other * (3 - 2 * qt)) + m) + is_mixed * 8

        def take(i, m):
            @pl.when(jnp.logical_not(jnp.logical_and(lead, i == 0)))
            def _():
                wait_for(wd_rows(i, m), r_wd.at[i, m])

                @pl.when(jnp.logical_and(lead, i == 2))
                def _():
                    remote(wd_rows(i, m), wd_rows(i, m), t_b.at[m], r_wd.at[i, m], partner).start()

                @pl.when(jnp.logical_and(jnp.logical_not(lead), i == 1))
                def _():
                    remote(wd_rows(i, m), wd_rows(i, m), t_b.at[m], r_wd.at[i, m], partner).start()

                @pl.when(jnp.logical_and(jnp.logical_not(lead), i == 3))
                def _():
                    remote(wd_rows(i, m), wd_rows(i, m), t_c.at[m], r_wd.at[i, m], partner).start()

        def load(i, m, dst, sem):
            @pl.when(jnp.logical_and(lead, i == 0))
            def _():
                pltpu.make_async_copy(wd_ref.at[part_rows(m), :], dst, sem).start()

            @pl.when(jnp.logical_not(jnp.logical_and(lead, i == 0)))
            def _():
                pltpu.make_async_copy(wd_rows(i, m), dst, sem).start()

        def load_main(u):
            i, m = place(u)
            load(i, m, wdv.at[m], l_wd.at[m])

        def load_rest(i):
            load(i, 2, wdv.at[2, pl.ds(pl.multiple_of(quarter(i) * rest, 8), rest), :], l_wd.at[2])

        def combine(g, rows_of, old_of, put):
            def tok_tile(r, carry):
                r0 = pl.multiple_of(r * t_tile, 8)
                gates = tok_keys[pl.ds(r0, t_tile), :]
                lanes = lax.broadcasted_iota(jnp.int32, (t_tile, 128), 1)
                total = old_of(r0)
                for x in range(n_x):
                    e = 2 * x + g
                    rows_x = jnp.dot(cmat[e, pl.ds(r0, t_tile), :], rows_of(x), preferred_element_type=F32)
                    gate_x = jnp.sum(jnp.where(lanes == e + 8, gates, 0.0), axis=1, keepdims=True)
                    total = gate_x * rows_x if total is None else total + gate_x * rows_x
                put(r0, total)
                return carry

            lax.fori_loop(0, tok // t_tile, tok_tile, 0)

        def combine_main(a, g, add, buf):
            def put(r0, total):
                acc[a, pl.ds(r0, t_tile), :] = total

            combine(g, lambda x: backv[buf, pl.ds(x * cap, cap), :], lambda r0: acc[a, pl.ds(r0, t_tile), :] if add else None, put)

        def to_y(c0, width, extra_of):
            cols = pl.ds(c0, width)

            def tok_tile(r, carry):
                r0 = pl.multiple_of(r * t_tile, 8)
                y[pl.ds(r0, t_tile), cols] = (y[pl.ds(r0, t_tile), cols].astype(F32) + extra_of(r0)).astype(BF16)
                return carry

            lax.fori_loop(0, tok // t_tile, tok_tile, 0)

        def fetch(u):
            here, there = chunk(u, 0), chunk(u, 1)

            @pl.when(u >= last - STAGES - 1)
            def _():
                wait_for(stage.at[0, 0, pl.ds(0, cap), :], l_ret.at[lax.rem(u, STAGES)])

            wait_for(back_ref.at[0, 0, pl.ds(0, (n_x - 1) * cap), :], r_back.at[here, half])
            pltpu.make_async_copy(back_ref.at[here, half], backv.at[0], l_back.at[0]).start()
            wait_for(back_ref.at[0, 0], r_back.at[there, 1 - half])
            pltpu.make_async_copy(back_ref.at[there, 1 - half], backv.at[1], l_back.at[1]).start()

        def add_up(u):
            here, there = chunk(u, 0), chunk(u, 1)
            i, m = place(u)
            is_mixed = u // 6 - u // 7
            held_here = (1 - is_mixed) * (2 * (i % 2) + m) + is_mixed * 4
            held_there = (1 - is_mixed) * (2 - 2 * (i % 2) + m) + is_mixed * 4

            def both(add_first, add_second):
                wait_for(backv.at[0], l_back.at[0])
                combine_main(held_here, half, add_first, 0)
                wait_for(backv.at[1], l_back.at[1])
                combine_main(held_there, 1 - half, add_second, 1)

            @pl.when(u == mixed)
            def _():
                both(False, True)

            @pl.when(jnp.logical_and(u != mixed, i % 2 == 0))
            def _():
                both(False, False)

            @pl.when(jnp.logical_and(u != mixed, i % 2 == 1))
            def _():
                both(True, True)
                for c in range(8):

                    for c_done, held in ((here, held_here), (there, held_there)):

                        @pl.when(c_done == c)
                        def _(c=c, held=held):
                            to_y(c // 2 * d_q + c % 2 * wk, wk, lambda r0: acc[held, pl.ds(r0, t_tile), :])

        def add_end():
            wait_for(stage_end.at[0, pl.ds(0, cap), :], l_ret.at[STAGES])
            wait_for(end_ref.at[0, pl.ds(0, (n_x - 1) * cap), :], r_end.at[half])
            first_load = pltpu.make_async_copy(end_ref.at[half], backe.at[0], l_back.at[0])
            first_load.start()
            wait_for(end_ref.at[0], r_end.at[1 - half])
            second_load = pltpu.make_async_copy(end_ref.at[1 - half], backe.at[1], l_back.at[1])
            second_load.start()
            for buf, g, load_end in ((0, half, first_load), (1, 1 - half, second_load)):
                load_end.wait()

                def put(r0, total, buf=buf):
                    acc[buf, pl.ds(r0, t_tile), pl.ds(0, rest)] = total

                combine(g, lambda x, buf=buf: backe[buf, pl.ds(x * cap, cap), :], lambda r0: None, put)

        slot_lane = lax.broadcasted_iota(jnp.int32, (tok, cap), 1).astype(F32)
        for e in range(2 * n_x):
            cmat[e] = (slot_lane == tok_keys[:, e:e + 1]).astype(F32).astype(BF16)

        x_load = pltpu.make_async_copy(x_ref, y, l_x.at[0])
        x_load.start()
        take(0, 0)
        load_main(0)
        wdv[2, pl.ds(pl.multiple_of(quarter(3) * rest, 8), rest), :] = jnp.zeros((rest, ffn), BF16)
        x_load.wait()

        def group_of(t):
            return (t + 1 - cc) % 2

        def send_back(t, out_ref, dst, send, recv, local_sem):
            s = group_of(t)
            for d in range(n_x):
                x_src = lax.rem(cx + 1 + d, n_x)
                src = out_ref.at[pl.ds(pl.multiple_of(x_src * cap, 8), cap), :]

                def go(src=src, x_src=x_src, d=d):
                    remote(src, dst, send.at[t * n_x + d], recv, dev(x_src, q + s * (outer - q), cc)).start()

                if d < n_x - 1:
                    go()
                else:
                    pl.when(s == 1)(go)

                    @pl.when(s == 0)
                    def _(src=src):
                        pltpu.make_async_copy(src, dst, local_sem).start()

        def sent_back(t, ref, send):
            for d in range(n_x - 1):
                wait_for(ref, send.at[t * n_x + d])

            @pl.when(group_of(t) == 1)
            def _():
                wait_for(ref, send.at[t * n_x + n_x - 1])

        g_tile = n_x * cap // 2

        def group_rows(t, r):
            return h[pl.ds(pl.multiple_of((group_of(t) * 2 + r) * g_tile, 8), g_tile), :]

        def times(left, right):
            return lax.dot_general(left, right, (((1,), (1,)), ((), ())), preferred_element_type=F32).astype(BF16)

        my_rows = pl.ds(pl.multiple_of(cx * cap, 8), cap)

        def add_later(v, carry):
            with jax.named_scope("fetch_tail"):
                fetch(v)
            add_up(v)
            return carry

        def part(u, carry):
            i, m = place(u)
            slot = lax.rem(u, STAGES)
            is_mixed = u // 6 - u // 7
            buf = (1 - is_mixed) * m + is_mixed * 2
            other_core = jnp.logical_not(lead)

            @pl.when(jnp.logical_and(u >= STAGES, u < last - 1))
            def _():
                wait_for(stage.at[0, 0, pl.ds(0, cap), :], l_ret.at[slot])

            @pl.when(u == 0)
            def _():
                take(0, 1)
                load_main(u + 1)
                take(0, 2)
                load_rest(0)

            @pl.when(jnp.logical_and(u == 1, other_core))
            def _():
                take(1, 0)

            @pl.when(jnp.logical_and(u == 2, other_core))
            def _():
                take(1, 1)

            @pl.when(jnp.logical_and(u == 2, lead))
            def _():
                take(2, 0)

            @pl.when(jnp.logical_and(u == 3, lead))
            def _():
                with jax.named_scope("take_11a"):
                    take(1, 1)
                    load_main(u)

            @pl.when(jnp.logical_and(u == 3, other_core))
            def _():
                take(1, 2)

            @pl.when(jnp.logical_and(u == 4, other_core))
            def _():
                for k in range(3):
                    remote(wd_rows(1, k), wd_rows(1, k), t_a.at[k], r_wd.at[3, k], inner_dev).start()

            @pl.when(u == 4)
            def _():
                load_rest(1)

            @pl.when(jnp.logical_and(u == 5, other_core))
            def _():
                with jax.named_scope("take_21b"):
                    take(2, 1)
                    load_main(u)

            @pl.when(jnp.logical_and(u == 5, lead))
            def _():
                take(2, 2)

            @pl.when(u == 7)
            def _():
                with jax.named_scope("add45"):
                    lax.fori_loop(4, 6, add_later, 0)

            @pl.when(u == 8)
            def _():
                with jax.named_scope("add6"):
                    lax.fori_loop(6, 7, add_later, 0)

            @pl.when(jnp.logical_or(u == 7, u == 8))
            def _():
                with jax.named_scope("take_late"):
                    take(3, m)
                    load_main(u)

            @pl.when(u != mixed)
            def _():
                with jax.named_scope("wdload"):
                    wait_for(wdv.at[0], l_wd.at[m])

            @pl.when(u == mixed)
            def _():
                with jax.named_scope("restload"):
                    wait_for(wdv.at[2, pl.ds(0, 3 * rest), :], l_wd.at[2])

            def middle():
                @pl.when(jnp.logical_and(u == 1, lead))
                def _():
                    take(1, 0)

                @pl.when(u == 1)
                def _():
                    load_main(u + 1)

                @pl.when(jnp.logical_and(u == 2, other_core))
                def _():
                    load_main(u + 1)

                @pl.when(jnp.logical_and(u == 3, lead))
                def _():
                    take(1, 2)

                @pl.when(jnp.logical_and(u == 3, other_core))
                def _():
                    take(2, 0)

                @pl.when(u == 3)
                def _():
                    load_main(u + 1)

                @pl.when(jnp.logical_and(u == 4, lead))
                def _():
                    with jax.named_scope("take_21a"):
                        take(2, 1)
                        load_main(u + 1)

                @pl.when(jnp.logical_and(u == 5, other_core))
                def _():
                    take(2, 2)

                @pl.when(u == 5)
                def _():
                    load_rest(2)

                @pl.when(u == last - 1)
                def _():
                    take(3, 2)
                    load_rest(3)

                @pl.when(jnp.logical_and(u >= STAGES, u <= mixed))
                def _():
                    fetch(u - STAGES)

            def group(t, carry2):
                with jax.named_scope('middle'):
                    pl.when(t == 1)(middle)

                @pl.when(u >= STAGES)
                def _():
                    with jax.named_scope("sent_wait"):
                        sent_back(t, stage.at[0, 0, pl.ds(0, cap), :], s_ret.at[slot])

                def rows_of_group(r, carry3):
                    stage[slot, t, pl.ds(pl.multiple_of(r * g_tile, 8), g_tile), :] = times(group_rows(t, r), wdv[buf])
                    return carry3

                lax.fori_loop(0, 2, rows_of_group, 0)
                c = chunk(u, 0)
                send_back(t, stage.at[slot, t], back_ref.at[c, half, my_rows, :], s_ret.at[slot], r_back.at[c, half], l_ret.at[slot])
                return carry2

            with jax.named_scope("groups"):
                lax.fori_loop(0, 2, group, 0)

            @pl.when(jnp.logical_and(u >= STAGES, u <= mixed))
            def _():
                with jax.named_scope("add_up"):
                    add_up(u - STAGES)

            return carry

        lax.fori_loop(0, last, part, 0)
        wait_for(wdv.at[2, pl.ds(0, rest), :], l_wd.at[2])
        end_rows = pl.ds(pl.multiple_of(quarter(3) * rest, 8), rest)

        def end_group(t, carry):
            def rows_of_group(r, carry2):
                stage_end[t, pl.ds(pl.multiple_of(r * g_tile, 8), g_tile), :] = times(group_rows(t, r), wdv[2, end_rows, :])
                return carry2

            lax.fori_loop(0, 2, rows_of_group, 0)
            send_back(t, stage_end.at[t], end_ref.at[half, my_rows, :], s_ret.at[STAGES], r_end.at[half], l_ret.at[STAGES])
            return carry

        with jax.named_scope("end_groups"):
            lax.fori_loop(0, 2, end_group, 0)

        with jax.named_scope("add_tail"):
            lax.fori_loop(7, 9, add_later, 0)
        with jax.named_scope("add_end"):
            add_end()
        for qt in range(4):
            c0, held = qt * d_q + 2 * wk, pl.ds(qt * rest, rest)

            @pl.when(jnp.logical_and(quarter(3) != qt, quarter(2) != qt))
            def _(c0=c0, held=held):
                to_y(c0, rest, lambda r0: acc[4, pl.ds(r0, t_tile), held])

            for buf, i in ((0, 3), (1, 2)):

                @pl.when(quarter(i) == qt)
                def _(c0=c0, held=held, buf=buf):
                    to_y(c0, rest, lambda r0: acc[4, pl.ds(r0, t_tile), held] + acc[buf, pl.ds(r0, t_tile), pl.ds(0, rest)])

        store = pltpu.make_async_copy(y, y_ref, l_x.at[0])
        store.start()

        for k in range(STAGES):
            for t in range(2):
                sent_back(t, stage.at[0, 0, pl.ds(0, cap), :], s_ret.at[k])
        for t in range(2):
            sent_back(t, stage_end.at[0, pl.ds(0, cap), :], s_ret.at[STAGES])
        store.wait()

    pl.run_scoped(phase_up, pltpu.VMEM((rows, d_model), BF16), pltpu.VMEM((2, d_model, 2 * fc), BF16))
    pl.run_scoped(
        phase_down,
        pltpu.VMEM((3, wk, ffn), BF16),
        pltpu.VMEM((STAGES, 2, n_x * cap, wk), BF16),
        pltpu.VMEM((2, n_x * cap, rest), BF16),
        pltpu.VMEM((5, tok, wk), F32),
        pltpu.VMEM((2 * n_x, tok, cap), BF16),
        pltpu.VMEM((2, n_x * cap, wk), BF16),
        pltpu.VMEM((2, n_x * cap, rest), BF16),
        pltpu.VMEM((tok, d_model), BF16),
    )

    def drain_gu(k, carry):
        wait_for(gu_rows(k, 0), s_main.at[k])
        wait_for(gu_rows(k, 0), s_a.at[k])
        wait_for(gu_rows(k, 0), s_b.at[k])

        @pl.when(jnp.logical_not(lead))
        def _():
            wait_for(gu_rows(k, 0), s_c.at[k])

        return carry

    with jax.named_scope("drain"):
        lax.fori_loop(0, n_k, drain_gu, 0)

    for m in range(3):
        for sem in (t_main, t_a, t_b):
            wait_for(wd_rows(0, m), sem.at[m])

    @pl.when(jnp.logical_not(lead))
    def _():
        for m in range(3):
            wait_for(wd_rows(0, m), t_c.at[m])


def solution(mesh):
    n_group, n_y = mesh.shape["expert"], mesh.shape["data"]
    assert n_y == 4 and n_group % 2 == 0
    n_x = n_group // 2
    tok_spec = P(("rep", "expert", "data"), None)
    wide_spec = P("expert", "data", None)
    down_spec = P("expert", None, "data")

    def device_step(x_loc, idx_loc, gate_loc, wg_loc, wu_loc, wd_loc):
        tok, d_model = x_loc.shape
        n_local, d_q, ffn = wg_loc.shape
        assert n_local == 1 and n_group == 8 and d_q % 72 == 0
        cap = capacity_rows(tok, idx_loc.shape[1], n_group)
        fc = pick(ffn, (384, 256, 128))
        n_k, n_j = ffn // fc, pick(d_model // 128, (3, 2, 1))
        rows = 2 * n_x * cap
        tile = pick(rows, (1280, 48, 8))
        dims = (n_x, tok, d_model, d_q, ffn, cap, fc, n_k, n_j, tile)
        hbm = pl.BlockSpec(memory_space=pl.ANY)
        vmem = pl.BlockSpec(memory_space=pltpu.VMEM)
        dma = pltpu.SemaphoreType.DMA
        shape = jax.ShapeDtypeStruct
        outs = pl.pallas_call(
            functools.partial(moe_kernel, dims),
            name="moe_layer",
            out_shape=[
                shape((tok, d_model), BF16),
                shape((tok, d_model), BF16),
                shape((rows, d_model), BF16),
                shape((n_k, d_model, 2 * fc), BF16),
                shape((4, d_q, ffn), BF16),
                shape((9, 2, n_x * cap, d_q // 9 * 4), BF16),
                shape((2, n_x * cap, d_q // 9), BF16),
            ],
            in_specs=[vmem, vmem, hbm, hbm, hbm, hbm],
            out_specs=[hbm] * 7,
            scratch_shapes=[
                pltpu.VMEM((rows, ffn), BF16),
                pltpu.VMEM((8, tok), F32),
                pltpu.VMEM((8, tok), F32),
                pltpu.VMEM((tok, 128), F32),
                dma((n_j + 1,)), dma((n_j + 1,)), dma((n_x - 1,)), dma, dma((n_x - 1, n_j)), dma, dma((n_j + 1,)), dma((2,)),
                dma((n_k,)), dma((n_k,)), dma((n_k,)), dma((n_k,)), dma((4, n_k)), dma((2,)),
                dma((3,)), dma((3,)), dma((3,)), dma((3,)), dma((4, 3)), dma((3,)),
                dma((STAGES + 1, 2 * n_x)), dma((STAGES + 1,)), dma((9, 2)), dma((2,)), dma((2,)),
            ],
            compiler_params=pltpu.CompilerParams(collective_id=0, has_side_effects=True, vmem_limit_bytes=67_043_328),
        )(idx_loc.T, gate_loc.T, x_loc, wg_loc.reshape(d_q, ffn), wu_loc.reshape(d_q, ffn), wd_loc.reshape(ffn, d_q).T)
        return outs[0]

    return jax.shard_map(device_step, mesh=mesh, in_specs=(tok_spec, tok_spec, tok_spec, wide_spec, wide_spec, down_spec), out_specs=tok_spec, check_vma=False)
```

```python
import functools

import jax
import jax.numpy as jnp
from jax import lax
from jax.experimental import pallas as pl
from jax.experimental.pallas import tpu as pltpu
from jax.sharding import PartitionSpec as P

MESH = pl.DeviceIdType.MESH
F32 = jnp.float32
BF16 = jnp.bfloat16
LEAD = 3
EARLY = 14
LATE_STEP = 10
DOWN_STEP = 13
STAGES = 3


def capacity_rows(tok_rows, top_k, n_exp):
    return max(8, ((5 * top_k * tok_rows) // (4 * n_exp) + 7) // 8 * 8)


def pick(total, options):
    return next(c for c in options if total % c == 0)


def moe_kernel(dims, idx_ref, gate_ref, x_ref, wg_ref, wu_ref, wd_ref, y_ref, xpar_ref, xrows_ref, gu_ref, wdb_ref, back_ref, end_ref,
               h, keyt, keyt_par, tok_keys,
               s_x, r_x, s_own, r_own, s_par, r_par, l_loc, l_x,
               s_main, s_a, s_b, s_c, r_gu, l_w,
               t_main, t_a, t_b, t_c, r_wd, l_wd, s_ret, l_ret, r_back, r_end, l_back, l_end):
    n_x, tok, d_model, d_q, ffn, cap, fc, n_k, n_j, tile = dims
    rows = 2 * n_x * cap
    wk = d_q // 9 * 4
    rest = d_q - 2 * wk
    xc = d_model // n_j
    p = lax.axis_index("expert")
    q = lax.axis_index("data")
    cx, cc = p // 2, p % 2
    half = q // 2
    inner = q + 1 - 2 * (q % 2)
    outer = 3 - q
    lead = cc == half

    def dev(x, y, c):
        return {"expert": 2 * x + c, "data": y}

    def quarter(i):
        base = q + (i // 2) * (inner - q)
        return base + (i % 2) * (3 - 2 * base)

    partner = dev(cx, q, 1 - cc)
    inner_dev = dev(cx, inner, cc)
    outer_dev = dev(cx, outer, 1 - cc)
    mirror = dev(cx, outer, cc)

    def remote(src, dst, send, recv, device):
        return pltpu.make_async_remote_copy(src_ref=src, dst_ref=dst, send_sem=send, recv_sem=recv, device_id=device, device_id_type=MESH)

    def wait_for(ref, sem):
        pltpu.make_async_copy(ref, ref, sem).wait()

    barrier = pltpu.get_barrier_semaphore()
    peers = [partner, inner_dev, outer_dev]
    peers += [dev((cx + d) % n_x, q, cc) for d in range(1, n_x)]
    peers += [dev((cx + d) % n_x, outer, cc) for d in range(n_x)]
    for peer in peers:
        pl.semaphore_signal(barrier, inc=1, device_id=peer, device_id_type=MESH)
    pl.semaphore_wait(barrier, len(peers))

    def gu_rows(k, i):
        return gu_ref.at[k, pl.ds(quarter(i) * d_q, d_q), :]

    def send_own_gu(k, device, send, recv):
        src = pl.ds(pl.multiple_of(k * fc, 128), fc)
        for w_ref, c0 in ((wg_ref, 0), (wu_ref, fc)):
            remote(w_ref.at[:, src], gu_ref.at[k, pl.ds(q * d_q, d_q), pl.ds(c0, fc)], send, recv, device).start()

    def pass_gu(k, i, device, send, i_there):
        remote(gu_rows(k, i), gu_rows(k, i), send, r_gu.at[i_there, k], device).start()

    def send_block(j):
        cols = pl.ds(j * xc, xc)
        remote(x_ref.at[:, cols], xpar_ref.at[:, cols], s_x.at[j], r_x.at[j], mirror).start()

    def each(count, body):
        lax.fori_loop(0, count, lambda k, carry: (body(k), carry)[1], 0)

    send_block(0)

    early = min(EARLY, n_k)

    @pl.when(lead)
    def _():
        each(early, lambda k: send_own_gu(k, inner_dev, s_main.at[k], r_gu.at[2, k]))

    own_x = pltpu.make_async_copy(x_ref, h.at[pl.ds(0, tok), pl.ds(d_model, d_model)], l_x.at[0])
    own_x.start()
    expert = lax.broadcasted_iota(jnp.int32, (128, tok), 0)
    first = expert == idx_ref[0:1, :]
    second = expert == idx_ref[1:2, :]
    chosen = jnp.logical_or(first, second)
    before = lax.broadcasted_iota(jnp.int32, (tok, tok), 0) < lax.broadcasted_iota(jnp.int32, (tok, tok), 1)
    slot = jnp.dot(chosen.astype(F32).astype(BF16), before.astype(F32).astype(BF16), preferred_element_type=F32)
    key = jnp.where(jnp.logical_and(chosen, slot < cap), slot, -1.0)
    keyt[...] = key[:8, :]
    gates = jnp.where(expert - 8 == idx_ref[0:1, :], gate_ref[0:1, :], 0.0) + jnp.where(expert - 8 == idx_ref[1:2, :], gate_ref[1:2, :], 0.0)
    tok_keys[...] = jnp.where(expert < 8, key, gates).T
    send_key = remote(keyt, keyt_par, s_x.at[n_j], r_x.at[n_j], mirror)
    send_key.start()
    for j in range(1, n_j):
        send_block(j)

    @pl.when(jnp.logical_not(lead))
    def _():
        each(n_k, lambda k: send_own_gu(k, outer_dev, s_main.at[k], r_gu.at[1, k]))


    slots = lax.broadcasted_iota(jnp.int32, (cap, tok), 0).astype(F32)

    def select(keys, d):
        e = 2 * lax.rem(cx + d, n_x) + half
        return (slots == keys[pl.ds(e, 1), :]).astype(F32).astype(BF16)

    own_x.wait()

    def own_rows(t, carry):
        d = lax.rem(t + 1, n_x)
        pick_rows = select(keyt, d)
        stage = h.at[pl.ds(pl.multiple_of(t * cap, 8), cap), pl.ds(0, d_model)]
        for j in range(n_j):
            got = jnp.dot(pick_rows, h[pl.ds(0, tok), pl.ds(d_model + j * xc, xc)], preferred_element_type=F32)
            h[pl.ds(pl.multiple_of(t * cap, 8), cap), pl.ds(j * xc, xc)] = got.astype(BF16)
        dst = xrows_ref.at[pl.ds(pl.multiple_of(cx * cap, 8), cap), :]

        @pl.when(t < n_x - 1)
        def _():
            remote(stage, dst, s_own.at[t], r_own, dev(lax.rem(cx + d, n_x), q, cc)).start()

        @pl.when(t == n_x - 1)
        def _():
            pltpu.make_async_copy(stage, dst, l_loc.at[n_j]).start()

        return carry

    lax.fori_loop(0, n_x, own_rows, 0)

    def start_own_pass(k, carry):
        @pl.when(lead)
        def _():
            send_own_gu(k, partner, s_a.at[k], r_gu.at[0, k])

        return carry

    lax.fori_loop(0, n_k, start_own_pass, 0)

    send_key.wait()

    def par_cols(j, carry):
        cols = pl.ds(pl.multiple_of(j * xc, 128), xc)
        with jax.named_scope("par_wait"):
            wait_for(xpar_ref.at[:, cols], r_x.at[j])
        here = pl.ds(pl.multiple_of(d_model + j * xc, 128), xc)
        load = pltpu.make_async_copy(xpar_ref.at[:, cols], h.at[pl.ds(tok, tok), here], l_x.at[1])
        load.start()
        load.wait()

        def par_rows(t, carry2):
            d = lax.rem(t + 1, n_x)
            r0 = pl.multiple_of((n_x + t) * cap, 8)
            got = jnp.dot(select(keyt_par, d), h[pl.ds(tok, tok), here], preferred_element_type=F32)
            h[pl.ds(r0, cap), cols] = got.astype(BF16)
            stage = h.at[pl.ds(r0, cap), cols]
            dst = xrows_ref.at[pl.ds(pl.multiple_of((n_x + cx) * cap, 8), cap), cols]

            @pl.when(t < n_x - 1)
            def _():
                remote(stage, dst, s_par.at[t, j], r_par, dev(lax.rem(cx + d, n_x), q, cc)).start()

            @pl.when(t == n_x - 1)
            def _():
                pltpu.make_async_copy(stage, dst, l_loc.at[j]).start()

            return carry2

        return lax.fori_loop(0, n_x, par_rows, carry)

    lax.fori_loop(0, n_j, par_cols, 0)

    def ahead(k):
        @pl.when(lead)
        def _():
            wait_for(gu_rows(k, 2), r_gu.at[2, k])
            pass_gu(k, 2, partner, s_b.at[k], 2)

        @pl.when(jnp.logical_not(lead))
        def _():
            wait_for(gu_rows(k, 1), r_gu.at[1, k])
            pass_gu(k, 1, inner_dev, s_a.at[k], 3)
            pass_gu(k, 1, partner, s_b.at[k], 1)

    def part_rows(m):
        return pl.ds(2 * wk, d_q - 2 * wk) if isinstance(m, int) and m == 2 else pl.ds(m * wk if isinstance(m, int) else pl.multiple_of(m * wk, 8), wk)

    def wd_rows(i, m):
        return wdb_ref.at[quarter(i), part_rows(m), :]

    def send_own_wd(m, device, send, recv):
        remote(wd_ref.at[part_rows(m), :], wd_rows(0, m), send, recv, device).start()

    def phase_up(xr, wbuf):
        def gather_chunk(k, slot):
            @pl.when(lead)
            def _():
                wait_for(gu_rows(k, 1), r_gu.at[1, k])
                wait_for(gu_rows(k, 3), r_gu.at[3, k])
                src = pl.ds(pl.multiple_of(k * fc, 128), fc)
                for w_ref, c0 in ((wg_ref, 0), (wu_ref, fc)):
                    pltpu.make_async_copy(w_ref.at[:, src], wbuf.at[slot, pl.ds(q * d_q, d_q), pl.ds(c0, fc)], l_w.at[slot]).start()
                for i in (1, 2, 3):
                    pltpu.make_async_copy(gu_rows(k, i), wbuf.at[slot, pl.ds(quarter(i) * d_q, d_q), :], l_w.at[slot]).start()

            @pl.when(jnp.logical_not(lead))
            def _():
                wait_for(gu_rows(k, 3), r_gu.at[3, k])
                pass_gu(k, 3, partner, s_c.at[k], 3)
                wait_for(gu_rows(k, 0), r_gu.at[0, k])
                wait_for(gu_rows(k, 2), r_gu.at[2, k])
                pltpu.make_async_copy(gu_ref.at[k], wbuf.at[slot], l_w.at[slot]).start()

        with jax.named_scope("ahead_first"):
            for k in range(LEAD - 1):
                ahead(k)

        with jax.named_scope("rows_wait"):
            wait_for(xrows_ref.at[pl.ds(0, (n_x - 1) * cap), :], r_own)
            wait_for(xrows_ref.at[pl.ds(0, (n_x - 1) * cap), :], r_par)
            wait_for(xrows_ref.at[pl.ds(0, cap), :], l_loc.at[n_j])
            for j in range(n_j):
                wait_for(xrows_ref.at[pl.ds(0, cap), pl.ds(0, xc)], l_loc.at[j])
        load = pltpu.make_async_copy(xrows_ref, xr, l_x.at[0])
        load.start()

        def drain(t, carry):
            wait_for(xrows_ref.at[pl.ds(0, cap), :], s_own.at[t])

            def inner_drain(j, carry2):
                wait_for(xrows_ref.at[pl.ds(0, cap), pl.ds(0, xc)], s_par.at[t, j])
                return carry2

            return lax.fori_loop(0, n_j, inner_drain, carry)

        lax.fori_loop(0, n_x - 1, drain, 0)
        for j in range(n_j):
            wait_for(xpar_ref.at[:, pl.ds(0, xc)], s_x.at[j])

        @pl.when(lead)
        def _():
            for m in range(3):
                send_own_wd(m, partner, t_a.at[m], r_wd.at[0, m])

        @pl.when(jnp.logical_not(lead))
        def _():
            for m in range(3):
                send_own_wd(m, outer_dev, t_main.at[m], r_wd.at[1, m])

        with jax.named_scope("first_chunk"):
            ahead(LEAD - 1)
            gather_chunk(0, 0)
            load.wait()

        def step(k, carry):
            slot = lax.rem(k, 2)

            late = k - min(LATE_STEP, n_k - 1) + early

            @pl.when(jnp.logical_and(lead, jnp.logical_and(late >= early, late < n_k)))
            def _():
                send_own_gu(late, inner_dev, s_main.at[late], r_gu.at[2, late])

            @pl.when(jnp.logical_and(k == min(DOWN_STEP, n_k - 1), lead))
            def _():
                for m in range(3):
                    send_own_wd(m, inner_dev, t_main.at[m], r_wd.at[2, m])

            with jax.named_scope("wload"):
                wait_for(wbuf.at[slot], l_w.at[slot])

            def row_tile(r, carry2):
                @pl.when(jnp.logical_and(r == 1, k + LEAD < n_k))
                def _():
                    with jax.named_scope("ahead"):
                        ahead(k + LEAD)

                @pl.when(jnp.logical_and(r == 1, k + 1 < n_k))
                def _():
                    with jax.named_scope("gather"):
                        gather_chunk(k + 1, lax.rem(k + 1, 2))

                r0 = pl.multiple_of(r * tile, 8)
                both = jnp.dot(xr[pl.ds(r0, tile), :], wbuf[slot], preferred_element_type=F32)
                act = jax.nn.silu(both[:, :fc]) * both[:, fc:]
                h[pl.ds(r0, tile), pl.ds(pl.multiple_of(k * fc, 128), fc)] = act.astype(BF16)
                return carry2

            with jax.named_scope("mm"):
                lax.fori_loop(0, rows // tile, row_tile, 0)
            return carry

        lax.fori_loop(0, n_k, step, 0)

    def phase_down(wdv, stage, stage_end, acc, cmat, backv, backe, y):
        t_tile = min(512, tok)
        mixed, last = 6, 9

        def place(u):
            v = u - u // 7
            return v // 2, v % 2

        def chunk(u, other):
            i, m = place(u)
            qt = quarter(i)
            is_mixed = u // 6 - u // 7
            return (1 - is_mixed) * (2 * (qt + other * (3 - 2 * qt)) + m) + is_mixed * 8

        def take(i, m):
            @pl.when(jnp.logical_not(jnp.logical_and(lead, i == 0)))
            def _():
                wait_for(wd_rows(i, m), r_wd.at[i, m])

                @pl.when(jnp.logical_and(lead, i == 2))
                def _():
                    remote(wd_rows(i, m), wd_rows(i, m), t_b.at[m], r_wd.at[i, m], partner).start()

                @pl.when(jnp.logical_and(jnp.logical_not(lead), i == 1))
                def _():
                    remote(wd_rows(i, m), wd_rows(i, m), t_b.at[m], r_wd.at[i, m], partner).start()

                @pl.when(jnp.logical_and(jnp.logical_not(lead), i == 3))
                def _():
                    remote(wd_rows(i, m), wd_rows(i, m), t_c.at[m], r_wd.at[i, m], partner).start()

        def load(i, m, dst, sem):
            @pl.when(jnp.logical_and(lead, i == 0))
            def _():
                pltpu.make_async_copy(wd_ref.at[part_rows(m), :], dst, sem).start()

            @pl.when(jnp.logical_not(jnp.logical_and(lead, i == 0)))
            def _():
                pltpu.make_async_copy(wd_rows(i, m), dst, sem).start()

        def load_main(u):
            i, m = place(u)
            load(i, m, wdv.at[m], l_wd.at[m])

        def load_rest(i):
            load(i, 2, wdv.at[2, pl.ds(pl.multiple_of(quarter(i) * rest, 8), rest), :], l_wd.at[2])

        def combine(g, rows_of, old_of, put):
            def tok_tile(r, carry):
                r0 = pl.multiple_of(r * t_tile, 8)
                gates = tok_keys[pl.ds(r0, t_tile), :]
                lanes = lax.broadcasted_iota(jnp.int32, (t_tile, 128), 1)
                total = old_of(r0)
                for x in range(n_x):
                    e = 2 * x + g
                    rows_x = jnp.dot(cmat[e, pl.ds(r0, t_tile), :], rows_of(x), preferred_element_type=F32)
                    gate_x = jnp.sum(jnp.where(lanes == e + 8, gates, 0.0), axis=1, keepdims=True)
                    total = gate_x * rows_x if total is None else total + gate_x * rows_x
                put(r0, total)
                return carry

            lax.fori_loop(0, tok // t_tile, tok_tile, 0)

        def combine_main(a, g, add, buf):
            def put(r0, total):
                acc[a, pl.ds(r0, t_tile), :] = total

            combine(g, lambda x: backv[buf, pl.ds(x * cap, cap), :], lambda r0: acc[a, pl.ds(r0, t_tile), :] if add else None, put)

        def to_y(c0, width, extra_of):
            cols = pl.ds(c0, width)

            def tok_tile(r, carry):
                r0 = pl.multiple_of(r * t_tile, 8)
                y[pl.ds(r0, t_tile), cols] = (y[pl.ds(r0, t_tile), cols].astype(F32) + extra_of(r0)).astype(BF16)
                return carry

            lax.fori_loop(0, tok // t_tile, tok_tile, 0)

        def fetch(u):
            here, there = chunk(u, 0), chunk(u, 1)

            @pl.when(u >= last - STAGES - 1)
            def _():
                wait_for(stage.at[0, 0, pl.ds(0, cap), :], l_ret.at[lax.rem(u, STAGES)])

            wait_for(back_ref.at[0, 0, pl.ds(0, (n_x - 1) * cap), :], r_back.at[here, half])
            pltpu.make_async_copy(back_ref.at[here, half], backv.at[0], l_back.at[0]).start()
            wait_for(back_ref.at[0, 0], r_back.at[there, 1 - half])
            pltpu.make_async_copy(back_ref.at[there, 1 - half], backv.at[1], l_back.at[1]).start()

        def add_up(u):
            here, there = chunk(u, 0), chunk(u, 1)
            i, m = place(u)
            is_mixed = u // 6 - u // 7
            held_here = (1 - is_mixed) * (2 * (i % 2) + m) + is_mixed * 4
            held_there = (1 - is_mixed) * (2 - 2 * (i % 2) + m) + is_mixed * 4

            def both(add_first, add_second):
                wait_for(backv.at[0], l_back.at[0])
                combine_main(held_here, half, add_first, 0)
                wait_for(backv.at[1], l_back.at[1])
                combine_main(held_there, 1 - half, add_second, 1)

            @pl.when(u == mixed)
            def _():
                both(False, True)

            @pl.when(jnp.logical_and(u != mixed, i % 2 == 0))
            def _():
                both(False, False)

            @pl.when(jnp.logical_and(u != mixed, i % 2 == 1))
            def _():
                both(True, True)
                for c in range(8):

                    for c_done, held in ((here, held_here), (there, held_there)):

                        @pl.when(c_done == c)
                        def _(c=c, held=held):
                            to_y(c // 2 * d_q + c % 2 * wk, wk, lambda r0: acc[held, pl.ds(r0, t_tile), :])

        def fetch_end():
            wait_for(stage_end.at[0, pl.ds(0, cap), :], l_ret.at[STAGES])
            wait_for(end_ref.at[0, pl.ds(0, (n_x - 1) * cap), :], r_end.at[half])
            pltpu.make_async_copy(end_ref.at[half], backe.at[0], l_end.at[0]).start()
            wait_for(end_ref.at[0], r_end.at[1 - half])
            pltpu.make_async_copy(end_ref.at[1 - half], backe.at[1], l_end.at[1]).start()

        def add_end():
            for buf, g in ((0, half), (1, 1 - half)):
                wait_for(backe.at[buf], l_end.at[buf])

                def put(r0, total, buf=buf):
                    acc[buf, pl.ds(r0, t_tile), pl.ds(0, rest)] = total

                combine(g, lambda x, buf=buf: backe[buf, pl.ds(x * cap, cap), :], lambda r0: None, put)

        slot_lane = lax.broadcasted_iota(jnp.int32, (tok, cap), 1).astype(F32)
        for e in range(2 * n_x):
            cmat[e] = (slot_lane == tok_keys[:, e:e + 1]).astype(F32).astype(BF16)

        x_load = pltpu.make_async_copy(x_ref, y, l_x.at[0])
        x_load.start()
        take(0, 0)
        load_main(0)
        wdv[2, pl.ds(pl.multiple_of(quarter(3) * rest, 8), rest), :] = jnp.zeros((rest, ffn), BF16)
        x_load.wait()

        def group_of(t):
            return (t + 1 - cc) % 2

        def send_back(t, out_ref, dst, send, recv, local_sem):
            s = group_of(t)
            for d in range(n_x):
                x_src = lax.rem(cx + 1 + d, n_x)
                src = out_ref.at[pl.ds(pl.multiple_of(x_src * cap, 8), cap), :]

                def go(src=src, x_src=x_src, d=d):
                    remote(src, dst, send.at[t * n_x + d], recv, dev(x_src, q + s * (outer - q), cc)).start()

                if d < n_x - 1:
                    go()
                else:
                    pl.when(s == 1)(go)

                    @pl.when(s == 0)
                    def _(src=src):
                        pltpu.make_async_copy(src, dst, local_sem).start()

        def sent_back(t, ref, send):
            for d in range(n_x - 1):
                wait_for(ref, send.at[t * n_x + d])

            @pl.when(group_of(t) == 1)
            def _():
                wait_for(ref, send.at[t * n_x + n_x - 1])

        g_tile = n_x * cap // 2

        def group_rows(t, r):
            return h[pl.ds(pl.multiple_of((group_of(t) * 2 + r) * g_tile, 8), g_tile), :]

        def times(left, right):
            return lax.dot_general(left, right, (((1,), (1,)), ((), ())), preferred_element_type=F32).astype(BF16)

        my_rows = pl.ds(pl.multiple_of(cx * cap, 8), cap)

        def add_later(v, carry):
            with jax.named_scope("fetch_tail"):
                fetch(v)
            add_up(v)
            return carry

        def part(u, carry):
            i, m = place(u)
            slot = lax.rem(u, STAGES)
            is_mixed = u // 6 - u // 7
            buf = (1 - is_mixed) * m + is_mixed * 2
            other_core = jnp.logical_not(lead)

            @pl.when(jnp.logical_and(u >= STAGES, u < last - 1))
            def _():
                wait_for(stage.at[0, 0, pl.ds(0, cap), :], l_ret.at[slot])

            @pl.when(u == 0)
            def _():
                take(0, 1)
                load_main(u + 1)
                take(0, 2)
                load_rest(0)

            @pl.when(jnp.logical_and(u == 1, other_core))
            def _():
                take(1, 0)

            @pl.when(jnp.logical_and(u == 2, other_core))
            def _():
                take(1, 1)

            @pl.when(jnp.logical_and(u == 2, lead))
            def _():
                take(2, 0)

            @pl.when(jnp.logical_and(u == 3, lead))
            def _():
                with jax.named_scope("take_11a"):
                    take(1, 1)
                    load_main(u)

            @pl.when(jnp.logical_and(u == 3, other_core))
            def _():
                take(1, 2)

            @pl.when(jnp.logical_and(u == 4, other_core))
            def _():
                for k in range(3):
                    remote(wd_rows(1, k), wd_rows(1, k), t_a.at[k], r_wd.at[3, k], inner_dev).start()

            @pl.when(u == 4)
            def _():
                load_rest(1)

            @pl.when(jnp.logical_and(u == 5, other_core))
            def _():
                with jax.named_scope("take_21b"):
                    take(2, 1)
                    load_main(u)

            @pl.when(jnp.logical_and(u == 5, lead))
            def _():
                take(2, 2)

            @pl.when(u == 7)
            def _():
                with jax.named_scope("add45"):
                    lax.fori_loop(4, 5, add_later, 0)

            @pl.when(u == 8)
            def _():
                with jax.named_scope("add6"):
                    lax.fori_loop(5, 7, add_later, 0)

            @pl.when(jnp.logical_or(u == 7, u == 8))
            def _():
                with jax.named_scope("take_late"):
                    take(3, m)
                    load_main(u)

            @pl.when(u != mixed)
            def _():
                with jax.named_scope("wdload"):
                    wait_for(wdv.at[0], l_wd.at[m])

            @pl.when(u == mixed)
            def _():
                with jax.named_scope("restload"):
                    wait_for(wdv.at[2, pl.ds(0, 3 * rest), :], l_wd.at[2])

            def middle():
                @pl.when(jnp.logical_and(u == 1, lead))
                def _():
                    take(1, 0)

                @pl.when(u == 1)
                def _():
                    load_main(u + 1)

                @pl.when(jnp.logical_and(u == 2, other_core))
                def _():
                    load_main(u + 1)

                @pl.when(jnp.logical_and(u == 3, lead))
                def _():
                    take(1, 2)

                @pl.when(jnp.logical_and(u == 3, other_core))
                def _():
                    take(2, 0)

                @pl.when(u == 3)
                def _():
                    load_main(u + 1)

                @pl.when(jnp.logical_and(u == 4, lead))
                def _():
                    with jax.named_scope("take_21a"):
                        take(2, 1)
                        load_main(u + 1)

                @pl.when(jnp.logical_and(u == 5, other_core))
                def _():
                    take(2, 2)

                @pl.when(u == 5)
                def _():
                    load_rest(2)

                @pl.when(u == last - 1)
                def _():
                    take(3, 2)
                    load_rest(3)

                @pl.when(jnp.logical_and(u >= STAGES, u <= mixed))
                def _():
                    fetch(u - STAGES)

            def group(t, carry2):
                with jax.named_scope('middle'):
                    pl.when(t == 1)(middle)

                @pl.when(u >= STAGES)
                def _():
                    with jax.named_scope("sent_wait"):
                        sent_back(t, stage.at[0, 0, pl.ds(0, cap), :], s_ret.at[slot])

                def rows_of_group(r, carry3):
                    stage[slot, t, pl.ds(pl.multiple_of(r * g_tile, 8), g_tile), :] = times(group_rows(t, r), wdv[buf])
                    return carry3

                lax.fori_loop(0, 2, rows_of_group, 0)
                c = chunk(u, 0)
                send_back(t, stage.at[slot, t], back_ref.at[c, half, my_rows, :], s_ret.at[slot], r_back.at[c, half], l_ret.at[slot])
                return carry2

            with jax.named_scope("groups"):
                lax.fori_loop(0, 2, group, 0)

            @pl.when(jnp.logical_and(u >= STAGES, u <= mixed))
            def _():
                with jax.named_scope("add_up"):
                    add_up(u - STAGES)

            return carry

        lax.fori_loop(0, last, part, 0)
        wait_for(wdv.at[2, pl.ds(0, rest), :], l_wd.at[2])
        end_rows = pl.ds(pl.multiple_of(quarter(3) * rest, 8), rest)

        def end_group(t, carry):
            @pl.when(t == 1)
            def _():
                fetch(jnp.int32(7))

            def rows_of_group(r, carry2):
                stage_end[t, pl.ds(pl.multiple_of(r * g_tile, 8), g_tile), :] = times(group_rows(t, r), wdv[2, end_rows, :])
                return carry2

            lax.fori_loop(0, 2, rows_of_group, 0)
            send_back(t, stage_end.at[t], end_ref.at[half, my_rows, :], s_ret.at[STAGES], r_end.at[half], l_ret.at[STAGES])
            return carry

        with jax.named_scope("end_groups"):
            lax.fori_loop(0, 2, end_group, 0)

        with jax.named_scope("add_tail"):
            add_up(jnp.int32(7))
            fetch(jnp.int32(8))
            fetch_end()
            add_up(jnp.int32(8))
        with jax.named_scope("add_end"):
            add_end()
        for qt in range(4):
            c0, held = qt * d_q + 2 * wk, pl.ds(qt * rest, rest)

            @pl.when(jnp.logical_and(quarter(3) != qt, quarter(2) != qt))
            def _(c0=c0, held=held):
                to_y(c0, rest, lambda r0: acc[4, pl.ds(r0, t_tile), held])

            for buf, i in ((0, 3), (1, 2)):

                @pl.when(quarter(i) == qt)
                def _(c0=c0, held=held, buf=buf):
                    to_y(c0, rest, lambda r0: acc[4, pl.ds(r0, t_tile), held] + acc[buf, pl.ds(r0, t_tile), pl.ds(0, rest)])

        store = pltpu.make_async_copy(y, y_ref, l_x.at[0])
        store.start()

        for k in range(STAGES):
            for t in range(2):
                sent_back(t, stage.at[0, 0, pl.ds(0, cap), :], s_ret.at[k])
        for t in range(2):
            sent_back(t, stage_end.at[0, pl.ds(0, cap), :], s_ret.at[STAGES])
        store.wait()

    pl.run_scoped(phase_up, pltpu.VMEM((rows, d_model), BF16), pltpu.VMEM((2, d_model, 2 * fc), BF16))
    pl.run_scoped(
        phase_down,
        pltpu.VMEM((3, wk, ffn), BF16),
        pltpu.VMEM((STAGES, 2, n_x * cap, wk), BF16),
        pltpu.VMEM((2, n_x * cap, rest), BF16),
        pltpu.VMEM((5, tok, wk), F32),
        pltpu.VMEM((2 * n_x, tok, cap), BF16),
        pltpu.VMEM((2, n_x * cap, wk), BF16),
        pltpu.VMEM((2, n_x * cap, rest), BF16),
        pltpu.VMEM((tok, d_model), BF16),
    )

    def drain_gu(k, carry):
        wait_for(gu_rows(k, 0), s_main.at[k])
        wait_for(gu_rows(k, 0), s_a.at[k])
        wait_for(gu_rows(k, 0), s_b.at[k])

        @pl.when(jnp.logical_not(lead))
        def _():
            wait_for(gu_rows(k, 0), s_c.at[k])

        return carry

    with jax.named_scope("drain"):
        lax.fori_loop(0, n_k, drain_gu, 0)

    for m in range(3):
        for sem in (t_main, t_a, t_b):
            wait_for(wd_rows(0, m), sem.at[m])

    @pl.when(jnp.logical_not(lead))
    def _():
        for m in range(3):
            wait_for(wd_rows(0, m), t_c.at[m])


def solution(mesh):
    n_group, n_y = mesh.shape["expert"], mesh.shape["data"]
    assert n_y == 4 and n_group % 2 == 0
    n_x = n_group // 2
    tok_spec = P(("rep", "expert", "data"), None)
    wide_spec = P("expert", "data", None)
    down_spec = P("expert", None, "data")

    def device_step(x_loc, idx_loc, gate_loc, wg_loc, wu_loc, wd_loc):
        tok, d_model = x_loc.shape
        n_local, d_q, ffn = wg_loc.shape
        assert n_local == 1 and n_group == 8 and d_q % 72 == 0
        cap = capacity_rows(tok, idx_loc.shape[1], n_group)
        fc = pick(ffn, (384, 256, 128))
        n_k, n_j = ffn // fc, pick(d_model // 128, (3, 2, 1))
        rows = 2 * n_x * cap
        tile = pick(rows, (1280, 48, 8))
        dims = (n_x, tok, d_model, d_q, ffn, cap, fc, n_k, n_j, tile)
        hbm = pl.BlockSpec(memory_space=pl.ANY)
        vmem = pl.BlockSpec(memory_space=pltpu.VMEM)
        dma = pltpu.SemaphoreType.DMA
        shape = jax.ShapeDtypeStruct
        outs = pl.pallas_call(
            functools.partial(moe_kernel, dims),
            name="moe_layer",
            out_shape=[
                shape((tok, d_model), BF16),
                shape((tok, d_model), BF16),
                shape((rows, d_model), BF16),
                shape((n_k, d_model, 2 * fc), BF16),
                shape((4, d_q, ffn), BF16),
                shape((9, 2, n_x * cap, d_q // 9 * 4), BF16),
                shape((2, n_x * cap, d_q // 9), BF16),
            ],
            in_specs=[vmem, vmem, hbm, hbm, hbm, hbm],
            out_specs=[hbm] * 7,
            scratch_shapes=[
                pltpu.VMEM((rows, ffn), BF16),
                pltpu.VMEM((8, tok), F32),
                pltpu.VMEM((8, tok), F32),
                pltpu.VMEM((tok, 128), F32),
                dma((n_j + 1,)), dma((n_j + 1,)), dma((n_x - 1,)), dma, dma((n_x - 1, n_j)), dma, dma((n_j + 1,)), dma((2,)),
                dma((n_k,)), dma((n_k,)), dma((n_k,)), dma((n_k,)), dma((4, n_k)), dma((2,)),
                dma((3,)), dma((3,)), dma((3,)), dma((3,)), dma((4, 3)), dma((3,)),
                dma((STAGES + 1, 2 * n_x)), dma((STAGES + 1,)), dma((9, 2)), dma((2,)), dma((2,)), dma((2,)),
            ],
            compiler_params=pltpu.CompilerParams(collective_id=0, has_side_effects=True, vmem_limit_bytes=67_043_328),
        )(idx_loc.T, gate_loc.T, x_loc, wg_loc.reshape(d_q, ffn), wu_loc.reshape(d_q, ffn), wd_loc.reshape(ffn, d_q).T)
        return outs[0]

    return jax.shard_map(device_step, mesh=mesh, in_specs=(tok_spec, tok_spec, tok_spec, wide_spec, wide_spec, down_spec), out_specs=tok_spec, check_vma=False)
```

```python
import functools

import jax
import jax.numpy as jnp
from jax import lax
from jax.experimental import pallas as pl
from jax.experimental.pallas import tpu as pltpu
from jax.sharding import PartitionSpec as P

MESH = pl.DeviceIdType.MESH
F32 = jnp.float32
BF16 = jnp.bfloat16
LEAD = 3
EARLY = 13
LATE_STEP = 6
DOWN_STEP = 13
STAGES = 3


def capacity_rows(tok_rows, top_k, n_exp):
    return max(8, ((5 * top_k * tok_rows) // (4 * n_exp) + 7) // 8 * 8)


def pick(total, options):
    return next(c for c in options if total % c == 0)


def moe_kernel(dims, idx_ref, gate_ref, x_ref, wg_ref, wu_ref, wd_ref, y_ref, xpar_ref, xrows_ref, gu_ref, wdb_ref, back_ref, end_ref,
               h, keyt, keyt_par, tok_keys,
               s_x, r_x, s_own, r_own, s_par, r_par, l_loc, l_x,
               s_main, s_a, s_b, s_c, r_gu, l_w,
               t_main, t_a, t_b, t_c, r_wd, l_wd, s_ret, l_ret, r_back, r_end, l_back, l_end):
    n_x, tok, d_model, d_q, ffn, cap, fc, n_k, n_j, tile = dims
    rows = 2 * n_x * cap
    wk = d_q // 9 * 4
    rest = d_q - 2 * wk
    quarters, parts3 = range(4), range(3)
    xc = d_model // n_j
    p = lax.axis_index("expert")
    q = lax.axis_index("data")
    cx, cc = p // 2, p % 2
    half = q // 2
    inner = q + 1 - 2 * (q % 2)
    outer = 3 - q
    lead = cc == half

    def dev(x, y, c):
        return {"expert": 2 * x + c, "data": y}

    def quarter(i):
        base = q + (i // 2) * (inner - q)
        return base + (i % 2) * (3 - 2 * base)

    partner = dev(cx, q, 1 - cc)
    inner_dev = dev(cx, inner, cc)
    outer_dev = dev(cx, outer, 1 - cc)
    mirror = dev(cx, outer, cc)

    def remote(src, dst, send, recv, device):
        return pltpu.make_async_remote_copy(src_ref=src, dst_ref=dst, send_sem=send, recv_sem=recv, device_id=device, device_id_type=MESH)

    def wait_for(ref, sem):
        pltpu.make_async_copy(ref, ref, sem).wait()

    barrier = pltpu.get_barrier_semaphore()
    peers = [partner, inner_dev, outer_dev]
    peers += [dev((cx + d) % n_x, q, cc) for d in range(1, n_x)]
    peers += [dev((cx + d) % n_x, outer, cc) for d in range(n_x)]
    for peer in peers:
        pl.semaphore_signal(barrier, inc=1, device_id=peer, device_id_type=MESH)
    pl.semaphore_wait(barrier, len(peers))

    def gu_rows(k, i):
        return gu_ref.at[k, pl.ds(quarter(i) * d_q, d_q), :]

    def send_own_gu(k, device, send, recv):
        src = pl.ds(pl.multiple_of(k * fc, 128), fc)
        for w_ref, c0 in ((wg_ref, 0), (wu_ref, fc)):
            remote(w_ref.at[:, src], gu_ref.at[k, pl.ds(q * d_q, d_q), pl.ds(c0, fc)], send, recv, device).start()

    def pass_gu(k, i, device, send, i_there):
        remote(gu_rows(k, i), gu_rows(k, i), send, r_gu.at[i_there, k], device).start()

    def send_block(j):
        cols = pl.ds(j * xc, xc)
        remote(x_ref.at[:, cols], xpar_ref.at[:, cols], s_x.at[j], r_x.at[j], mirror).start()

    def each(count, body):
        lax.fori_loop(0, count, lambda k, carry: (body(k), carry)[1], 0)

    send_block(0)

    early = min(EARLY, n_k)

    @pl.when(lead)
    def _():
        each(early, lambda k: send_own_gu(k, inner_dev, s_main.at[k], r_gu.at[2, k]))

    own_x = pltpu.make_async_copy(x_ref, h.at[pl.ds(0, tok), pl.ds(d_model, d_model)], l_x.at[0])
    own_x.start()
    expert = lax.broadcasted_iota(jnp.int32, (128, tok), 0)
    first = expert == idx_ref[0:1, :]
    second = expert == idx_ref[1:2, :]
    chosen = jnp.logical_or(first, second)
    before = lax.broadcasted_iota(jnp.int32, (tok, tok), 0) < lax.broadcasted_iota(jnp.int32, (tok, tok), 1)
    slot = jnp.dot(chosen.astype(F32).astype(BF16), before.astype(F32).astype(BF16), preferred_element_type=F32)
    key = jnp.where(jnp.logical_and(chosen, slot < cap), slot, -1.0)
    keyt[...] = key[:8, :]
    gates = jnp.where(expert - 8 == idx_ref[0:1, :], gate_ref[0:1, :], 0.0) + jnp.where(expert - 8 == idx_ref[1:2, :], gate_ref[1:2, :], 0.0)
    tok_keys[...] = jnp.where(expert < 8, key, gates).T
    send_key = remote(keyt, keyt_par, s_x.at[n_j], r_x.at[n_j], mirror)
    send_key.start()
    for j in range(1, n_j):
        send_block(j)

    @pl.when(jnp.logical_not(lead))
    def _():
        each(n_k, lambda k: send_own_gu(k, outer_dev, s_main.at[k], r_gu.at[1, k]))


    slots = lax.broadcasted_iota(jnp.int32, (cap, tok), 0).astype(F32)

    def select(keys, d):
        e = 2 * lax.rem(cx + d, n_x) + half
        return (slots == keys[pl.ds(e, 1), :]).astype(F32).astype(BF16)

    own_x.wait()

    def own_rows(t, carry):
        d = lax.rem(t + 1, n_x)
        pick_rows = select(keyt, d)
        stage = h.at[pl.ds(pl.multiple_of(t * cap, 8), cap), pl.ds(0, d_model)]
        for j in range(n_j):
            got = jnp.dot(pick_rows, h[pl.ds(0, tok), pl.ds(d_model + j * xc, xc)], preferred_element_type=F32)
            h[pl.ds(pl.multiple_of(t * cap, 8), cap), pl.ds(j * xc, xc)] = got.astype(BF16)
        dst = xrows_ref.at[pl.ds(pl.multiple_of(cx * cap, 8), cap), :]

        @pl.when(t < n_x - 1)
        def _():
            remote(stage, dst, s_own.at[t], r_own, dev(lax.rem(cx + d, n_x), q, cc)).start()

        @pl.when(t == n_x - 1)
        def _():
            pltpu.make_async_copy(stage, dst, l_loc.at[n_j]).start()

        return carry

    lax.fori_loop(0, n_x, own_rows, 0)

    def start_own_pass(k, carry):
        @pl.when(lead)
        def _():
            send_own_gu(k, partner, s_a.at[k], r_gu.at[0, k])

        return carry

    lax.fori_loop(0, n_k, start_own_pass, 0)

    send_key.wait()

    def par_cols(j, carry):
        cols = pl.ds(pl.multiple_of(j * xc, 128), xc)
        wait_for(xpar_ref.at[:, cols], r_x.at[j])
        here = pl.ds(pl.multiple_of(d_model + j * xc, 128), xc)
        load = pltpu.make_async_copy(xpar_ref.at[:, cols], h.at[pl.ds(tok, tok), here], l_x.at[1])
        load.start()
        load.wait()

        def par_rows(t, carry2):
            d = lax.rem(t + 1, n_x)
            r0 = pl.multiple_of((n_x + t) * cap, 8)
            got = jnp.dot(select(keyt_par, d), h[pl.ds(tok, tok), here], preferred_element_type=F32)
            h[pl.ds(r0, cap), cols] = got.astype(BF16)
            stage = h.at[pl.ds(r0, cap), cols]
            dst = xrows_ref.at[pl.ds(pl.multiple_of((n_x + cx) * cap, 8), cap), cols]

            @pl.when(t < n_x - 1)
            def _():
                remote(stage, dst, s_par.at[t, j], r_par, dev(lax.rem(cx + d, n_x), q, cc)).start()

            @pl.when(t == n_x - 1)
            def _():
                pltpu.make_async_copy(stage, dst, l_loc.at[j]).start()

            return carry2

        return lax.fori_loop(0, n_x, par_rows, carry)

    lax.fori_loop(0, n_j, par_cols, 0)

    def ahead(k):
        @pl.when(lead)
        def _():
            wait_for(gu_rows(k, 2), r_gu.at[2, k])
            pass_gu(k, 2, partner, s_b.at[k], 2)

        @pl.when(jnp.logical_not(lead))
        def _():
            wait_for(gu_rows(k, 1), r_gu.at[1, k])
            pass_gu(k, 1, inner_dev, s_a.at[k], 3)
            pass_gu(k, 1, partner, s_b.at[k], 1)

    def part_rows(m):
        return pl.ds(2 * wk, d_q - 2 * wk) if isinstance(m, int) and m == 2 else pl.ds(m * wk if isinstance(m, int) else pl.multiple_of(m * wk, 8), wk)

    def wd_rows(i, m):
        return wdb_ref.at[quarter(i), part_rows(m), :]

    def send_own_wd(m, device, send, recv):
        remote(wd_ref.at[part_rows(m), :], wd_rows(0, m), send, recv, device).start()

    def phase_up(xr, wbuf):
        def gather_chunk(k, slot):
            @pl.when(lead)
            def _():
                wait_for(gu_rows(k, 1), r_gu.at[1, k])
                wait_for(gu_rows(k, 3), r_gu.at[3, k])
                src = pl.ds(pl.multiple_of(k * fc, 128), fc)
                for w_ref, c0 in ((wg_ref, 0), (wu_ref, fc)):
                    pltpu.make_async_copy(w_ref.at[:, src], wbuf.at[slot, pl.ds(q * d_q, d_q), pl.ds(c0, fc)], l_w.at[slot]).start()
                for i in (1, 2, 3):
                    pltpu.make_async_copy(gu_rows(k, i), wbuf.at[slot, pl.ds(quarter(i) * d_q, d_q), :], l_w.at[slot]).start()

            @pl.when(jnp.logical_not(lead))
            def _():
                wait_for(gu_rows(k, 3), r_gu.at[3, k])
                pass_gu(k, 3, partner, s_c.at[k], 3)
                wait_for(gu_rows(k, 0), r_gu.at[0, k])
                wait_for(gu_rows(k, 2), r_gu.at[2, k])
                pltpu.make_async_copy(gu_ref.at[k], wbuf.at[slot], l_w.at[slot]).start()

        for k in range(LEAD - 1):
            ahead(k)

        wait_for(xrows_ref.at[pl.ds(0, (n_x - 1) * cap), :], r_own)
        wait_for(xrows_ref.at[pl.ds(0, (n_x - 1) * cap), :], r_par)
        wait_for(xrows_ref.at[pl.ds(0, cap), :], l_loc.at[n_j])
        for j in range(n_j):
            wait_for(xrows_ref.at[pl.ds(0, cap), pl.ds(0, xc)], l_loc.at[j])
        load = pltpu.make_async_copy(xrows_ref, xr, l_x.at[0])
        load.start()

        def drain(t, carry):
            wait_for(xrows_ref.at[pl.ds(0, cap), :], s_own.at[t])

            def inner_drain(j, carry2):
                wait_for(xrows_ref.at[pl.ds(0, cap), pl.ds(0, xc)], s_par.at[t, j])
                return carry2

            return lax.fori_loop(0, n_j, inner_drain, carry)

        lax.fori_loop(0, n_x - 1, drain, 0)
        for j in range(n_j):
            wait_for(xpar_ref.at[:, pl.ds(0, xc)], s_x.at[j])

        @pl.when(lead)
        def _():
            for m in parts3:
                send_own_wd(m, partner, t_a.at[m], r_wd.at[0, m])

        @pl.when(jnp.logical_not(lead))
        def _():
            for m in parts3:
                send_own_wd(m, outer_dev, t_main.at[m], r_wd.at[1, m])

        ahead(LEAD - 1)
        gather_chunk(0, 0)
        load.wait()

        def step(k, carry):
            slot = lax.rem(k, 2)

            late = k - min(LATE_STEP, n_k - 1) + early

            @pl.when(jnp.logical_and(lead, jnp.logical_and(late >= early, late < n_k)))
            def _():
                send_own_gu(late, inner_dev, s_main.at[late], r_gu.at[2, late])

            @pl.when(jnp.logical_and(k == min(DOWN_STEP, n_k - 1), lead))
            def _():
                for m in parts3:
                    send_own_wd(m, inner_dev, t_main.at[m], r_wd.at[2, m])

            wait_for(wbuf.at[slot], l_w.at[slot])

            def row_tile(r, carry2):
                @pl.when(jnp.logical_and(r == 1, k + LEAD < n_k))
                def _():
                    ahead(k + LEAD)

                @pl.when(jnp.logical_and(r == 1, k + 1 < n_k))
                def _():
                    gather_chunk(k + 1, lax.rem(k + 1, 2))

                r0 = pl.multiple_of(r * tile, 8)
                both = jnp.dot(xr[pl.ds(r0, tile), :], wbuf[slot], preferred_element_type=F32)
                act = jax.nn.silu(both[:, :fc]) * both[:, fc:]
                h[pl.ds(r0, tile), pl.ds(pl.multiple_of(k * fc, 128), fc)] = act.astype(BF16)
                return carry2

            lax.fori_loop(0, rows // tile, row_tile, 0)
            return carry

        lax.fori_loop(0, n_k, step, 0)

    def phase_down(wdv, stage, stage_end, acc, cmat, backv, backe, y):
        t_tile = min(512, tok)
        mixed, last = 6, 9
        one_block = stage.at[0, 0, pl.ds(0, cap), :]
        part_far = back_ref.at[0, 0]
        part_near = part_far.at[pl.ds(0, (n_x - 1) * cap), :]

        def place(u):
            v = u - u // 7
            return v // 2, v % 2

        def chunk(u, other):
            i, m = place(u)
            qt = quarter(i)
            is_mixed = u // 6 - u // 7
            return (1 - is_mixed) * (2 * (qt + other * (3 - 2 * qt)) + m) + is_mixed * 8

        def take(i, m):
            @pl.when(jnp.logical_not(jnp.logical_and(lead, i == 0)))
            def _():
                wait_for(wd_rows(i, m), r_wd.at[i, m])

                @pl.when(jnp.logical_and(lead, i == 2))
                def _():
                    remote(wd_rows(i, m), wd_rows(i, m), t_b.at[m], r_wd.at[i, m], partner).start()

                @pl.when(jnp.logical_and(jnp.logical_not(lead), i == 1))
                def _():
                    remote(wd_rows(i, m), wd_rows(i, m), t_b.at[m], r_wd.at[i, m], partner).start()

                @pl.when(jnp.logical_and(jnp.logical_not(lead), i == 3))
                def _():
                    remote(wd_rows(i, m), wd_rows(i, m), t_c.at[m], r_wd.at[i, m], partner).start()

        def load(i, m, dst, sem):
            @pl.when(jnp.logical_and(lead, i == 0))
            def _():
                pltpu.make_async_copy(wd_ref.at[part_rows(m), :], dst, sem).start()

            @pl.when(jnp.logical_not(jnp.logical_and(lead, i == 0)))
            def _():
                pltpu.make_async_copy(wd_rows(i, m), dst, sem).start()

        def load_main(u):
            i, m = place(u)
            load(i, m, wdv.at[m], l_wd.at[m])

        def load_rest(i):
            load(i, 2, wdv.at[2, pl.ds(pl.multiple_of(quarter(i) * rest, 8), rest), :], l_wd.at[2])

        def combine(g, rows_of, old_of, put):
            def tok_tile(r, carry):
                r0 = pl.multiple_of(r * t_tile, 8)
                gates = tok_keys[pl.ds(r0, t_tile), :]
                lanes = lax.broadcasted_iota(jnp.int32, (t_tile, 128), 1)
                total = old_of(r0)
                for x in range(n_x):
                    e = 2 * x + g
                    rows_x = jnp.dot(cmat[e, pl.ds(r0, t_tile), :], rows_of(x), preferred_element_type=F32)
                    gate_x = jnp.sum(jnp.where(lanes == e + 8, gates, 0.0), axis=1, keepdims=True)
                    total = gate_x * rows_x if total is None else total + gate_x * rows_x
                put(r0, total)
                return carry

            lax.fori_loop(0, tok // t_tile, tok_tile, 0)

        def combine_main(a, g, add, buf):
            def put(r0, total):
                acc[a, pl.ds(r0, t_tile), :] = total

            combine(g, lambda x: backv[buf, pl.ds(x * cap, cap), :], lambda r0: acc[a, pl.ds(r0, t_tile), :] if add else None, put)

        def to_y(c0, width, extra_of):
            cols = pl.ds(c0, width)

            def tok_tile(r, carry):
                r0 = pl.multiple_of(r * t_tile, 8)
                y[pl.ds(r0, t_tile), cols] = (y[pl.ds(r0, t_tile), cols].astype(F32) + extra_of(r0)).astype(BF16)
                return carry

            lax.fori_loop(0, tok // t_tile, tok_tile, 0)

        def fetch(u):
            here, there = chunk(u, 0), chunk(u, 1)

            @pl.when(u >= last - STAGES - 1)
            def _():
                wait_for(one_block, l_ret.at[lax.rem(u, STAGES)])

            wait_for(part_near, r_back.at[here, half])
            pltpu.make_async_copy(back_ref.at[here, half], backv.at[0], l_back.at[0]).start()
            wait_for(part_far, r_back.at[there, 1 - half])
            pltpu.make_async_copy(back_ref.at[there, 1 - half], backv.at[1], l_back.at[1]).start()

        def add_up(u):
            here, there = chunk(u, 0), chunk(u, 1)
            i, m = place(u)
            is_mixed = u // 6 - u // 7
            held_here = (1 - is_mixed) * (2 * (i % 2) + m) + is_mixed * 4
            held_there = (1 - is_mixed) * (2 - 2 * (i % 2) + m) + is_mixed * 4

            def both(add_first, add_second):
                wait_for(backv.at[0], l_back.at[0])
                combine_main(held_here, half, add_first, 0)
                wait_for(backv.at[1], l_back.at[1])
                combine_main(held_there, 1 - half, add_second, 1)

            @pl.when(u == mixed)
            def _():
                both(False, True)

            @pl.when(jnp.logical_and(u != mixed, i % 2 == 0))
            def _():
                both(False, False)

            @pl.when(jnp.logical_and(u != mixed, i % 2 == 1))
            def _():
                both(True, True)
                for c in range(8):

                    for c_done, held in ((here, held_here), (there, held_there)):

                        @pl.when(c_done == c)
                        def _(c=c, held=held):
                            to_y(c // 2 * d_q + c % 2 * wk, wk, lambda r0: acc[held, pl.ds(r0, t_tile), :])

        def fetch_end():
            wait_for(stage_end.at[0, pl.ds(0, cap), :], l_ret.at[STAGES])
            wait_for(end_ref.at[0, pl.ds(0, (n_x - 1) * cap), :], r_end.at[half])
            pltpu.make_async_copy(end_ref.at[half], backe.at[0], l_end.at[0]).start()
            wait_for(end_ref.at[0], r_end.at[1 - half])
            pltpu.make_async_copy(end_ref.at[1 - half], backe.at[1], l_end.at[1]).start()

        def add_end():
            for buf, g in ((0, half), (1, 1 - half)):
                wait_for(backe.at[buf], l_end.at[buf])

                def put(r0, total, buf=buf):
                    acc[buf, pl.ds(r0, t_tile), pl.ds(0, rest)] = total

                combine(g, lambda x, buf=buf: backe[buf, pl.ds(x * cap, cap), :], lambda r0: None, put)

        slot_lane = lax.broadcasted_iota(jnp.int32, (tok, cap), 1).astype(F32)
        for e in range(2 * n_x):
            cmat[e] = (slot_lane == tok_keys[:, e:e + 1]).astype(F32).astype(BF16)

        x_load = pltpu.make_async_copy(x_ref, y, l_x.at[0])
        x_load.start()
        take(0, 0)
        load_main(0)
        wdv[2, pl.ds(pl.multiple_of(quarter(3) * rest, 8), rest), :] = jnp.zeros((rest, ffn), BF16)
        x_load.wait()

        def group_of(t):
            return (t + 1 - cc) % 2

        def send_back(t, out_ref, dst, send, recv, local_sem):
            s = group_of(t)
            for d in range(n_x):
                x_src = lax.rem(cx + 1 + d, n_x)
                src = out_ref.at[pl.ds(pl.multiple_of(x_src * cap, 8), cap), :]

                def go(src=src, x_src=x_src, d=d):
                    remote(src, dst, send.at[t * n_x + d], recv, dev(x_src, q + s * (outer - q), cc)).start()

                if d < n_x - 1:
                    go()
                else:
                    pl.when(s == 1)(go)

                    @pl.when(s == 0)
                    def _(src=src):
                        pltpu.make_async_copy(src, dst, local_sem).start()

        def sent_back(t, ref, send):
            for d in range(n_x - 1):
                wait_for(ref, send.at[t * n_x + d])

            @pl.when(group_of(t) == 1)
            def _():
                wait_for(ref, send.at[t * n_x + n_x - 1])

        g_tile = n_x * cap // 2
        end_block = stage_end.at[0, pl.ds(0, cap), :]

        def group_rows(t, r):
            return h[pl.ds(pl.multiple_of((group_of(t) * 2 + r) * g_tile, 8), g_tile), :]

        def times(left, right):
            return lax.dot_general(left, right, (((1,), (1,)), ((), ())), preferred_element_type=F32).astype(BF16)

        my_rows = pl.ds(pl.multiple_of(cx * cap, 8), cap)

        def add_later(v, carry):
            fetch(v)
            add_up(v)
            return carry

        def part(u, carry):
            i, m = place(u)
            slot = lax.rem(u, STAGES)
            is_mixed = u // 6 - u // 7
            buf = (1 - is_mixed) * m + is_mixed * 2
            other_core = jnp.logical_not(lead)

            @pl.when(jnp.logical_and(u >= STAGES, u < last - 1))
            def _():
                wait_for(one_block, l_ret.at[slot])

            @pl.when(u == 0)
            def _():
                take(0, 1)
                load_main(u + 1)
                take(0, 2)
                load_rest(0)

            @pl.when(jnp.logical_and(u == 1, other_core))
            def _():
                take(1, 0)

            @pl.when(jnp.logical_and(u == 2, other_core))
            def _():
                take(1, 1)

            @pl.when(jnp.logical_and(u == 2, lead))
            def _():
                take(2, 0)

            @pl.when(jnp.logical_and(u == 3, lead))
            def _():
                take(1, 1)
                load_main(u)

            @pl.when(jnp.logical_and(u == 3, other_core))
            def _():
                take(1, 2)

            @pl.when(jnp.logical_and(u == 4, other_core))
            def _():
                for k in parts3:
                    remote(wd_rows(1, k), wd_rows(1, k), t_a.at[k], r_wd.at[3, k], inner_dev).start()

            @pl.when(u == 4)
            def _():
                load_rest(1)

            @pl.when(jnp.logical_and(u == 5, other_core))
            def _():
                take(2, 1)
                load_main(u)

            @pl.when(jnp.logical_and(u == 5, lead))
            def _():
                take(2, 2)

            @pl.when(u == 7)
            def _():
                lax.fori_loop(4, 5, add_later, 0)

            @pl.when(u == 8)
            def _():
                lax.fori_loop(5, 7, add_later, 0)

            @pl.when(jnp.logical_or(u == 7, u == 8))
            def _():
                take(3, m)
                load_main(u)

            @pl.when(u != mixed)
            def _():
                wait_for(wdv.at[0], l_wd.at[m])

            @pl.when(u == mixed)
            def _():
                wait_for(wdv.at[2, pl.ds(0, 3 * rest), :], l_wd.at[2])

            def middle():
                @pl.when(jnp.logical_and(u == 1, lead))
                def _():
                    take(1, 0)

                @pl.when(u == 1)
                def _():
                    load_main(u + 1)

                @pl.when(jnp.logical_and(u == 2, other_core))
                def _():
                    load_main(u + 1)

                @pl.when(jnp.logical_and(u == 3, lead))
                def _():
                    take(1, 2)

                @pl.when(jnp.logical_and(u == 3, other_core))
                def _():
                    take(2, 0)

                @pl.when(u == 3)
                def _():
                    load_main(u + 1)

                @pl.when(jnp.logical_and(u == 4, lead))
                def _():
                    take(2, 1)
                    load_main(u + 1)

                @pl.when(jnp.logical_and(u == 5, other_core))
                def _():
                    take(2, 2)

                @pl.when(u == 5)
                def _():
                    load_rest(2)

                @pl.when(u == last - 1)
                def _():
                    take(3, 2)
                    load_rest(3)

                @pl.when(jnp.logical_and(u >= STAGES, u <= mixed))
                def _():
                    fetch(u - STAGES)

            def group(t, carry2):
                pl.when(t == 1)(middle)

                @pl.when(u >= STAGES)
                def _():
                    sent_back(t, one_block, s_ret.at[slot])

                def rows_of_group(r, carry3):
                    stage[slot, t, pl.ds(pl.multiple_of(r * g_tile, 8), g_tile), :] = times(group_rows(t, r), wdv[buf])
                    return carry3

                lax.fori_loop(0, 2, rows_of_group, 0)
                c = chunk(u, 0)
                send_back(t, stage.at[slot, t], back_ref.at[c, half, my_rows, :], s_ret.at[slot], r_back.at[c, half], l_ret.at[slot])
                return carry2

            lax.fori_loop(0, 2, group, 0)

            @pl.when(jnp.logical_and(u >= STAGES, u <= mixed))
            def _():
                add_up(u - STAGES)

            return carry

        lax.fori_loop(0, last, part, 0)
        wait_for(wdv.at[2, pl.ds(0, rest), :], l_wd.at[2])
        end_rows = pl.ds(pl.multiple_of(quarter(3) * rest, 8), rest)

        def end_group(t, carry):
            @pl.when(t == 1)
            def _():
                fetch(jnp.int32(7))

            def rows_of_group(r, carry2):
                stage_end[t, pl.ds(pl.multiple_of(r * g_tile, 8), g_tile), :] = times(group_rows(t, r), wdv[2, end_rows, :])
                return carry2

            lax.fori_loop(0, 2, rows_of_group, 0)
            send_back(t, stage_end.at[t], end_ref.at[half, my_rows, :], s_ret.at[STAGES], r_end.at[half], l_ret.at[STAGES])
            return carry

        lax.fori_loop(0, 2, end_group, 0)

        add_up(jnp.int32(7))
        fetch(jnp.int32(8))
        fetch_end()
        add_up(jnp.int32(8))
        add_end()
        for qt in quarters:
            c0, held = qt * d_q + 2 * wk, pl.ds(qt * rest, rest)

            @pl.when(jnp.logical_and(quarter(3) != qt, quarter(2) != qt))
            def _(c0=c0, held=held):
                to_y(c0, rest, lambda r0: acc[4, pl.ds(r0, t_tile), held])

            for buf, i in ((0, 3), (1, 2)):

                @pl.when(quarter(i) == qt)
                def _(c0=c0, held=held, buf=buf):
                    to_y(c0, rest, lambda r0: acc[4, pl.ds(r0, t_tile), held] + acc[buf, pl.ds(r0, t_tile), pl.ds(0, rest)])

        store = pltpu.make_async_copy(y, y_ref, l_x.at[0])
        store.start()

        for k in range(STAGES):
            for t in range(2):
                sent_back(t, one_block, s_ret.at[k])
        for t in range(2):
            sent_back(t, end_block, s_ret.at[STAGES])
        store.wait()

    pl.run_scoped(phase_up, pltpu.VMEM((rows, d_model), BF16), pltpu.VMEM((2, d_model, 2 * fc), BF16))
    pl.run_scoped(
        phase_down,
        pltpu.VMEM((3, wk, ffn), BF16),
        pltpu.VMEM((STAGES, 2, n_x * cap, wk), BF16),
        pltpu.VMEM((2, n_x * cap, rest), BF16),
        pltpu.VMEM((5, tok, wk), F32),
        pltpu.VMEM((2 * n_x, tok, cap), BF16),
        pltpu.VMEM((2, n_x * cap, wk), BF16),
        pltpu.VMEM((2, n_x * cap, rest), BF16),
        pltpu.VMEM((tok, d_model), BF16),
    )

    def drain_gu(k, carry):
        wait_for(gu_rows(k, 0), s_main.at[k])
        wait_for(gu_rows(k, 0), s_a.at[k])
        wait_for(gu_rows(k, 0), s_b.at[k])

        @pl.when(jnp.logical_not(lead))
        def _():
            wait_for(gu_rows(k, 0), s_c.at[k])

        return carry

    lax.fori_loop(0, n_k, drain_gu, 0)

    for m in parts3:
        for sem in (t_main, t_a, t_b):
            wait_for(wd_rows(0, m), sem.at[m])

    @pl.when(jnp.logical_not(lead))
    def _():
        for m in parts3:
            wait_for(wd_rows(0, m), t_c.at[m])


def solution(mesh):
    n_group, n_y = mesh.shape["expert"], mesh.shape["data"]
    assert n_y == 4 and n_group % 2 == 0
    n_x = n_group // 2
    tok_spec = P(("rep", "expert", "data"), None)
    wide_spec = P("expert", "data", None)
    down_spec = P("expert", None, "data")

    def device_step(x_loc, idx_loc, gate_loc, wg_loc, wu_loc, wd_loc):
        tok, d_model = x_loc.shape
        n_local, d_q, ffn = wg_loc.shape
        assert n_local == 1 and n_group == 8 and d_q % 72 == 0
        cap = capacity_rows(tok, idx_loc.shape[1], n_group)
        fc = pick(ffn, (384, 256, 128))
        n_k, n_j = ffn // fc, pick(d_model // 128, (3, 2, 1))
        rows = 2 * n_x * cap
        tile = pick(rows, (1280, 48, 8))
        dims = (n_x, tok, d_model, d_q, ffn, cap, fc, n_k, n_j, tile)
        hbm = pl.BlockSpec(memory_space=pl.ANY)
        vmem = pl.BlockSpec(memory_space=pltpu.VMEM)
        dma = pltpu.SemaphoreType.DMA
        shape = jax.ShapeDtypeStruct
        outs = pl.pallas_call(
            functools.partial(moe_kernel, dims),
            name="moe_layer",
            out_shape=[
                shape((tok, d_model), BF16),
                shape((tok, d_model), BF16),
                shape((rows, d_model), BF16),
                shape((n_k, d_model, 2 * fc), BF16),
                shape((4, d_q, ffn), BF16),
                shape((9, 2, n_x * cap, d_q // 9 * 4), BF16),
                shape((2, n_x * cap, d_q // 9), BF16),
            ],
            in_specs=[vmem, vmem, hbm, hbm, hbm, hbm],
            out_specs=[hbm] * 7,
            scratch_shapes=[
                pltpu.VMEM((rows, ffn), BF16),
                pltpu.VMEM((8, tok), F32),
                pltpu.VMEM((8, tok), F32),
                pltpu.VMEM((tok, 128), F32),
                *[dma((n_j + 1,)) for _ in "sr"], dma((n_x - 1,)), dma, dma((n_x - 1, n_j)), dma, dma((n_j + 1,)), dma((2,)),
                *[dma((n_k,)) for _ in "mabc"], dma((4, n_k)), dma((2,)),
                *[dma((3,)) for _ in "mabc"], dma((4, 3)), dma((3,)),
                dma((STAGES + 1, 2 * n_x)), dma((STAGES + 1,)), dma((9, 2)), *[dma((2,)) for _ in "ele"],
            ],
            compiler_params=pltpu.CompilerParams(collective_id=0, has_side_effects=True, vmem_limit_bytes=67_043_328),
        )(idx_loc.T, gate_loc.T, x_loc, wg_loc.reshape(d_q, ffn), wu_loc.reshape(d_q, ffn), wd_loc.reshape(ffn, d_q).T)
        return outs[0]

    return jax.shard_map(device_step, mesh=mesh, in_specs=(tok_spec, tok_spec, tok_spec, wide_spec, wide_spec, down_spec), out_specs=tok_spec, check_vma=False)
```
